32 devices in a mesh: gx: 4 (over x, core), gy: 4 (over z), gz: 2 (over y).
Axes of the slice: x: 2, y: 2, z: 4, core: 2. Of those that a mesh axis runs over, the one named last changes fastest.
Arguments:
- velocity: float32 [3, 32, 128, 512], P(None, 'gz', 'gy', 'gx'), may hold values from -14 to 14, as said below
- geometry: bfloat16 [6, 32, 128, 512], P(None, 'gz', 'gy', 'gx'), may hold values from -0.015 to 0.041, as said below
- mass_weights: bfloat16 [32, 128, 512], P('gz', 'gy', 'gx'), may hold values from 0.0099487305 to 0.099609375
Outputs:
- residual: float32 [3, 32, 128, 512], P(None, 'gz', 'gy', 'gx')
- kinetic: float32 [], replicated
- enstrophy: float32 [], replicated
The draws below stay inside these ranges and needn't reach their ends.
Inputs may be any that keep to these rules, and one draw needn't show every extreme that they name: `velocity`: coincident points of neighbouring elements hold equal values, and points on the outer boundary of the grid hold zero. `geometry`: at every point the matrix [[g0, g3, g4], [g3, g1, g5], [g4, g5, g2]] is positive definite.
All inputs are finite; a program needn't handle non-finite values.
Results may differ from the reference program's by a relative error of at most 0.0003.
Values sent between devices are 32-bit elements; how exact they have to be, the bound alone decides.
No kernel may reach another device: no remote copies, remote signals or barrier semaphores. Data moves between devices by JAX's collectives and lax.ppermute only.
A program may use at most 128 MiB of HBM per device.

```python
import math
import jax
import jax.numpy as jnp
import numpy as np
from jax import lax

ORDER = 7
POINTS = 8
GX = 512
GY = 128
GZ = 32


def join_faces(source, which_dim):
    position = lax.broadcasted_iota(jnp.int32, source.shape, which_dim)
    prev_val = jnp.roll(source, 1, which_dim)
    return jnp.where((position % (ORDER + 1) == 0) & (position > 0), prev_val, source)


def ramp_along(extent, which_dim):
    position = lax.broadcasted_iota(jnp.int32, extent, which_dim).astype(jnp.float32)
    return 0.5 + position / (extent[which_dim] - 1)


def draw_velocity(key, part):
    extent = (GZ, GY, GX)
    ramp_total = ramp_along(extent, 0) * ramp_along(extent, 1) * ramp_along(extent, 2)

    def one_component(comp_id):
        subkey = jax.random.fold_in(key, comp_id)
        noise = jnp.clip(jax.random.normal(subkey, extent, jnp.float32), -4.0, 4.0)
        field_now = noise * ramp_total
        field_now = join_faces(join_faces(join_faces(field_now, 2), 1), 0)
        inside = jnp.ones(extent, dtype=bool)
        for which_dim in range(3):
            position = lax.broadcasted_iota(jnp.int32, extent, which_dim)
            inside = inside & (position > 0) & (position < extent[which_dim] - 1)
        return jnp.where(inside, field_now, 0.0)
    return lax.map(one_component, jnp.arange(3)).astype(jnp.float32)


def draw_geometry(key, part):
    extent = (GZ, GY, GX)
    keyset = jax.random.split(key, 6)
    bottom, upper_end, reach = (0.003, 0.03, 0.3)
    diagonal = []
    for slot_id in range(3):
        drawn = jax.random.uniform(keyset[slot_id], extent, jnp.float32, math.log(bottom), math.log(upper_end))
        diagonal.append(jnp.exp(drawn))
    pairs_list = ((0, 1), (0, 2), (1, 2))
    offdiag = []
    for slot_id in range(3):
        first_id, second_id = pairs_list[slot_id]
        factor = jax.random.uniform(keyset[3 + slot_id], extent, jnp.float32, -reach, reach)
        offdiag.append(factor * jnp.sqrt(diagonal[first_id] * diagonal[second_id]))
    return jnp.stack(diagonal + offdiag, 0).astype(jnp.bfloat16)


def level_of(rng, shape, cuts, low, largest):
    level = 1.0
    for dim, shards_of in cuts:
        draws = jax.random.uniform(jax.random.fold_in(jax.random.fold_in(rng, 6), dim), (shards_of,), jnp.float32, low / len(cuts), largest / len(cuts))
        level = level * jnp.repeat(jnp.exp(draws), shape[dim] // shards_of).reshape((-1,) + (1,) * (len(shape) - 1 - dim))
    return level


def setup_inputs(seed: int = 0) -> dict:
    key_list = jax.random.split(jax.random.key(seed), 4)
    return {
        "velocity": draw_velocity(jax.random.fold_in(key_list[3], 71), 0),
        "geometry": draw_geometry(jax.random.fold_in(key_list[3], 71), 0),
        "mass_weights": jnp.clip(jnp.exp(math.log(0.099609375) - 2.3038113 * jax.random.uniform(key_list[2], (GZ, GY, GX), jnp.float32) ** level_of(key_list[2], (GZ, GY, GX), ((0, 2), (1, 4), (2, 4)), -0.2, 0.2)), 0.0099487305, 0.099609375).astype(jnp.bfloat16),
    }


def gll_derivative(poly_order):
    node_count = poly_order + 1
    abscissa = np.cos(np.pi * np.arange(node_count) / poly_order)
    legendre = np.zeros((node_count, node_count))
    for newton_step in range(60):
        legendre[:, 0] = 1.0
        legendre[:, 1] = abscissa
        for degree in range(2, node_count):
            legendre[:, degree] = ((2 * degree - 1) * abscissa * legendre[:, degree - 1] - (degree - 1) * legendre[:, degree - 2]) / degree
        abscissa = abscissa - (abscissa * legendre[:, poly_order] - legendre[:, poly_order - 1]) / (node_count * legendre[:, poly_order])
    abscissa = abscissa[::-1]
    end_values = legendre[::-1, poly_order]
    spacing = abscissa[:, None] - abscissa[None, :] + np.eye(node_count)
    deriv_table = end_values[:, None] / end_values[None, :] / spacing
    deriv_table = deriv_table * (1.0 - np.eye(node_count))
    deriv_table[0, 0] = -poly_order * node_count / 4.0
    deriv_table[poly_order, poly_order] = poly_order * node_count / 4.0
    return deriv_table.astype(np.float32)


def derive(source, matrix, which_dim):
    highest = lax.Precision.HIGHEST
    points = matrix.shape[0]
    extent = source.shape
    split_shape = extent[:which_dim] + (extent[which_dim] // points, points) + extent[which_dim + 1:]
    pieces = source.reshape(split_shape)
    if which_dim == 3:
        result = jnp.einsum('czyex,wx->czyew', pieces, matrix, precision=highest)
    elif which_dim == 2:
        result = jnp.einsum('czeyx,wy->czewx', pieces, matrix, precision=highest)
    else:
        result = jnp.einsum('cezyx,wz->cewyx', pieces, matrix, precision=highest)
    return result.reshape(extent)


def metric(geometry, slot_id):
    return geometry[slot_id].astype(jnp.float32)[None]


def apply_local(velocity, geometry, matrix):
    grad_r = derive(velocity, matrix, 3)
    grad_s = derive(velocity, matrix, 2)
    grad_t = derive(velocity, matrix, 1)
    flux_r = metric(geometry, 0) * grad_r + metric(geometry, 3) * grad_s + metric(geometry, 4) * grad_t
    flux_s = metric(geometry, 3) * grad_r + metric(geometry, 1) * grad_s + metric(geometry, 5) * grad_t
    flux_t = metric(geometry, 4) * grad_r + metric(geometry, 5) * grad_s + metric(geometry, 2) * grad_t
    enstrophy_part = jnp.sum(grad_r * flux_r + grad_s * flux_s + grad_t * flux_t)
    transposed = matrix.T
    applied = derive(flux_r, transposed, 3) + derive(flux_s, transposed, 2) + derive(flux_t, transposed, 1)
    return applied, enstrophy_part


def assemble_axis(source, which_dim):
    length = source.shape[which_dim]
    position = lax.broadcasted_iota(jnp.int32, source.shape, which_dim)
    next_val = jnp.roll(source, -1, which_dim)
    prev_val = jnp.roll(source, 1, which_dim)
    up_mask = (position % POINTS == POINTS - 1) & (position < length - 1)
    low_mask = (position % POINTS == 0) & (position > 0)
    return source + jnp.where(up_mask, next_val, 0.0) + jnp.where(low_mask, prev_val, 0.0)


def assemble_one(single_field):
    return assemble_axis(assemble_axis(assemble_axis(single_field, 2), 1), 0)


def reference(velocity, geometry, mass_weights):
    matrix = jnp.asarray(gll_derivative(ORDER), jnp.float32)
    mass_float = mass_weights.astype(jnp.float32)
    kinetic = 0.5 * jnp.sum(mass_float[None] * velocity * velocity)
    layers = velocity.shape[1] // POINTS

    def layer_step(layer_id, state_pair):
        applied, energy = state_pair
        offset = (layer_id * POINTS).astype(jnp.int32)
        block_vel = lax.dynamic_slice_in_dim(velocity, offset, POINTS, 1)
        block_geo = lax.dynamic_slice_in_dim(geometry, offset, POINTS, 1)
        part_field, part_energy = apply_local(block_vel, block_geo, matrix)
        applied = lax.dynamic_update_slice_in_dim(applied, part_field, offset, 1)
        return applied, energy + part_energy

    start_pair = (jnp.zeros(velocity.shape, jnp.float32), jnp.zeros((), jnp.float32))
    applied, enstrophy = lax.fori_loop(0, layers, layer_step, start_pair)
    stacked = jnp.concatenate([applied, mass_float[None]], 0)
    assembled = lax.map(assemble_one, stacked)
    extent = velocity.shape[1:]
    interior = jnp.ones(extent, dtype=bool)
    for which_dim in range(3):
        position = lax.broadcasted_iota(jnp.int32, extent, which_dim)
        interior = interior & (position > 0) & (position < extent[which_dim] - 1)
    rayleigh = enstrophy / (2.0 * kinetic)
    residual = jnp.where(interior[None], assembled[:3] - rayleigh * assembled[3][None] * velocity, 0.0)
    return residual, kinetic, enstrophy
```

```python
import functools

import jax
import jax.numpy as jnp
import numpy as np
from jax import lax
from jax.experimental import pallas as pl
from jax.experimental.pallas import tpu as pltpu
from jax.sharding import PartitionSpec as P

ORDER = 7
PTS = ORDER + 1
F32 = jnp.float32
BF16 = jnp.bfloat16
SCALAR_ROWS = 16


def gll_derivative(poly_order):
    node_count = poly_order + 1
    abscissa = np.cos(np.pi * np.arange(node_count) / poly_order)
    legendre = np.zeros((node_count, node_count))
    for newton_step in range(60):
        legendre[:, 0] = 1.0
        legendre[:, 1] = abscissa
        for degree in range(2, node_count):
            legendre[:, degree] = (
                (2 * degree - 1) * abscissa * legendre[:, degree - 1]
                - (degree - 1) * legendre[:, degree - 2]
            ) / degree
        abscissa = abscissa - (abscissa * legendre[:, poly_order] - legendre[:, poly_order - 1]) / (
            node_count * legendre[:, poly_order]
        )
    abscissa = abscissa[::-1]
    end_values = legendre[::-1, poly_order]
    spacing = abscissa[:, None] - abscissa[None, :] + np.eye(node_count)
    deriv_table = end_values[:, None] / end_values[None, :] / spacing
    deriv_table = deriv_table * (1.0 - np.eye(node_count))
    deriv_table[0, 0] = -poly_order * node_count / 4.0
    deriv_table[poly_order, poly_order] = poly_order * node_count / 4.0
    return deriv_table.astype(np.float32)


def split(x):
    high = x.astype(BF16)
    return high, (x - high.astype(F32)).astype(BF16)


def iota(shape, dim):
    return lax.broadcasted_iota(jnp.int32, shape, dim)


def block_diagonal(tile, size):
    wide = jnp.concatenate([tile] * (size // 128), axis=1)
    full = jnp.concatenate([wide] * (size // PTS), axis=0)
    same = iota((size, size), 0) // PTS == iota((size, size), 1) // PTS
    return split(jnp.where(same, full, 0.0))


def combine_planes(planes, table):
    half = PTS // 2
    even = [planes[k] + planes[PTS - 1 - k] for k in range(half)]
    odd = [planes[k] - planes[PTS - 1 - k] for k in range(half)]
    low, high = [], []
    for w in range(half):
        p = q = None
        for k in range(half):
            a, b = float(table[w, k]), float(table[w, PTS - 1 - k])
            pe = np.float32((a + b) / 2) * even[k]
            qo = np.float32((a - b) / 2) * odd[k]
            p = pe if p is None else p + pe
            q = qo if q is None else q + qo
        low.append(p + q)
        high.append(q - p)
    return low + high[::-1]


def dot(a, b):
    return jnp.dot(a, b, preferred_element_type=F32)


def assemble_plane(u, ny, nx):
    lane = iota((PTS, nx), 1)
    sub = iota((PTS, nx), 0)
    last = (lane % PTS == PTS - 1) & (lane < nx - 1)
    first = (lane % PTS == 0) & (lane > 0)
    tiles = []
    for e in range(ny // PTS):
        t = u[e * PTS : (e + 1) * PTS]
        t = (
            t
            + jnp.where(last, pltpu.roll(t, nx - 1, 1), 0.0)
            + jnp.where(first, pltpu.roll(t, 1, 1), 0.0)
        )
        tiles.append(t)
    done = []
    for e, t in enumerate(tiles):
        if e + 1 < len(tiles):
            t = t + jnp.where(sub == PTS - 1, pltpu.roll(tiles[e + 1], PTS - 1, 0), 0.0)
        if e > 0:
            t = t + jnp.where(sub == 0, pltpu.roll(tiles[e - 1], 1, 0), 0.0)
        done.append(t)
    return jnp.concatenate(done, axis=0)


def local_kernel(table, v_ref, g_ref, m_ref, d_ref, dt_ref, u_ref, px_ref, gr_ref, gs_ref):
    comps, nz, ny, nx = v_ref.shape
    rows = PTS * ny
    right_h, right_l = block_diagonal(dt_ref[...], nx)
    right_hh = jnp.concatenate([right_h, right_h], axis=0)
    left_h, left_l = block_diagonal(d_ref[...], rows)
    left = jnp.concatenate([left_h, left_l, left_h], axis=1)
    back_h, back_l = block_diagonal(d_ref[...], nx)
    back_hh = jnp.concatenate([back_h, back_h], axis=0)
    leftt_h, leftt_l = block_diagonal(dt_ref[...], rows)
    leftt = jnp.concatenate([leftt_h, leftt_l, leftt_h], axis=1)
    kin = jnp.zeros((PTS, nx), F32)
    ens = jnp.zeros((PTS, nx), F32)
    for layer in range(nz // PTS):
        z0 = layer * PTS
        vh, vl = [], []
        for c in range(comps):
            h, l = split(v_ref[c, z0 : z0 + PTS].reshape(rows, nx))
            vh.append(h)
            vl.append(l)
        vh_all = jnp.concatenate(vh, axis=1)
        vl_all = jnp.concatenate(vl, axis=1)
        grad_s = dot(left, jnp.concatenate([vh_all, vh_all, vl_all], axis=0))
        for c in range(comps):
            gs_ref[c] = grad_s[:, c * nx : (c + 1) * nx].reshape(PTS, ny, nx)
            gr_ref[c] = (
                dot(jnp.concatenate([vh[c], vl[c]], axis=1), right_hh) + dot(vh[c], right_l)
            ).reshape(PTS, ny, nx)
        for e in range(ny // PTS):
            ys = slice(e * PTS, (e + 1) * PTS)
            g = [
                [g_ref[i, z0 + z, ys].astype(F32) for z in range(PTS)] for i in range(6)
            ]
            mass = [m_ref[z0 + z, ys].astype(F32) for z in range(PTS)]
            for z in range(PTS):
                u_ref[comps, z0 + z, ys] = mass[z]
            for c in range(comps):
                v = [v_ref[c, z0 + z, ys] for z in range(PTS)]
                gt = combine_planes(v, table)
                ft = []
                for z in range(PTS):
                    gr, gs = gr_ref[c, z, ys], gs_ref[c, z, ys]
                    kin = kin + mass[z] * (v[z] * v[z])
                    fr = g[0][z] * gr + g[3][z] * gs + g[4][z] * gt[z]
                    fs = g[3][z] * gr + g[1][z] * gs + g[5][z] * gt[z]
                    f3 = g[4][z] * gr + g[5][z] * gs + g[2][z] * gt[z]
                    ens = ens + (gr * fr + gs * fs + gt[z] * f3)
                    gr_ref[c, z, ys] = fr
                    gs_ref[c, z, ys] = fs
                    ft.append(f3)
                at = combine_planes(ft, table.T)
                for z in range(PTS):
                    u_ref[c, z0 + z, ys] = at[z]
        fsh, fsl = [], []
        for c in range(comps):
            h, l = split(gs_ref[c].reshape(rows, nx))
            fsh.append(h)
            fsl.append(l)
        fsh_all = jnp.concatenate(fsh, axis=1)
        fsl_all = jnp.concatenate(fsl, axis=1)
        div_s = dot(leftt, jnp.concatenate([fsh_all, fsh_all, fsl_all], axis=0))
        for c in range(comps):
            h, l = split(gr_ref[c].reshape(rows, nx))
            div_r = dot(jnp.concatenate([h, l], axis=1), back_hh) + dot(h, back_l)
            total = div_r + div_s[:, c * nx : (c + 1) * nx]
            u_ref[c, z0 : z0 + PTS] = u_ref[c, z0 : z0 + PTS] + total.reshape(PTS, ny, nx)
    lane = iota((ny, nx), 1)
    packed = jnp.zeros((ny, nx), F32)
    for f in range(comps + 1):
        for z in range(nz):
            u_ref[f, z] = assemble_plane(u_ref[f, z], ny, nx)
        for z in range(PTS - 1, nz - 1, PTS):
            both = u_ref[f, z] + u_ref[f, z + 1]
            u_ref[f, z] = both
            u_ref[f, z + 1] = both
        for z in range(nz):
            j = f * nz + z
            moved = pltpu.roll(u_ref[f, z], 2 * j, 1) if j else u_ref[f, z]
            packed = jnp.where((lane == 2 * j) | (lane == (2 * j - 1) % nx), moved, packed)
    px_ref[0:ny] = packed
    px_ref[ny : ny + PTS] = kin
    px_ref[ny + PTS : ny + 2 * PTS] = ens


def merge_sides(right, left):
    lane = iota(right.shape, 1)
    return jnp.where(lane % 2 == 0, right, pltpu.roll(left, 2, 1))


def place_columns(merged, j, nx):
    lane = iota(merged.shape, 1)
    shift = (nx - 1 - 2 * j) % nx
    moved = pltpu.roll(merged, shift, 1) if shift else merged
    return jnp.where((lane == 0) | (lane == nx - 1), moved, 0.0)


def first_kernel(u_ref, px_ref, qa_ref, pb_ref, pz_ref):
    fields, nz, ny, nx = u_ref.shape
    x_even = lax.axis_index("gx") % 2 == 0
    z_even = lax.axis_index("gz") % 2 == 0
    qa = qa_ref[0:ny]
    merged = merge_sides(jnp.where(x_even, qa, 0.0), jnp.where(x_even, 0.0, qa))
    sums = px_ref[ny:] + qa_ref[ny:]
    pb_ref[0:ny] = px_ref[0:ny]
    pb_ref[ny:] = sums
    for f in range(fields):
        ends = [
            u_ref[f, z] + place_columns(merged, f * nz + z, nx) for z in (0, nz - 1)
        ]
        pz_ref[f * ny : (f + 1) * ny] = jnp.where(z_even, ends[1], ends[0])
    pz_ref[fields * ny :] = sums


def x_sides(qa, qb, x_even):
    return merge_sides(jnp.where(x_even, qa, qb), jnp.where(x_even, qb, qa))


def diagonal_sides(qd, x_even):
    return merge_sides(jnp.where(x_even, 0.0, qd), jnp.where(x_even, qd, 0.0))


def second_kernel(
    u_ref, pb_ref, qa_ref, qb_ref, qz_ref, qd_ref, pya_ref, pyb_ref, ps_ref, low_ref, high_ref
):
    fields, nz, ny, nx = u_ref.shape
    x_even = lax.axis_index("gx") % 2 == 0
    y_even = lax.axis_index("gy") % 2 == 0
    for ys, row, out in (
        (slice(0, PTS), 0, low_ref),
        (slice(ny - PTS, ny), PTS - 1, high_ref),
    ):
        merged = x_sides(qa_ref[ys], qb_ref[ys], x_even)
        diag = diagonal_sides(qd_ref[ys], x_even)
        for f in range(fields):
            for z in range(nz):
                j = f * nz + z
                t = u_ref[f, z, ys] + place_columns(merged, j, nx)
                if z in (0, nz - 1):
                    t = t + qz_ref[f * ny + ys.start : f * ny + ys.stop]
                    t = t + place_columns(diag, f * nz + nz - 1 - z, nx)
                out[j : j + 1] = t[row : row + 1]
    sums = pb_ref[ny:] + qb_ref[ny:] + qz_ref[fields * ny :] + qd_ref[ny:]
    count = fields * nz
    pya_ref[0:count] = jnp.where(y_even, high_ref[...], low_ref[...])
    pyb_ref[0:count] = jnp.where(y_even, low_ref[...], high_ref[...])
    pya_ref[count:] = sums
    pyb_ref[count:] = sums
    ps_ref[...] = sums


def last_kernel(
    sizes,
    v_ref,
    u_ref,
    qa_ref,
    qb_ref,
    qz_ref,
    qd_ref,
    qya_ref,
    qyb_ref,
    qs_ref,
    ps_ref,
    out_ref,
    kin_ref,
    ens_ref,
    low_ref,
    high_ref,
):
    fields, nz, ny, nx = u_ref.shape
    gx, gy, gz = (lax.axis_index(name) for name in ("gx", "gy", "gz"))
    x_even, y_even = gx % 2 == 0, gy % 2 == 0
    count = fields * nz
    sums = ps_ref[...] + qya_ref[count:] + qyb_ref[count:] + qs_ref[...]
    kinetic = 0.5 * jnp.sum(sums[0:PTS])
    enstrophy = jnp.sum(sums[PTS : 2 * PTS])
    kin_ref[0, 0] = kinetic
    ens_ref[0, 0] = enstrophy
    rayleigh = jnp.full((ny, nx), enstrophy, F32) / jnp.full((ny, nx), 2.0 * kinetic, F32)
    low_ref[...] = jnp.where(y_even, qyb_ref[0:count], qya_ref[0:count])
    high_ref[...] = jnp.where(y_even, qya_ref[0:count], qyb_ref[0:count])
    merged = x_sides(qa_ref[0:ny], qb_ref[0:ny], x_even)
    diag = diagonal_sides(qd_ref[0:ny], x_even)
    row = iota((ny, nx), 0)
    lane = iota((ny, nx), 1)
    x_first = jnp.where(gx == 0, 0, -1)
    x_last = jnp.where(gx == sizes[0] - 1, nx - 1, -1)
    y_first = jnp.where(gy == 0, 0, -1)
    y_last = jnp.where(gy == sizes[1] - 1, ny - 1, -1)
    inside = (lane != x_first) & (lane != x_last) & (row != y_first) & (row != y_last)
    sub = iota((PTS, nx), 0)
    for z in range(nz):
        whole = []
        for f in range(fields):
            j = f * nz + z
            t = u_ref[f, z] + place_columns(merged, j, nx)
            if z in (0, nz - 1):
                t = t + qz_ref[f * ny : (f + 1) * ny]
                t = t + place_columns(diag, f * nz + nz - 1 - z, nx)
            low = jnp.where(sub == 0, low_ref[j : j + 1], 0.0)
            high = jnp.where(sub == PTS - 1, high_ref[j : j + 1], 0.0)
            t = jnp.concatenate(
                [t[0:PTS] + low, t[PTS : ny - PTS], t[ny - PTS : ny] + high], axis=0
            )
            whole.append(t)
        scaled = rayleigh * whole[fields - 1]
        keep = inside
        if z == 0:
            keep = keep & (gz > 0)
        if z == nz - 1:
            keep = keep & (gz < sizes[2] - 1)
        for c in range(fields - 1):
            out_ref[c, z] = jnp.where(keep, whole[c] - scaled * v_ref[c, z], 0.0)


VMEM = pl.BlockSpec(memory_space=pltpu.VMEM)
SMEM = pl.BlockSpec(memory_space=pltpu.SMEM)


def call(kernel, name, outs, ins, scratch=(), out_specs=None, flops=1 << 20):
    return pl.pallas_call(
        kernel,
        out_shape=[jax.ShapeDtypeStruct(shape, F32) for shape in outs],
        in_specs=[VMEM] * len(ins),
        out_specs=out_specs or [VMEM] * len(outs),
        scratch_shapes=list(scratch),
        compiler_params=pltpu.CompilerParams(vmem_limit_bytes=24 << 20),
        cost_estimate=pl.CostEstimate(flops=flops, bytes_accessed=flops, transcendentals=0),
        name=name,
    )(*ins)


def local_part(velocity, geometry, mass_weights):
    comps, nz, ny, nx = velocity.shape
    table = gll_derivative(ORDER)
    tile = np.tile(table, (1, 128 // PTS))
    tile_t = np.tile(table.T, (1, 128 // PTS))
    return call(
        functools.partial(local_kernel, table),
        "local",
        [(comps + 1, nz, ny, nx), (ny + SCALAR_ROWS, nx)],
        [velocity, geometry, mass_weights, jnp.asarray(tile), jnp.asarray(tile_t)],
        scratch=[pltpu.VMEM((comps, PTS, ny, nx), F32)] * 2,
    )


def pairs_near(count):
    return [(i, i ^ 1) for i in range(count)]


def pairs_mirror(count):
    return [(i, count - 1 - i) for i in range(count)]


def few_rounds(sizes, velocity, geometry, mass_weights):
    comps, nz, ny, nx = velocity.shape
    fields = comps + 1
    u, px = local_part(velocity, geometry, mass_weights)
    qa = lax.ppermute(px, "gx", pairs_near(sizes[0]))
    pb, pz = call(
        first_kernel,
        "first",
        [(ny + SCALAR_ROWS, nx), (fields * ny + SCALAR_ROWS, nx)],
        [u, px, qa],
    )
    mirror = pairs_mirror(sizes[0])
    qb = lax.ppermute(pb, "gx", mirror)
    qz = lax.ppermute(pz, "gz", pairs_near(sizes[2]))
    both = [
        (i * sizes[2] + k, mirror[i][1] * sizes[2] + (k ^ 1))
        for i in range(sizes[0])
        for k in range(sizes[2])
    ]
    qd = lax.ppermute(pb, ("gx", "gz"), both)
    count = fields * nz
    pya, pyb, ps = call(
        second_kernel,
        "second",
        [(count + SCALAR_ROWS, nx), (count + SCALAR_ROWS, nx), (SCALAR_ROWS, nx)],
        [u, pb, qa, qb, qz, qd],
        scratch=[pltpu.VMEM((count, nx), F32)] * 2,
    )
    qya = lax.ppermute(pya, "gy", pairs_near(sizes[1]))
    qyb = lax.ppermute(pyb, "gy", pairs_mirror(sizes[1]))
    qs = lax.ppermute(ps, "gy", [(i, i ^ 2) for i in range(sizes[1])])
    residual, kinetic, enstrophy = call(
        functools.partial(last_kernel, sizes),
        "last",
        [velocity.shape, (1, 1), (1, 1)],
        [velocity, u, qa, qb, qz, qd, qya, qyb, qs, ps],
        scratch=[pltpu.VMEM((count, nx), F32)] * 2,
        out_specs=[VMEM, SMEM, SMEM],
    )
    return residual, kinetic[0, 0], enstrophy[0, 0]


def add_neighbours(field, axis, dim):
    count = lax.axis_size(axis)
    extent = field.shape[dim]
    first = lax.slice_in_dim(field, 0, 1, axis=dim)
    last = lax.slice_in_dim(field, extent - 1, extent, axis=dim)
    low = lax.ppermute(last, axis, [(i, i + 1) for i in range(count - 1)])
    high = lax.ppermute(first, axis, [(i + 1, i) for i in range(count - 1)])
    middle = lax.slice_in_dim(field, 1, extent - 1, axis=dim)
    return jnp.concatenate([first + low, middle, last + high], axis=dim)


def any_mesh(sizes, velocity, geometry, mass_weights):
    comps, nz, ny, nx = velocity.shape
    u, px = local_part(velocity, geometry, mass_weights)
    kinetic = 0.5 * jnp.sum(px[ny : ny + PTS])
    enstrophy = jnp.sum(px[ny + PTS :])
    kinetic, enstrophy = lax.psum((kinetic, enstrophy), ("gx", "gy", "gz"))
    for axis, dim in (("gx", 3), ("gy", 2), ("gz", 1)):
        u = add_neighbours(u, axis, dim)
    inside = jnp.ones((nz, ny, nx), bool)
    for dim, (axis, size) in enumerate(zip(("gz", "gy", "gx"), sizes[::-1])):
        place = lax.axis_index(axis) * inside.shape[dim] + iota(inside.shape, dim)
        inside = inside & (place > 0) & (place < size * inside.shape[dim] - 1)
    rayleigh = enstrophy / (2.0 * kinetic)
    residual = jnp.where(inside[None], u[:comps] - rayleigh * u[comps][None] * velocity, 0.0)
    return residual, kinetic, enstrophy


def solution(mesh):
    sizes = tuple(mesh.shape[name] for name in ("gx", "gy", "gz"))
    plan = few_rounds if sizes == (4, 4, 2) else any_mesh
    in_specs = (P(None, "gz", "gy", "gx"), P(None, "gz", "gy", "gx"), P("gz", "gy", "gx"))
    out_specs = (P(None, "gz", "gy", "gx"), P(), P())
    return jax.shard_map(
        functools.partial(plan, sizes),
        mesh=mesh,
        in_specs=in_specs,
        out_specs=out_specs,
        check_vma=False,
    )
```

```python
import functools

import jax
import jax.numpy as jnp
import numpy as np
from jax import lax
from jax.experimental import pallas as pl
from jax.experimental.pallas import tpu as pltpu
from jax.sharding import PartitionSpec as P

ORDER = 7
PTS = ORDER + 1
F32 = jnp.float32
BF16 = jnp.bfloat16
SCALAR_ROWS = 16


def gll_derivative(poly_order):
    node_count = poly_order + 1
    abscissa = np.cos(np.pi * np.arange(node_count) / poly_order)
    legendre = np.zeros((node_count, node_count))
    for newton_step in range(60):
        legendre[:, 0] = 1.0
        legendre[:, 1] = abscissa
        for degree in range(2, node_count):
            legendre[:, degree] = (
                (2 * degree - 1) * abscissa * legendre[:, degree - 1]
                - (degree - 1) * legendre[:, degree - 2]
            ) / degree
        abscissa = abscissa - (abscissa * legendre[:, poly_order] - legendre[:, poly_order - 1]) / (
            node_count * legendre[:, poly_order]
        )
    abscissa = abscissa[::-1]
    end_values = legendre[::-1, poly_order]
    spacing = abscissa[:, None] - abscissa[None, :] + np.eye(node_count)
    deriv_table = end_values[:, None] / end_values[None, :] / spacing
    deriv_table = deriv_table * (1.0 - np.eye(node_count))
    deriv_table[0, 0] = -poly_order * node_count / 4.0
    deriv_table[poly_order, poly_order] = poly_order * node_count / 4.0
    return deriv_table.astype(np.float32)


def split(x):
    high = x.astype(BF16)
    return high, (x - high.astype(F32)).astype(BF16)


def iota(shape, dim):
    return lax.broadcasted_iota(jnp.int32, shape, dim)


def block_diagonal(tile, size):
    wide = jnp.concatenate([tile] * (size // 128), axis=1)
    full = jnp.concatenate([wide] * (size // PTS), axis=0)
    same = iota((size, size), 0) // PTS == iota((size, size), 1) // PTS
    return split(jnp.where(same, full, 0.0))


def combine_planes(planes, table):
    half = PTS // 2
    even = [planes[k] + planes[PTS - 1 - k] for k in range(half)]
    odd = [planes[k] - planes[PTS - 1 - k] for k in range(half)]
    low, high = [], []
    for w in range(half):
        p = q = None
        for k in range(half):
            a, b = float(table[w, k]), float(table[w, PTS - 1 - k])
            pe = np.float32((a + b) / 2) * even[k]
            qo = np.float32((a - b) / 2) * odd[k]
            p = pe if p is None else p + pe
            q = qo if q is None else q + qo
        low.append(p + q)
        high.append(q - p)
    return low + high[::-1]


def dot(a, b):
    return jnp.dot(a, b, preferred_element_type=F32)


def join_rows(tiles, sub):
    done = []
    for e, t in enumerate(tiles):
        if e + 1 < len(tiles):
            t = t + jnp.where(sub == PTS - 1, pltpu.roll(tiles[e + 1], PTS - 1, 0), 0.0)
        if e > 0:
            t = t + jnp.where(sub == 0, pltpu.roll(tiles[e - 1], 1, 0), 0.0)
        done.append(t)
    return done


def assemble_plane(u, ny, nx):
    lane = iota((PTS, nx), 1)
    sub = iota((PTS, nx), 0)
    last = (lane % PTS == PTS - 1) & (lane < nx - 1)
    first = (lane % PTS == 0) & (lane > 0)
    tiles = []
    for e in range(ny // PTS):
        t = u[e * PTS : (e + 1) * PTS]
        t = (
            t
            + jnp.where(last, pltpu.roll(t, nx - 1, 1), 0.0)
            + jnp.where(first, pltpu.roll(t, 1, 1), 0.0)
        )
        tiles.append(t)
    return jnp.concatenate(join_rows(tiles, sub), axis=0)


def table_tile(table, nx):
    sub = iota((PTS, nx), 0)
    lane = iota((PTS, nx), 1) % PTS
    tile = jnp.zeros((PTS, nx), F32)
    for k in range(PTS):
        column = jnp.full((PTS, nx), float(table[0, k]), F32)
        for w in range(1, PTS):
            column = jnp.where(sub == w, float(table[w, k]), column)
        tile = jnp.where(lane == k, column, tile)
    return tile


def local_kernel(
    table, v_hbm, g_hbm, m_hbm, u_ref, px_ref, v_ref, m_ref, g_ref, gr_ref, gs_ref, sems
):
    comps, nz, ny, nx = v_ref.shape
    layers = nz // PTS
    copies = []
    for layer in range(layers):
        zs = pl.ds(layer * PTS, PTS)
        copies.append(
            [
                pltpu.make_async_copy(v_hbm.at[:, zs], v_ref.at[:, zs], sems.at[layer, 0]),
                pltpu.make_async_copy(g_hbm.at[:, zs], g_ref.at[:, zs], sems.at[layer, 1]),
                pltpu.make_async_copy(m_hbm.at[zs], m_ref.at[zs], sems.at[layer, 2]),
            ]
        )
    for group in copies:
        for copy in group:
            copy.start()
    rows = PTS * ny
    tile, tile_t = table_tile(table, nx), table_tile(table.T, nx)
    right_h, right_l = block_diagonal(tile_t, nx)
    right_hh = jnp.concatenate([right_h, right_h], axis=0)
    left_h, left_l = block_diagonal(tile, rows)
    left = jnp.concatenate([left_h, left_l, left_h], axis=1)
    back_h, back_l = block_diagonal(tile, nx)
    back_hh = jnp.concatenate([back_h, back_h], axis=0)
    leftt_h, leftt_l = block_diagonal(tile_t, rows)
    leftt = jnp.concatenate([leftt_h, leftt_l, leftt_h], axis=1)
    kin = jnp.zeros((PTS, nx), F32)
    ens = jnp.zeros((PTS, nx), F32)
    for layer in range(layers):
        z0 = layer * PTS
        copies[layer][0].wait()
        vh, vl = [], []
        for c in range(comps):
            h, l = split(v_ref[c, z0 : z0 + PTS].reshape(rows, nx))
            vh.append(h)
            vl.append(l)
        vh_all = jnp.concatenate(vh, axis=1)
        vl_all = jnp.concatenate(vl, axis=1)
        grad_s = dot(left, jnp.concatenate([vh_all, vh_all, vl_all], axis=0))
        for c in range(comps):
            gs_ref[c] = grad_s[:, c * nx : (c + 1) * nx].reshape(PTS, ny, nx)
            gr_ref[c] = (
                dot(jnp.concatenate([vh[c], vl[c]], axis=1), right_hh) + dot(vh[c], right_l)
            ).reshape(PTS, ny, nx)
        copies[layer][1].wait()
        copies[layer][2].wait()
        for e in range(ny // PTS):
            ys = slice(e * PTS, (e + 1) * PTS)
            g = [
                [g_ref[i, z0 + z, ys].astype(F32) for z in range(PTS)] for i in range(6)
            ]
            mass = [m_ref[z0 + z, ys].astype(F32) for z in range(PTS)]
            for z in range(PTS):
                u_ref[comps, z0 + z, ys] = mass[z]
            for c in range(comps):
                v = [v_ref[c, z0 + z, ys] for z in range(PTS)]
                gt = combine_planes(v, table)
                ft = []
                for z in range(PTS):
                    gr, gs = gr_ref[c, z, ys], gs_ref[c, z, ys]
                    kin = kin + mass[z] * (v[z] * v[z])
                    fr = g[0][z] * gr + g[3][z] * gs + g[4][z] * gt[z]
                    fs = g[3][z] * gr + g[1][z] * gs + g[5][z] * gt[z]
                    f3 = g[4][z] * gr + g[5][z] * gs + g[2][z] * gt[z]
                    ens = ens + (gr * fr + gs * fs + gt[z] * f3)
                    gr_ref[c, z, ys] = fr
                    gs_ref[c, z, ys] = fs
                    ft.append(f3)
                at = combine_planes(ft, table.T)
                for z in range(PTS):
                    u_ref[c, z0 + z, ys] = at[z]
        fsh, fsl = [], []
        for c in range(comps):
            h, l = split(gs_ref[c].reshape(rows, nx))
            fsh.append(h)
            fsl.append(l)
        fsh_all = jnp.concatenate(fsh, axis=1)
        fsl_all = jnp.concatenate(fsl, axis=1)
        div_s = dot(leftt, jnp.concatenate([fsh_all, fsh_all, fsl_all], axis=0))
        for c in range(comps):
            h, l = split(gr_ref[c].reshape(rows, nx))
            div_r = dot(jnp.concatenate([h, l], axis=1), back_hh) + dot(h, back_l)
            total = div_r + div_s[:, c * nx : (c + 1) * nx]
            u_ref[c, z0 : z0 + PTS] = u_ref[c, z0 : z0 + PTS] + total.reshape(PTS, ny, nx)
    px_ref[0:ny] = pack_columns(u_ref)
    px_ref[ny : ny + PTS] = kin
    px_ref[ny + PTS : ny + 2 * PTS] = ens


def pack_columns(u_ref):
    fields, nz, ny, nx = u_ref.shape
    lane = iota((ny, nx), 1)
    packed = jnp.zeros((ny, nx), F32)
    for f in range(fields):
        for z in range(nz):
            j = f * nz + z
            moved = pltpu.roll(u_ref[f, z], 2 * j, 1) if j else u_ref[f, z]
            packed = jnp.where((lane == 2 * j) | (lane == (2 * j - 1) % nx), moved, packed)
    sub = iota((PTS, nx), 0)
    tiles = [packed[e : e + PTS] for e in range(0, ny, PTS)]
    packed = jnp.concatenate(join_rows(tiles, sub), axis=0)
    plane = (lane + 1) % nx // 2 % nz
    up = (plane % PTS == PTS - 1) & (plane < nz - 1)
    down = (plane % PTS == 0) & (plane > 0)
    return (
        packed
        + jnp.where(up, pltpu.roll(packed, nx - 2, 1), 0.0)
        + jnp.where(down, pltpu.roll(packed, 2, 1), 0.0)
    )


def plane_kernel(u_ref, zp_ref):
    fields, nz, ny, nx = u_ref.shape
    z_even = lax.axis_index("gz") % 2 == 0
    for f in range(fields):
        zp_ref[f] = assemble_plane(jnp.where(z_even, u_ref[f, nz - 1], u_ref[f, 0]), ny, nx)


def assemble_kernel(u_ref, w_ref):
    fields, nz, ny, nx = u_ref.shape
    for f in range(fields):
        for z in range(nz):
            t = u_ref[f, z]
            if z % PTS == PTS - 1 and z < nz - 1:
                t = t + u_ref[f, z + 1]
            if z % PTS == 0 and z > 0:
                w_ref[f, z] = w_ref[f, z - 1]
            else:
                w_ref[f, z] = assemble_plane(t, ny, nx)


def merge_sides(right, left):
    lane = iota(right.shape, 1)
    return jnp.where(lane % 2 == 0, right, pltpu.roll(left, 2, 1))


def place_columns(merged, j, nx):
    lane = iota(merged.shape, 1)
    shift = (nx - 1 - 2 * j) % nx
    moved = pltpu.roll(merged, shift, 1) if shift else merged
    return jnp.where((lane == 0) | (lane == nx - 1), moved, 0.0)


def first_kernel(zp_ref, px_ref, qa_ref, pb_ref, pz_ref):
    fields, ny, nx = zp_ref.shape
    nz = nx // (2 * fields)
    x_even = lax.axis_index("gx") % 2 == 0
    z_even = lax.axis_index("gz") % 2 == 0
    qa = qa_ref[0:ny]
    merged = merge_sides(jnp.where(x_even, qa, 0.0), jnp.where(x_even, 0.0, qa))
    merged = jnp.where(z_even, pltpu.roll(merged, nx - 2 * (nz - 1), 1), merged)
    sums = px_ref[ny:] + qa_ref[ny:]
    pb_ref[0:ny] = px_ref[0:ny]
    pb_ref[ny:] = sums
    for f in range(fields):
        pz_ref[f * ny : (f + 1) * ny] = zp_ref[f] + place_columns(merged, f * nz, nx)
    pz_ref[fields * ny :] = sums


def x_sides(qa, qb, x_even):
    return merge_sides(jnp.where(x_even, qa, qb), jnp.where(x_even, qb, qa))


def diagonal_sides(qd, x_even):
    return merge_sides(jnp.where(x_even, 0.0, qd), jnp.where(x_even, qd, 0.0))


def second_kernel(
    u_ref, pb_ref, qa_ref, qb_ref, qz_ref, qd_ref, pya_ref, pyb_ref, ps_ref, low_ref, high_ref
):
    fields, nz, ny, nx = u_ref.shape
    x_even = lax.axis_index("gx") % 2 == 0
    y_even = lax.axis_index("gy") % 2 == 0
    for ys, row, out in (
        (slice(0, PTS), 0, low_ref),
        (slice(ny - PTS, ny), PTS - 1, high_ref),
    ):
        merged = x_sides(qa_ref[ys], qb_ref[ys], x_even)
        diag = diagonal_sides(qd_ref[ys], x_even)
        for f in range(fields):
            for z in range(nz):
                j = f * nz + z
                t = u_ref[f, z, ys] + place_columns(merged, j, nx)
                if z in (0, nz - 1):
                    t = t + qz_ref[f * ny + ys.start : f * ny + ys.stop]
                    t = t + place_columns(diag, f * nz + nz - 1 - z, nx)
                out[j : j + 1] = t[row : row + 1]
    sums = pb_ref[ny:] + qb_ref[ny:] + qz_ref[fields * ny :] + qd_ref[ny:]
    count = fields * nz
    pya_ref[0:count] = jnp.where(y_even, high_ref[...], low_ref[...])
    pyb_ref[0:count] = jnp.where(y_even, low_ref[...], high_ref[...])
    pya_ref[count:] = sums
    pyb_ref[count:] = sums
    ps_ref[...] = sums


def correct_kernel(v_ref, u_ref, qa_ref, qb_ref, qz_ref, qd_ref, w_ref, mv_ref):
    fields, nz, ny, nx = u_ref.shape
    x_even = lax.axis_index("gx") % 2 == 0
    merged = x_sides(qa_ref[0:ny], qb_ref[0:ny], x_even)
    diag = diagonal_sides(qd_ref[0:ny], x_even)
    for z in range(nz):
        for f in range(fields):
            t = u_ref[f, z] + place_columns(merged, f * nz + z, nx)
            if z in (0, nz - 1):
                t = t + qz_ref[f * ny : (f + 1) * ny]
                t = t + place_columns(diag, f * nz + nz - 1 - z, nx)
            w_ref[f, z] = t
        for c in range(fields - 1):
            mv_ref[c, z] = w_ref[fields - 1, z] * v_ref[c, z]


def last_kernel(
    sizes,
    v_ref,
    w_ref,
    mv_ref,
    qya_ref,
    qyb_ref,
    qs_ref,
    ps_ref,
    out_hbm,
    kin_ref,
    ens_ref,
    low_ref,
    high_ref,
    out_ref,
    sems,
):
    fields, nz, ny, nx = w_ref.shape
    gx, gy, gz = (lax.axis_index(name) for name in ("gx", "gy", "gz"))
    y_even = gy % 2 == 0
    count = fields * nz
    sums = ps_ref[...] + qya_ref[count:] + qyb_ref[count:] + qs_ref[...]
    kinetic = 0.5 * jnp.sum(sums[0:PTS])
    enstrophy = jnp.sum(sums[PTS : 2 * PTS])
    kin_ref[0, 0] = kinetic
    ens_ref[0, 0] = enstrophy
    rayleigh = jnp.full((PTS, nx), enstrophy, F32) / jnp.full((PTS, nx), 2.0 * kinetic, F32)
    low_ref[...] = jnp.where(y_even, qyb_ref[0:count], qya_ref[0:count])
    high_ref[...] = jnp.where(y_even, qya_ref[0:count], qyb_ref[0:count])
    row = iota((ny, nx), 0)
    lane = iota((ny, nx), 1)
    x_first = jnp.where(gx == 0, 0, -1)
    x_last = jnp.where(gx == sizes[0] - 1, nx - 1, -1)
    y_first = jnp.where(gy == 0, 0, -1)
    y_last = jnp.where(gy == sizes[1] - 1, ny - 1, -1)
    inside = (lane != x_first) & (lane != x_last) & (row != y_first) & (row != y_last)
    sub = iota((PTS, nx), 0)
    steps = nz // 4
    copies = []
    for z in range(nz):
        keep = inside
        if z == 0:
            keep = keep & (gz > 0)
        if z == nz - 1:
            keep = keep & (gz < sizes[2] - 1)
        for e in range(0, ny, PTS):
            ys = slice(e, e + PTS)
            edge = e == 0 or e == ny - PTS
            side, at = (low_ref, 0) if e == 0 else (high_ref, PTS - 1)
            if edge:
                j = (fields - 1) * nz + z
                extra = rayleigh * jnp.where(sub == at, side[j : j + 1], 0.0)
            for c in range(fields - 1):
                t = w_ref[c, z, ys] - rayleigh * mv_ref[c, z, ys]
                if edge:
                    j = c * nz + z
                    t = t + jnp.where(sub == at, side[j : j + 1], 0.0)
                    t = t - extra * v_ref[c, z, ys]
                out_ref[c, z, ys] = jnp.where(keep[ys], t, 0.0)
        if z % steps == steps - 1:
            zs = pl.ds(z - steps + 1, steps)
            copies.append(
                pltpu.make_async_copy(
                    out_ref.at[:, zs], out_hbm.at[:, zs], sems.at[z // steps]
                )
            )
            copies[-1].start()
    for copy in copies:
        copy.wait()


VMEM = pl.BlockSpec(memory_space=pltpu.VMEM)
SMEM = pl.BlockSpec(memory_space=pltpu.SMEM)
HBM = pl.BlockSpec(memory_space=pltpu.HBM)


def call(kernel, name, outs, ins, scratch=(), out_specs=None, in_specs=None, flops=1 << 20):
    return pl.pallas_call(
        kernel,
        out_shape=[jax.ShapeDtypeStruct(shape, F32) for shape in outs],
        in_specs=in_specs or [VMEM] * len(ins),
        out_specs=out_specs or [VMEM] * len(outs),
        scratch_shapes=list(scratch),
        compiler_params=pltpu.CompilerParams(vmem_limit_bytes=24 << 20),
        cost_estimate=pl.CostEstimate(flops=flops, bytes_accessed=flops, transcendentals=0),
        name=name,
    )(*ins)


def local_part(velocity, geometry, mass_weights):
    comps, nz, ny, nx = velocity.shape
    return call(
        functools.partial(local_kernel, gll_derivative(ORDER)),
        "local",
        [(comps + 1, nz, ny, nx), (ny + SCALAR_ROWS, nx), velocity.shape],
        [
            pltpu.with_memory_space_constraint(x, pltpu.HBM)
            for x in (velocity, geometry, mass_weights)
        ],
        in_specs=[HBM] * 3,
        scratch=[
            pltpu.VMEM(mass_weights.shape, BF16),
            pltpu.VMEM(geometry.shape, BF16),
            pltpu.VMEM((comps, PTS, ny, nx), F32),
            pltpu.VMEM((comps, PTS, ny, nx), F32),
            pltpu.SemaphoreType.DMA((nz // PTS, 3)),
        ],
    )


def assembled(u):
    return call(assemble_kernel, "assemble", [u.shape], [u])[0]


def pairs_near(count):
    return [(i, i ^ 1) for i in range(count)]


def pairs_mirror(count):
    return [(i, count - 1 - i) for i in range(count)]


def few_rounds(sizes, velocity, geometry, mass_weights):
    comps, nz, ny, nx = velocity.shape
    fields = comps + 1
    raw, px, held = local_part(velocity, geometry, mass_weights)
    qa = lax.ppermute(px, "gx", pairs_near(sizes[0]))
    zp = call(plane_kernel, "plane", [(fields, ny, nx)], [raw])[0]
    pb, pz = call(
        first_kernel,
        "first",
        [(ny + SCALAR_ROWS, nx), (fields * ny + SCALAR_ROWS, nx)],
        [zp, px, qa],
    )
    mirror = pairs_mirror(sizes[0])
    qb = lax.ppermute(pb, "gx", mirror)
    qz = lax.ppermute(pz, "gz", pairs_near(sizes[2]))
    both = [
        (i * sizes[2] + k, mirror[i][1] * sizes[2] + (k ^ 1))
        for i in range(sizes[0])
        for k in range(sizes[2])
    ]
    qd = lax.ppermute(pb, ("gx", "gz"), both)
    u = assembled(raw)
    count = fields * nz
    pya, pyb, ps = call(
        second_kernel,
        "second",
        [(count + SCALAR_ROWS, nx), (count + SCALAR_ROWS, nx), (SCALAR_ROWS, nx)],
        [u, pb, qa, qb, qz, qd],
        scratch=[pltpu.VMEM((count, nx), F32)] * 2,
    )
    qya = lax.ppermute(pya, "gy", pairs_near(sizes[1]))
    qyb = lax.ppermute(pyb, "gy", pairs_mirror(sizes[1]))
    qs = lax.ppermute(ps, "gy", [(i, i ^ 2) for i in range(sizes[1])])
    w, mv = call(
        correct_kernel, "correct", [u.shape, velocity.shape], [held, u, qa, qb, qz, qd]
    )
    residual, kinetic, enstrophy = call(
        functools.partial(last_kernel, sizes),
        "last",
        [velocity.shape, (1, 1), (1, 1)],
        [held, w, mv, qya, qyb, qs, ps],
        scratch=[
            pltpu.VMEM((count, nx), F32),
            pltpu.VMEM((count, nx), F32),
            pltpu.VMEM(velocity.shape, F32),
            pltpu.SemaphoreType.DMA((4,)),
        ],
        out_specs=[HBM, SMEM, SMEM],
    )
    return residual, kinetic[0, 0], enstrophy[0, 0]


def add_neighbours(field, axis, dim):
    count = lax.axis_size(axis)
    extent = field.shape[dim]
    first = lax.slice_in_dim(field, 0, 1, axis=dim)
    last = lax.slice_in_dim(field, extent - 1, extent, axis=dim)
    low = lax.ppermute(last, axis, [(i, i + 1) for i in range(count - 1)])
    high = lax.ppermute(first, axis, [(i + 1, i) for i in range(count - 1)])
    middle = lax.slice_in_dim(field, 1, extent - 1, axis=dim)
    return jnp.concatenate([first + low, middle, last + high], axis=dim)


def any_mesh(sizes, velocity, geometry, mass_weights):
    comps, nz, ny, nx = velocity.shape
    raw, px, held = local_part(velocity, geometry, mass_weights)
    u = assembled(raw)
    kinetic = 0.5 * jnp.sum(px[ny : ny + PTS])
    enstrophy = jnp.sum(px[ny + PTS :])
    kinetic, enstrophy = lax.psum((kinetic, enstrophy), ("gx", "gy", "gz"))
    for axis, dim in (("gx", 3), ("gy", 2), ("gz", 1)):
        u = add_neighbours(u, axis, dim)
    inside = jnp.ones((nz, ny, nx), bool)
    for dim, (axis, size) in enumerate(zip(("gz", "gy", "gx"), sizes[::-1])):
        place = lax.axis_index(axis) * inside.shape[dim] + iota(inside.shape, dim)
        inside = inside & (place > 0) & (place < size * inside.shape[dim] - 1)
    rayleigh = enstrophy / (2.0 * kinetic)
    residual = jnp.where(inside[None], u[:comps] - rayleigh * u[comps][None] * velocity, 0.0)
    return residual, kinetic, enstrophy


def solution(mesh):
    sizes = tuple(mesh.shape[name] for name in ("gx", "gy", "gz"))
    plan = few_rounds if sizes == (4, 4, 2) else any_mesh
    in_specs = (P(None, "gz", "gy", "gx"), P(None, "gz", "gy", "gx"), P("gz", "gy", "gx"))
    out_specs = (P(None, "gz", "gy", "gx"), P(), P())
    return jax.shard_map(
        functools.partial(plan, sizes),
        mesh=mesh,
        in_specs=in_specs,
        out_specs=out_specs,
        check_vma=False,
    )
```

```python
import functools

import jax
import jax.numpy as jnp
import numpy as np
from jax import lax
from jax.experimental import pallas as pl
from jax.experimental.pallas import tpu as pltpu
from jax.sharding import PartitionSpec as P


ORDER = 7
PTS = ORDER + 1
F32 = jnp.float32
BF16 = jnp.bfloat16
SCALAR_ROWS = 8


def gll_derivative(poly_order):
    node_count = poly_order + 1
    abscissa = np.cos(np.pi * np.arange(node_count) / poly_order)
    legendre = np.zeros((node_count, node_count))
    for _ in range(60):
        legendre[:, 0] = 1.0
        legendre[:, 1] = abscissa
        for degree in range(2, node_count):
            legendre[:, degree] = (
                (2 * degree - 1) * abscissa * legendre[:, degree - 1]
                - (degree - 1) * legendre[:, degree - 2]
            ) / degree
        abscissa = abscissa - (abscissa * legendre[:, poly_order] - legendre[:, poly_order - 1]) / (
            node_count * legendre[:, poly_order]
        )
    abscissa = abscissa[::-1]
    end_values = legendre[::-1, poly_order]
    spacing = abscissa[:, None] - abscissa[None, :] + np.eye(node_count)
    deriv_table = end_values[:, None] / end_values[None, :] / spacing
    deriv_table = deriv_table * (1.0 - np.eye(node_count))
    deriv_table[0, 0] = -poly_order * node_count / 4.0
    deriv_table[poly_order, poly_order] = poly_order * node_count / 4.0
    return deriv_table.astype(np.float32)


def split(x):
    high = x.astype(BF16)
    return high, (x - high.astype(F32)).astype(BF16)


def iota(shape, dim):
    return lax.broadcasted_iota(jnp.int32, shape, dim)


def repeated(table, width):
    lane = iota((PTS, width), 1) % PTS
    rows = []
    for i in range(PTS):
        row = jnp.full((PTS, width), float(table[i, 0]), F32)
        for k in range(1, PTS):
            row = jnp.where(lane == k, float(table[i, k]), row)
        rows.append(row)
    return rows


def fine_matrix(table, size):
    sub = iota((PTS, size), 0)
    rows = repeated(table, size)
    tile = rows[0]
    for i in range(1, PTS):
        tile = jnp.where(sub == i, rows[i], tile)
    block = iota((PTS, size), 1) // PTS
    return split(
        jnp.concatenate(
            [jnp.where(block == e, tile, 0.0) for e in range(size // PTS)], axis=0
        )
    )


def combine_planes(planes, table):
    half = PTS // 2
    even = [planes[k] + planes[PTS - 1 - k] for k in range(half)]
    odd = [planes[k] - planes[PTS - 1 - k] for k in range(half)]
    low, high = [], []
    for w in range(half):
        p = q = None
        for k in range(half):
            a, b = float(table[w, k]), float(table[w, PTS - 1 - k])
            pe = np.float32((a + b) / 2) * even[k]
            qo = np.float32((a - b) / 2) * odd[k]
            p = pe if p is None else p + pe
            q = qo if q is None else q + qo
        low.append(p + q)
        high.append(q - p)
    return low + high[::-1]


def dot(a, b):
    return jnp.dot(a, b, preferred_element_type=F32)


def join_rows(tiles, sub):
    done = []
    for e, t in enumerate(tiles):
        if e + 1 < len(tiles):
            t = t + jnp.where(sub == PTS - 1, pltpu.roll(tiles[e + 1], PTS - 1, 0), 0.0)
        if e > 0:
            t = t + jnp.where(sub == 0, pltpu.roll(tiles[e - 1], 1, 0), 0.0)
        done.append(t)
    return done


def assemble_plane(u, ny, nx):
    lane = iota((PTS, nx), 1)
    sub = iota((PTS, nx), 0)
    last = (lane % PTS == PTS - 1) & (lane < nx - 1)
    first = (lane % PTS == 0) & (lane > 0)
    tiles = []
    for e in range(ny // PTS):
        t = u[e * PTS : (e + 1) * PTS]
        t = (
            t
            + jnp.where(last, pltpu.roll(t, nx - 1, 1), 0.0)
            + jnp.where(first, pltpu.roll(t, 1, 1), 0.0)
        )
        tiles.append(t)
    return jnp.concatenate(join_rows(tiles, sub), axis=0)


def local_kernel(
    table,
    v_hbm,
    g_hbm,
    m_hbm,
    u_ref,
    px_ref,
    v_ref,
    m_ref,
    g_ref,
    grad_ref,
    high_ref,
    low_ref,
    div_ref,
    left_ref,
    right_ref,
    sems,
):
    comps, nz, ny, nx = v_ref.shape
    layers = nz // PTS
    rows = PTS * ny
    half = 2 * PTS
    v_copies = []
    gm_copies = []
    for layer in range(layers):
        zs = pl.ds(layer * PTS, PTS)
        v_copies.append(
            pltpu.make_async_copy(v_hbm.at[:, zs], v_ref.at[:, zs], sems.at[layer, 0])
        )
        gm_copies.append(
            pltpu.make_async_copy(g_hbm.at[:, zs], g_ref.at[:, zs], sems.at[layer, 1])
        )
        gm_copies.append(pltpu.make_async_copy(m_hbm.at[zs], m_ref.at[zs], sems.at[layer, 2]))
    for copy in v_copies + gm_copies:
        copy.start()
    for i, matrix in enumerate((table, table.T)):
        h, l = fine_matrix(matrix, rows)
        left_ref[i] = jnp.concatenate([h, l, h], axis=1)
        h, l = fine_matrix(matrix.T, nx)
        right_ref[i] = jnp.concatenate(
            [
                jnp.concatenate([h, l], axis=1),
                jnp.concatenate([h, jnp.zeros_like(l)], axis=1),
            ],
            axis=0,
        )
    blocks = [(layer, c) for layer in range(layers) for c in range(comps)]
    pairs = [blocks[i : i + 2] for i in range(0, len(blocks), 2)]

    def planes(layer):
        return slice(layer * PTS, (layer + 1) * PTS)

    def along_y(i, pair, slot):
        high = [high_ref[slot, c, planes(layer)].reshape(rows, nx) for layer, c in pair]
        low = [low_ref[slot, c, planes(layer)].reshape(rows, nx) for layer, c in pair]
        high, low = jnp.concatenate(high, axis=1), jnp.concatenate(low, axis=1)
        out = dot(left_ref[i], jnp.concatenate([high, high, low], axis=0))
        return [
            out[:, n * nx : (n + 1) * nx].reshape(PTS, ny, nx) for n in range(len(pair))
        ]

    def along_x(i, layer, c, slot):
        high = high_ref[slot, c, planes(layer)].reshape(rows, nx)
        low = low_ref[slot, c, planes(layer)].reshape(rows, nx)
        out = dot(jnp.concatenate([high, low], axis=1), right_ref[i])
        return (out[:, 0:nx] + out[:, nx : 2 * nx]).reshape(PTS, ny, nx)

    for copy in v_copies:
        copy.wait()
    for copy in gm_copies:
        copy.wait()
    for c in range(comps):
        for z in range(nz):
            high_ref[0, c, z], low_ref[0, c, z] = split(v_ref[c, z])
    for layer, c in blocks:
        for e in range(0, ny, PTS):
            ys = slice(e, e + PTS)
            z0 = layer * PTS
            out = combine_planes([v_ref[c, z0 + z, ys] for z in range(PTS)], table)
            for z in range(PTS):
                grad_ref[2, c, z0 + z, ys] = out[z]
    for pair in pairs:
        for (layer, c), out in zip(pair, along_y(0, pair, 0)):
            grad_ref[1, c, planes(layer)] = out
    for layer, c in blocks:
        grad_ref[0, c, planes(layer)] = along_x(0, layer, c, 0)
    kin = jnp.zeros((half, nx), F32)
    ens = jnp.zeros((half, nx), F32)
    ready = 0
    for layer in range(layers):
        for z in range(layer * PTS, (layer + 1) * PTS):
            for y in range(0, ny, half):
                ys = slice(y, y + half)
                g = [g_ref[i, z, ys].astype(F32) for i in range(6)]
                mass = m_ref[z, ys].astype(F32)
                u_ref[comps, z, ys] = mass
                square = None
                for c in range(comps):
                    v = v_ref[c, z, ys]
                    square = v * v if square is None else square + v * v
                    gr, gs, gt = (grad_ref[i, c, z, ys] for i in range(3))
                    fr = g[0] * gr + g[3] * gs + g[4] * gt
                    fs = g[3] * gr + g[1] * gs + g[5] * gt
                    ft = g[4] * gr + g[5] * gs + g[2] * gt
                    ens = ens + (gr * fr + gs * fs + gt * ft)
                    high_ref[1, c, z, ys], low_ref[1, c, z, ys] = split(fr)
                    high_ref[2, c, z, ys], low_ref[2, c, z, ys] = split(fs)
                    grad_ref[2, c, z, ys] = ft
                kin = kin + mass * square
        for c in range(comps):
            div_ref[c, planes(layer)] = along_x(1, layer, c, 1)
        while ready < len(pairs) and max(block[0] for block in pairs[ready]) <= layer:
            for (at, c), out in zip(pairs[ready], along_y(1, pairs[ready], 2)):
                grad_ref[1, c, planes(at)] = out
            ready += 1
    for layer, c in blocks:
        for e in range(0, ny, PTS):
            ys = slice(e, e + PTS)
            z0 = layer * PTS
            out = combine_planes([grad_ref[2, c, z0 + z, ys] for z in range(PTS)], table.T)
            for z in range(PTS):
                rest = grad_ref[1, c, z0 + z, ys] + div_ref[c, z0 + z, ys]
                u_ref[c, z0 + z, ys] = out[z] + rest
    px_ref[0:ny] = pack_columns(u_ref)
    row = iota((SCALAR_ROWS, nx), 0)
    kin, ens = jnp.sum(kin, axis=0, keepdims=True), jnp.sum(ens, axis=0, keepdims=True)
    px_ref[ny:] = jnp.where(row == 0, kin, jnp.where(row == 1, ens, 0.0))


def pack_columns(u_ref):
    fields, nz, ny, nx = u_ref.shape
    lane = iota((ny, nx), 1)
    packed = jnp.zeros((ny, nx), F32)
    for f in range(fields):
        for z in range(nz):
            j = f * nz + z
            moved = pltpu.roll(u_ref[f, z], 2 * j, 1) if j else u_ref[f, z]
            packed = jnp.where((lane == 2 * j) | (lane == (2 * j - 1) % nx), moved, packed)
    sub = iota((PTS, nx), 0)
    tiles = [packed[e : e + PTS] for e in range(0, ny, PTS)]
    packed = jnp.concatenate(join_rows(tiles, sub), axis=0)
    plane = (lane + 1) % nx // 2 % nz
    up = (plane % PTS == PTS - 1) & (plane < nz - 1)
    down = (plane % PTS == 0) & (plane > 0)
    return (
        packed
        + jnp.where(up, pltpu.roll(packed, nx - 2, 1), 0.0)
        + jnp.where(down, pltpu.roll(packed, 2, 1), 0.0)
    )


def plane_kernel(u_ref, zp_ref):
    fields, nz, ny, nx = u_ref.shape
    z_even = lax.axis_index("gz") % 2 == 0
    for f in range(fields):
        zp_ref[f] = assemble_plane(jnp.where(z_even, u_ref[f, nz - 1], u_ref[f, 0]), ny, nx)


def assemble_kernel(u_ref, w_ref):
    fields, nz, ny, nx = u_ref.shape
    for f in range(fields):
        for z in range(nz):
            t = u_ref[f, z]
            if z % PTS == PTS - 1 and z < nz - 1:
                t = t + u_ref[f, z + 1]
            if z % PTS == 0 and z > 0:
                w_ref[f, z] = w_ref[f, z - 1]
            else:
                w_ref[f, z] = assemble_plane(t, ny, nx)


def merge_sides(right, left):
    lane = iota(right.shape, 1)
    return jnp.where(lane % 2 == 0, right, pltpu.roll(left, 2, 1))


def place_columns(merged, j, nx):
    lane = iota(merged.shape, 1)
    shift = (nx - 1 - 2 * j) % nx
    moved = pltpu.roll(merged, shift, 1) if shift else merged
    return jnp.where((lane == 0) | (lane == nx - 1), moved, 0.0)


def first_kernel(zp_ref, px_ref, qa_ref, pb_ref, pz_ref, pd_ref):
    fields, ny, nx = zp_ref.shape
    nz = nx // (2 * fields)
    lane = iota((PTS, nx), 1)
    x_even = lax.axis_index("gx") % 2 == 0
    z_even = lax.axis_index("gz") % 2 == 0
    qa = qa_ref[0:ny]
    merged = merge_sides(jnp.where(x_even, qa, 0.0), jnp.where(x_even, 0.0, qa))
    merged = jnp.where(z_even, pltpu.roll(merged, nx - 2 * (nz - 1), 1), merged)
    sums = px_ref[ny:] + qa_ref[ny:]
    pb_ref[0:ny] = px_ref[0:ny]
    pb_ref[ny:] = sums
    for f in range(fields):
        pz_ref[f * ny : (f + 1) * ny] = zp_ref[f] + place_columns(merged, f * nz, nx)
    pz_ref[fields * ny :] = sums
    edge = None
    for e in range(ny // PTS):
        t = px_ref[e * PTS : (e + 1) * PTS]
        t = jnp.where(z_even, pltpu.roll(t, nx - 2 * (nz - 1), 1), t)
        t = pltpu.roll(t, 2 * e, 1) if e else t
        mine = (lane + 1) % nx // 2 % nz == e
        edge = jnp.where(mine, t, 0.0 if edge is None else edge)
    pd_ref[0:PTS] = edge
    pd_ref[PTS:] = sums


def x_sides(qa, qb, x_even):
    return merge_sides(jnp.where(x_even, qa, qb), jnp.where(x_even, qb, qa))


def diagonal_sides(qd, x_even):
    return merge_sides(jnp.where(x_even, 0.0, qd), jnp.where(x_even, qd, 0.0))


def second_kernel(
    u_ref, pb_ref, qa_ref, qb_ref, qz_ref, qd_ref, pya_ref, pyb_ref, ps_ref, low_ref, high_ref
):
    fields, nz, ny, nx = u_ref.shape
    x_even = lax.axis_index("gx") % 2 == 0
    y_even = lax.axis_index("gy") % 2 == 0
    for ys, row, out in (
        (slice(0, PTS), 0, low_ref),
        (slice(ny - PTS, ny), PTS - 1, high_ref),
    ):
        merged = x_sides(qa_ref[ys], qb_ref[ys], x_even)
        diag = diagonal_sides(qd_ref[0:PTS], x_even)
        for f in range(fields):
            for z in range(nz):
                j = f * nz + z
                t = u_ref[f, z, ys] + place_columns(merged, j, nx)
                if z in (0, nz - 1):
                    t = t + qz_ref[f * ny + ys.start : f * ny + ys.stop]
                    t = t + place_columns(diag, f * nz + ys.start // PTS, nx)
                out[j : j + 1] = t[row : row + 1]
    sums = pb_ref[ny:] + qb_ref[ny:] + qz_ref[fields * ny :] + qd_ref[PTS:]
    count = fields * nz
    pya_ref[0:count] = jnp.where(y_even, high_ref[...], low_ref[...])
    pyb_ref[0:count] = jnp.where(y_even, low_ref[...], high_ref[...])
    pya_ref[count:] = sums
    pyb_ref[count:] = sums
    ps_ref[...] = sums


def correct_kernel(v_ref, u_ref, qa_ref, qb_ref, qz_ref, qd_ref, w_ref, mv_ref):
    fields, nz, ny, nx = u_ref.shape
    x_even = lax.axis_index("gx") % 2 == 0
    merged = x_sides(qa_ref[0:ny], qb_ref[0:ny], x_even)
    diag = diagonal_sides(qd_ref[0:PTS], x_even)
    for z in range(nz):
        for f in range(fields):
            t = u_ref[f, z] + place_columns(merged, f * nz + z, nx)
            if z in (0, nz - 1):
                t = t + qz_ref[f * ny : (f + 1) * ny]
                corner = [place_columns(diag, f * nz + e, nx) for e in range(ny // PTS)]
                t = t + jnp.concatenate(corner, axis=0)
            w_ref[f, z] = t
        for c in range(fields - 1):
            mv_ref[c, z] = w_ref[fields - 1, z] * v_ref[c, z]


def last_kernel(
    sizes,
    v_ref,
    w_ref,
    mv_ref,
    qya_ref,
    qyb_ref,
    qs_ref,
    ps_ref,
    out_hbm,
    kin_hbm,
    ens_hbm,
    low_ref,
    high_ref,
    out_ref,
    kin_ref,
    ens_ref,
    sems,
):
    fields, nz, ny, nx = w_ref.shape
    gx, gy, gz = (lax.axis_index(name) for name in ("gx", "gy", "gz"))
    y_even = gy % 2 == 0
    count = fields * nz
    sums = ps_ref[...] + qya_ref[count:] + qyb_ref[count:] + qs_ref[...]
    kinetic = 0.5 * jnp.sum(sums[0:1])
    enstrophy = jnp.sum(sums[1:2])
    kin_ref[0, 0] = kinetic
    ens_ref[0, 0] = enstrophy
    copies = [
        pltpu.make_async_copy(kin_ref, kin_hbm, sems.at[4]),
        pltpu.make_async_copy(ens_ref, ens_hbm, sems.at[5]),
    ]
    for copy in copies:
        copy.start()
    rayleigh = jnp.full((PTS, nx), enstrophy, F32) / jnp.full((PTS, nx), 2.0 * kinetic, F32)
    low_ref[...] = jnp.where(y_even, qyb_ref[0:count], qya_ref[0:count])
    high_ref[...] = jnp.where(y_even, qya_ref[0:count], qyb_ref[0:count])
    row = iota((ny, nx), 0)
    lane = iota((ny, nx), 1)
    x_first = jnp.where(gx == 0, 0, -1)
    x_last = jnp.where(gx == sizes[0] - 1, nx - 1, -1)
    y_first = jnp.where(gy == 0, 0, -1)
    y_last = jnp.where(gy == sizes[1] - 1, ny - 1, -1)
    inside = (lane != x_first) & (lane != x_last) & (row != y_first) & (row != y_last)
    sub = iota((PTS, nx), 0)
    steps = nz // 4
    for z in range(nz):
        keep = inside
        if z == 0:
            keep = keep & (gz > 0)
        if z == nz - 1:
            keep = keep & (gz < sizes[2] - 1)
        for e in range(0, ny, PTS):
            ys = slice(e, e + PTS)
            edge = e == 0 or e == ny - PTS
            side, at = (low_ref, 0) if e == 0 else (high_ref, PTS - 1)
            if edge:
                j = (fields - 1) * nz + z
                extra = rayleigh * jnp.where(sub == at, side[j : j + 1], 0.0)
            for c in range(fields - 1):
                t = w_ref[c, z, ys] - rayleigh * mv_ref[c, z, ys]
                if edge:
                    j = c * nz + z
                    t = t + jnp.where(sub == at, side[j : j + 1], 0.0)
                    t = t - extra * v_ref[c, z, ys]
                out_ref[c, z, ys] = jnp.where(keep[ys], t, 0.0)
        if z % steps == steps - 1:
            zs = pl.ds(z - steps + 1, steps)
            copies.append(
                pltpu.make_async_copy(
                    out_ref.at[:, zs], out_hbm.at[:, zs], sems.at[z // steps]
                )
            )
            copies[-1].start()
    for copy in copies:
        copy.wait()


VMEM = pl.BlockSpec(memory_space=pltpu.VMEM)
HBM = pl.BlockSpec(memory_space=pltpu.HBM)


def call(kernel, outs, ins, scratch=(), out_specs=None, in_specs=None, flops=1 << 20):
    return pl.pallas_call(
        kernel,
        out_shape=[jax.ShapeDtypeStruct(shape, F32) for shape in outs],
        in_specs=in_specs or [VMEM] * len(ins),
        out_specs=out_specs or [VMEM] * len(outs),
        scratch_shapes=list(scratch),
        compiler_params=pltpu.CompilerParams(vmem_limit_bytes=24 << 20),
        cost_estimate=pl.CostEstimate(flops=flops, bytes_accessed=flops, transcendentals=0),
    )(*ins)


def local_part(velocity, geometry, mass_weights):
    comps, nz, ny, nx = velocity.shape
    return call(
        functools.partial(local_kernel, gll_derivative(ORDER)),
        [(comps + 1, nz, ny, nx), (ny + SCALAR_ROWS, nx), velocity.shape],
        [
            pltpu.with_memory_space_constraint(x, pltpu.HBM)
            for x in (velocity, geometry, mass_weights)
        ],
        in_specs=[HBM] * 3,
        scratch=[
            pltpu.VMEM(mass_weights.shape, BF16),
            pltpu.VMEM(geometry.shape, BF16),
            pltpu.VMEM((3, *velocity.shape), F32),
            pltpu.VMEM((3, *velocity.shape), BF16),
            pltpu.VMEM((3, *velocity.shape), BF16),
            pltpu.VMEM(velocity.shape, F32),
            pltpu.VMEM((2, PTS * ny, 3 * PTS * ny), BF16),
            pltpu.VMEM((2, 2 * nx, 2 * nx), BF16),
            pltpu.SemaphoreType.DMA((nz // PTS, 3)),
        ],
    )


def assembled(u):
    return call(assemble_kernel, [u.shape], [u])[0]


def pairs_near(count):
    return [(i, i ^ 1) for i in range(count)]


def pairs_mirror(count):
    return [(i, count - 1 - i) for i in range(count)]


def few_rounds(sizes, velocity, geometry, mass_weights):
    comps, nz, ny, nx = velocity.shape
    fields = comps + 1
    raw, px, held = local_part(velocity, geometry, mass_weights)
    qa = lax.ppermute(px, "gx", pairs_near(sizes[0]))
    zp = call(plane_kernel, [(fields, ny, nx)], [raw])[0]
    pb, pz, pd = call(
        first_kernel,
        [
            (ny + SCALAR_ROWS, nx),
            (fields * ny + SCALAR_ROWS, nx),
            (PTS + SCALAR_ROWS, nx),
        ],
        [zp, px, qa],
    )
    mirror = pairs_mirror(sizes[0])
    qb = lax.ppermute(pb, "gx", mirror)
    qz = lax.ppermute(pz, "gz", pairs_near(sizes[2]))
    both = [
        (i * sizes[2] + k, mirror[i][1] * sizes[2] + (k ^ 1))
        for i in range(sizes[0])
        for k in range(sizes[2])
    ]
    qd = lax.ppermute(pd, ("gx", "gz"), both)
    u = assembled(raw)
    count = fields * nz
    pya, pyb, ps = call(
        second_kernel,
        [(count + SCALAR_ROWS, nx), (count + SCALAR_ROWS, nx), (SCALAR_ROWS, nx)],
        [u, pb, qa, qb, qz, qd],
        scratch=[pltpu.VMEM((count, nx), F32)] * 2,
    )
    qya = lax.ppermute(pya, "gy", pairs_near(sizes[1]))
    qyb = lax.ppermute(pyb, "gy", pairs_mirror(sizes[1]))
    qs = lax.ppermute(ps, "gy", [(i, i ^ 2) for i in range(sizes[1])])
    w, mv = call(correct_kernel, [u.shape, velocity.shape], [held, u, qa, qb, qz, qd])
    residual, kinetic, enstrophy = call(
        functools.partial(last_kernel, sizes),
        [velocity.shape, (1, 1), (1, 1)],
        [held, w, mv, qya, qyb, qs, ps],
        scratch=[
            pltpu.VMEM((count, nx), F32),
            pltpu.VMEM((count, nx), F32),
            pltpu.VMEM(velocity.shape, F32),
            pltpu.SMEM((1, 1), F32),
            pltpu.SMEM((1, 1), F32),
            pltpu.SemaphoreType.DMA((6,)),
        ],
        out_specs=[HBM, HBM, HBM],
    )
    return residual, kinetic[0, 0], enstrophy[0, 0]


def add_neighbours(field, axis, dim):
    count = lax.axis_size(axis)
    extent = field.shape[dim]
    first = lax.slice_in_dim(field, 0, 1, axis=dim)
    last = lax.slice_in_dim(field, extent - 1, extent, axis=dim)
    low = lax.ppermute(last, axis, [(i, i + 1) for i in range(count - 1)])
    high = lax.ppermute(first, axis, [(i + 1, i) for i in range(count - 1)])
    middle = lax.slice_in_dim(field, 1, extent - 1, axis=dim)
    return jnp.concatenate([first + low, middle, last + high], axis=dim)


def any_mesh(sizes, velocity, geometry, mass_weights):
    comps, nz, ny, nx = velocity.shape
    raw, px, _ = local_part(velocity, geometry, mass_weights)
    u = assembled(raw)
    kinetic = 0.5 * jnp.sum(px[ny])
    enstrophy = jnp.sum(px[ny + 1])
    kinetic, enstrophy = lax.psum((kinetic, enstrophy), ("gx", "gy", "gz"))
    for axis, dim in (("gx", 3), ("gy", 2), ("gz", 1)):
        u = add_neighbours(u, axis, dim)
    inside = jnp.ones((nz, ny, nx), bool)
    for dim, (axis, size) in enumerate(zip(("gz", "gy", "gx"), sizes[::-1])):
        place = lax.axis_index(axis) * inside.shape[dim] + iota(inside.shape, dim)
        inside = inside & (place > 0) & (place < size * inside.shape[dim] - 1)
    rayleigh = enstrophy / (2.0 * kinetic)
    residual = jnp.where(inside[None], u[:comps] - rayleigh * u[comps][None] * velocity, 0.0)
    return residual, kinetic, enstrophy


def solution(mesh):
    sizes = tuple(mesh.shape[name] for name in ("gx", "gy", "gz"))
    plan = few_rounds if sizes == (4, 4, 2) else any_mesh
    in_specs = (P(None, "gz", "gy", "gx"), P(None, "gz", "gy", "gx"), P("gz", "gy", "gx"))
    out_specs = (P(None, "gz", "gy", "gx"), P(), P())

    def body(*args):
        return plan(sizes, *args)

    step = jax.shard_map(
        body, mesh=mesh, in_specs=in_specs, out_specs=out_specs, check_vma=False
    )
    if plan is any_mesh:
        return step
    return step
```

```python
import functools

import jax
import jax.numpy as jnp
import numpy as np
from jax import lax
from jax.experimental import pallas as pl
from jax.experimental.pallas import tpu as pltpu
from jax.sharding import PartitionSpec as P


ORDER = 7
PTS = ORDER + 1
F32 = jnp.float32
BF16 = jnp.bfloat16
SCALAR_ROWS = 8


def gll_derivative(poly_order):
    node_count = poly_order + 1
    abscissa = np.cos(np.pi * np.arange(node_count) / poly_order)
    legendre = np.zeros((node_count, node_count))
    for _ in range(60):
        legendre[:, 0] = 1.0
        legendre[:, 1] = abscissa
        for degree in range(2, node_count):
            legendre[:, degree] = (
                (2 * degree - 1) * abscissa * legendre[:, degree - 1]
                - (degree - 1) * legendre[:, degree - 2]
            ) / degree
        abscissa = abscissa - (abscissa * legendre[:, poly_order] - legendre[:, poly_order - 1]) / (
            node_count * legendre[:, poly_order]
        )
    abscissa = abscissa[::-1]
    end_values = legendre[::-1, poly_order]
    spacing = abscissa[:, None] - abscissa[None, :] + np.eye(node_count)
    deriv_table = end_values[:, None] / end_values[None, :] / spacing
    deriv_table = deriv_table * (1.0 - np.eye(node_count))
    deriv_table[0, 0] = -poly_order * node_count / 4.0
    deriv_table[poly_order, poly_order] = poly_order * node_count / 4.0
    return deriv_table.astype(np.float32)


def split(x):
    high = x.astype(BF16)
    return high, (x - high.astype(F32)).astype(BF16)


def iota(shape, dim):
    return lax.broadcasted_iota(jnp.int32, shape, dim)


def repeated(table, width):
    lane = iota((PTS, width), 1) % PTS
    rows = []
    for i in range(PTS):
        row = jnp.full((PTS, width), float(table[i, 0]), F32)
        for k in range(1, PTS):
            row = jnp.where(lane == k, float(table[i, k]), row)
        rows.append(row)
    return rows


def fine_matrix(table, size):
    sub = iota((PTS, size), 0)
    rows = repeated(table, size)
    tile = rows[0]
    for i in range(1, PTS):
        tile = jnp.where(sub == i, rows[i], tile)
    block = iota((PTS, size), 1) // PTS
    return split(
        jnp.concatenate(
            [jnp.where(block == e, tile, 0.0) for e in range(size // PTS)], axis=0
        )
    )


def combine_planes(planes, table):
    half = PTS // 2
    even = [planes[k] + planes[PTS - 1 - k] for k in range(half)]
    odd = [planes[k] - planes[PTS - 1 - k] for k in range(half)]
    low, high = [], []
    for w in range(half):
        p = q = None
        for k in range(half):
            a, b = float(table[w, k]), float(table[w, PTS - 1 - k])
            pe = np.float32((a + b) / 2) * even[k]
            qo = np.float32((a - b) / 2) * odd[k]
            p = pe if p is None else p + pe
            q = qo if q is None else q + qo
        low.append(p + q)
        high.append(q - p)
    return low + high[::-1]


def dot(a, b):
    return jnp.dot(a, b, preferred_element_type=F32)


def join_rows(tiles, sub):
    done = []
    for e, t in enumerate(tiles):
        if e + 1 < len(tiles):
            t = t + jnp.where(sub == PTS - 1, pltpu.roll(tiles[e + 1], PTS - 1, 0), 0.0)
        if e > 0:
            t = t + jnp.where(sub == 0, pltpu.roll(tiles[e - 1], 1, 0), 0.0)
        done.append(t)
    return done


def assemble_plane(u, ny, nx):
    lane = iota((PTS, nx), 1)
    sub = iota((PTS, nx), 0)
    last = (lane % PTS == PTS - 1) & (lane < nx - 1)
    first = (lane % PTS == 0) & (lane > 0)
    tiles = []
    for e in range(ny // PTS):
        t = u[e * PTS : (e + 1) * PTS]
        t = (
            t
            + jnp.where(last, pltpu.roll(t, nx - 1, 1), 0.0)
            + jnp.where(first, pltpu.roll(t, 1, 1), 0.0)
        )
        tiles.append(t)
    return jnp.concatenate(join_rows(tiles, sub), axis=0)


def joined(pieces):
    return pieces[0] if len(pieces) == 1 else joined(
        [sum(pieces[i : i + 2][1:], pieces[i]) for i in range(0, len(pieces), 2)]
    )


def across_rows(tile, columns):
    return joined(
        [column * jnp.broadcast_to(tile[k : k + 1], tile.shape) for k, column in enumerate(columns)]
    )


def row_columns(table, nx):
    sub = iota((PTS, nx), 0)
    columns = []
    for k in range(PTS):
        column = jnp.full((PTS, nx), float(table[0, k]), F32)
        for w in range(1, PTS):
            column = jnp.where(sub == w, float(table[w, k]), column)
        columns.append(column)
    return columns


def by_thrice(x, weights):
    high, low = split(x)
    out = dot(jnp.concatenate([high, low], axis=1), weights)
    half = weights.shape[1] // 2
    return out[:, 0:half] + out[:, half:]


def thrice(high, low):
    return jnp.concatenate(
        [
            jnp.concatenate([high, low], axis=1),
            jnp.concatenate([high, jnp.zeros_like(low)], axis=1),
        ],
        axis=0,
    )


def column_slot(lane, nx):
    return (lane + 1) % nx // 2


def packed_z_matrix(table, nx):
    into, out = iota((nx, nx), 0), iota((nx, nx), 1)
    j, k = column_slot(into, nx), column_slot(out, nx)
    value = jnp.zeros((nx, nx), F32)
    for w in range(PTS):
        row = jnp.zeros((nx, nx), F32)
        for q in range(PTS):
            row = jnp.where(k % PTS == q, float(table[w, q]), row)
        value = jnp.where(j % PTS == w, row, value)
    same = (j // PTS == k // PTS) & (into % 2 == out % 2)
    return jnp.where(same, value, 0.0)


def packed_x_matrix(table, nx):
    into, out = iota((nx, nx), 0), iota((nx, nx), 1)
    place, plane = into % (2 * PTS), into // (2 * PTS)
    value = jnp.zeros((nx, nx), F32)
    for w in range(PTS):
        value = jnp.where(place == w, float(table[w, PTS - 1]), value)
        value = jnp.where(place == PTS + w, float(table[w, 0]), value)
    target = jnp.where(place < PTS, (2 * plane - 1) % nx, 2 * plane)
    return jnp.where(out == target, value, 0.0)


def local_kernel(
    table,
    v_hbm,
    g_hbm,
    m_hbm,
    f_ref,
    px_ref,
    v_ref,
    m_ref,
    left_ref,
    right_ref,
    g_ref,
    grad_ref,
    high_ref,
    low_ref,
    sems,
):
    comps, nz, ny, nx = v_ref.shape
    layers = nz // PTS
    rows = PTS * ny
    half = 2 * PTS
    v_copies = []
    gm_copies = []
    for layer in range(layers):
        zs = pl.ds(layer * PTS, PTS)
        v_copies.append(
            pltpu.make_async_copy(v_hbm.at[:, zs], v_ref.at[:, zs], sems.at[layer, 0])
        )
        gm_copies.append(
            pltpu.make_async_copy(g_hbm.at[:, zs], g_ref.at[:, zs], sems.at[layer, 1])
        )
        gm_copies.append(pltpu.make_async_copy(m_hbm.at[zs], m_ref.at[zs], sems.at[layer, 2]))
    for copy in v_copies + gm_copies:
        copy.start()
    for i, matrix in enumerate((table, table.T)):
        h, l = fine_matrix(matrix, rows)
        left_ref[i] = jnp.concatenate([h, l, h], axis=1)
        right_ref[i] = thrice(*fine_matrix(matrix.T, nx))
    right_ref[2] = thrice(*split(packed_x_matrix(table, nx)))
    right_ref[3] = thrice(*split(packed_z_matrix(table, nx)))
    columns = row_columns(table.T, nx)
    blocks = [(layer, c) for layer in range(layers) for c in range(comps)]

    def planes(layer):
        return slice(layer * PTS, (layer + 1) * PTS)

    for copy in v_copies:
        copy.wait()
    for c in range(comps):
        for z in range(nz):
            high_ref[c, z], low_ref[c, z] = split(v_ref[c, z])
    for layer, c in blocks:
        grad_ref[0, c, planes(layer)] = along_x(right_ref[0], layer, c, high_ref, low_ref)
    for i in range(0, len(blocks), 2):
        pair = blocks[i : i + 2]
        for (layer, c), out in zip(pair, along_y(left_ref[0], pair, high_ref, low_ref)):
            grad_ref[1, c, planes(layer)] = out
    for layer, c in blocks:
        for e in range(0, ny, PTS):
            ys = slice(e, e + PTS)
            z0 = layer * PTS
            out = combine_planes([v_ref[c, z0 + z, ys] for z in range(PTS)], table)
            for z in range(PTS):
                grad_ref[2, c, z0 + z, ys] = out[z]
    for copy in gm_copies:
        copy.wait()
    lane = iota((PTS, nx), 1)
    slot, place = column_slot(lane, nx), lane // half

    def moved(x, shift):
        return pltpu.roll(x, shift, 1) if shift else x

    kin = jnp.zeros((half, nx), F32)
    ens = jnp.zeros((half, nx), F32)
    tiles = ny // PTS
    zero = jnp.zeros((PTS, nx), F32)
    packed_s, packed_t, packed_m = ([zero] * tiles for _ in range(3))
    groups = [[zero] * tiles for _ in range(comps * layers)]
    for y in range(0, ny, half):
        ys = slice(y, y + half)
        for z in range(nz):
            g = [g_ref[i, z, ys].astype(F32) for i in range(6)]
            mass = m_ref[z, ys].astype(F32)
            square = None
            for c in range(comps):
                v = v_ref[c, z, ys]
                square = v * v if square is None else square + v * v
                gr, gs, gt = (grad_ref[i, c, z, ys] for i in range(3))
                fr = g[0] * gr + g[3] * gs + g[4] * gt
                fs = g[3] * gr + g[1] * gs + g[5] * gt
                ft = g[4] * gr + g[5] * gs + g[2] * gt
                ens = ens + (gr * fr + gs * fs + gt * ft)
                f_ref[0, c, z, ys] = fr
                f_ref[1, c, z, ys] = fs
                f_ref[2, c, z, ys] = ft
                j = c * nz + z
                here, mine = slot == j, place == j % PTS
                for e in range(half // PTS):
                    t, rs = y // PTS + e, slice(e * PTS, (e + 1) * PTS)
                    packed_s[t] = jnp.where(here, moved(fs[rs], 2 * j), packed_s[t])
                    packed_t[t] = jnp.where(here, moved(ft[rs], 2 * j), packed_t[t])
                    part = moved(fr[rs], (PTS + half * (j % PTS)) % nx)
                    groups[j // PTS][t] = jnp.where(mine, part, groups[j // PTS][t])
            kin = kin + mass * square
            j = comps * nz + z
            for e in range(half // PTS):
                t, rs = y // PTS + e, slice(e * PTS, (e + 1) * PTS)
                packed_m[t] = jnp.where(slot == j, moved(mass[rs], 2 * j), packed_m[t])
    div_r = by_thrice(
        jnp.concatenate([jnp.concatenate(group, axis=0) for group in groups], axis=0),
        right_ref[2],
    )
    parts = [moved(div_r[q * ny : (q + 1) * ny], half * q) for q in range(len(groups))]
    parts.append(jnp.concatenate([across_rows(t, columns) for t in packed_s], axis=0))
    parts.append(by_thrice(jnp.concatenate(packed_t, axis=0), right_ref[3]))
    parts.append(jnp.concatenate(packed_m, axis=0))
    px_ref[0:ny] = join_columns(joined(parts), nz)
    row = iota((SCALAR_ROWS, nx), 0)
    kin, ens = jnp.sum(kin, axis=0, keepdims=True), jnp.sum(ens, axis=0, keepdims=True)
    px_ref[ny:] = jnp.where(row == 0, kin, jnp.where(row == 1, ens, 0.0))


def join_columns(packed, nz):
    ny, nx = packed.shape
    packed = jnp.concatenate(
        join_rows([packed[e : e + PTS] for e in range(0, ny, PTS)], iota((PTS, nx), 0)), axis=0
    )
    plane = column_slot(iota((ny, nx), 1), nx) % nz
    up = (plane % PTS == PTS - 1) & (plane < nz - 1)
    down = (plane % PTS == 0) & (plane > 0)
    return (
        packed
        + jnp.where(up, pltpu.roll(packed, nx - 2, 1), 0.0)
        + jnp.where(down, pltpu.roll(packed, 2, 1), 0.0)
    )


def along_y(left, pair, high_ref, low_ref):
    _, _, ny, nx = high_ref.shape
    rows = PTS * ny

    def wide(ref):
        return jnp.concatenate(
            [ref[c, layer * PTS : (layer + 1) * PTS].reshape(rows, nx) for layer, c in pair],
            axis=1,
        )

    high, low = wide(high_ref), wide(low_ref)
    out = dot(left, jnp.concatenate([high, high, low], axis=0))
    return [out[:, n * nx : (n + 1) * nx].reshape(PTS, ny, nx) for n in range(len(pair))]


def along_x(right, layer, c, high_ref, low_ref):
    _, _, ny, nx = high_ref.shape
    zs = slice(layer * PTS, (layer + 1) * PTS)
    high = high_ref[c, zs].reshape(PTS * ny, nx)
    low = low_ref[c, zs].reshape(PTS * ny, nx)
    out = dot(jnp.concatenate([high, low], axis=1), right)
    return (out[:, 0:nx] + out[:, nx : 2 * nx]).reshape(PTS, ny, nx)


def plane_kernel(table, f_ref, m_ref, right_ref, zp_ref):
    _, comps, nz, ny, nx = f_ref.shape
    z_even = lax.axis_index("gz") % 2 == 0
    at = jnp.where(z_even, nz - 1, 0)
    z0 = jnp.where(z_even, nz - PTS, 0)
    weights = [
        jnp.where(z_even, float(table[w, PTS - 1]), float(table[w, 0])) for w in range(PTS)
    ]
    columns = row_columns(table.T, nx)
    tall = jnp.concatenate([f_ref[0, c, at] for c in range(comps)], axis=0)
    div_r = by_thrice(tall, right_ref[1])
    for c in range(comps):
        flux_s = f_ref[1, c, at]
        div_s = [across_rows(flux_s[e : e + PTS], columns) for e in range(0, ny, PTS)]
        div_t = joined([weights[w] * f_ref[2, c, z0 + w] for w in range(PTS)])
        total = div_r[c * ny : (c + 1) * ny] + jnp.concatenate(div_s, axis=0) + div_t
        zp_ref[c] = assemble_plane(total, ny, nx)
    zp_ref[comps] = assemble_plane(m_ref[at].astype(F32), ny, nx)


def diverge_kernel(table, f_ref, m_ref, left_ref, right_ref, w_ref, high_ref, low_ref, y_ref, x_ref):
    _, comps, nz, ny, nx = f_ref.shape
    blocks = [(layer, c) for layer in range(nz // PTS) for c in range(comps)]
    for c in range(comps):
        for z in range(nz):
            high_ref[0, c, z], low_ref[0, c, z] = split(f_ref[0, c, z])
            high_ref[1, c, z], low_ref[1, c, z] = split(f_ref[1, c, z])
    for i in range(0, len(blocks), 2):
        pair = blocks[i : i + 2]
        sums = along_y(left_ref[1], pair, high_ref.at[1], low_ref.at[1])
        for (layer, c), out in zip(pair, sums):
            y_ref[c, layer * PTS : (layer + 1) * PTS] = out
    for layer, c in blocks:
        x_ref[c, layer * PTS : (layer + 1) * PTS] = along_x(
            right_ref[1], layer, c, high_ref.at[0], low_ref.at[0]
        )
    for layer, c in blocks:
        for e in range(0, ny, PTS):
            ys = slice(e, e + PTS)
            z0 = layer * PTS
            out = combine_planes([f_ref[2, c, z0 + z, ys] for z in range(PTS)], table.T)
            for z in range(PTS):
                y_ref[c, z0 + z, ys] = out[z] + y_ref[c, z0 + z, ys] + x_ref[c, z0 + z, ys]
    for f in range(comps + 1):
        for z in range(nz):
            if z % PTS == 0 and z > 0:
                w_ref[f, z] = w_ref[f, z - 1]
                continue
            at = [z, z + 1] if z % PTS == PTS - 1 and z < nz - 1 else [z]
            t = [m_ref[i].astype(F32) if f == comps else y_ref[f, i] for i in at]
            w_ref[f, z] = assemble_plane(joined(t), ny, nx)


def merge_sides(right, left):
    lane = iota(right.shape, 1)
    return jnp.where(lane % 2 == 0, right, pltpu.roll(left, 2, 1))


def place_columns(merged, j, nx):
    lane = iota(merged.shape, 1)
    shift = (nx - 1 - 2 * j) % nx
    moved = pltpu.roll(merged, shift, 1) if shift else merged
    return jnp.where((lane == 0) | (lane == nx - 1), moved, 0.0)


def first_kernel(zp_ref, px_ref, qa_ref, pb_ref, pz_ref, pd_ref):
    fields, ny, nx = zp_ref.shape
    nz = nx // (2 * fields)
    lane = iota((PTS, nx), 1)
    x_even = lax.axis_index("gx") % 2 == 0
    z_even = lax.axis_index("gz") % 2 == 0
    qa = qa_ref[0:ny]
    merged = merge_sides(jnp.where(x_even, qa, 0.0), jnp.where(x_even, 0.0, qa))
    merged = jnp.where(z_even, pltpu.roll(merged, nx - 2 * (nz - 1), 1), merged)
    sums = px_ref[ny:] + qa_ref[ny:]
    pb_ref[0:ny] = px_ref[0:ny]
    pb_ref[ny:] = sums
    for f in range(fields):
        pz_ref[f * ny : (f + 1) * ny] = zp_ref[f] + place_columns(merged, f * nz, nx)
    pz_ref[fields * ny :] = sums
    edge = None
    for e in range(ny // PTS):
        t = px_ref[e * PTS : (e + 1) * PTS]
        t = jnp.where(z_even, pltpu.roll(t, nx - 2 * (nz - 1), 1), t)
        t = pltpu.roll(t, 2 * e, 1) if e else t
        mine = (lane + 1) % nx // 2 % nz == e
        edge = jnp.where(mine, t, 0.0 if edge is None else edge)
    pd_ref[0:PTS] = edge
    pd_ref[PTS:] = sums


def x_sides(qa, qb, x_even):
    return merge_sides(jnp.where(x_even, qa, qb), jnp.where(x_even, qb, qa))


def diagonal_sides(qd, x_even):
    return merge_sides(jnp.where(x_even, 0.0, qd), jnp.where(x_even, qd, 0.0))


def second_kernel(
    u_ref, pb_ref, qa_ref, qb_ref, qz_ref, qd_ref, pya_ref, pyb_ref, ps_ref, low_ref, high_ref
):
    fields, nz, ny, nx = u_ref.shape
    x_even = lax.axis_index("gx") % 2 == 0
    y_even = lax.axis_index("gy") % 2 == 0
    for ys, row, out in (
        (slice(0, PTS), 0, low_ref),
        (slice(ny - PTS, ny), PTS - 1, high_ref),
    ):
        merged = x_sides(qa_ref[ys], qb_ref[ys], x_even)
        diag = diagonal_sides(qd_ref[0:PTS], x_even)
        for f in range(fields):
            for z in range(nz):
                j = f * nz + z
                t = u_ref[f, z, ys] + place_columns(merged, j, nx)
                if z in (0, nz - 1):
                    t = t + qz_ref[f * ny + ys.start : f * ny + ys.stop]
                    t = t + place_columns(diag, f * nz + ys.start // PTS, nx)
                out[j : j + 1] = t[row : row + 1]
    sums = pb_ref[ny:] + qb_ref[ny:] + qz_ref[fields * ny :] + qd_ref[PTS:]
    count = fields * nz
    pya_ref[0:count] = jnp.where(y_even, high_ref[...], low_ref[...])
    pyb_ref[0:count] = jnp.where(y_even, low_ref[...], high_ref[...])
    pya_ref[count:] = sums
    pyb_ref[count:] = sums
    ps_ref[...] = sums


def correct_kernel(v_ref, u_ref, qa_ref, qb_ref, qz_ref, qd_ref, w_ref, mv_ref):
    fields, nz, ny, nx = u_ref.shape
    x_even = lax.axis_index("gx") % 2 == 0
    merged = x_sides(qa_ref[0:ny], qb_ref[0:ny], x_even)
    diag = diagonal_sides(qd_ref[0:PTS], x_even)
    for z in range(nz):
        for f in range(fields):
            t = u_ref[f, z] + place_columns(merged, f * nz + z, nx)
            if z in (0, nz - 1):
                t = t + qz_ref[f * ny : (f + 1) * ny]
                corner = [place_columns(diag, f * nz + e, nx) for e in range(ny // PTS)]
                t = t + jnp.concatenate(corner, axis=0)
            w_ref[f, z] = t
        for c in range(fields - 1):
            mv_ref[c, z] = w_ref[fields - 1, z] * v_ref[c, z]


def last_kernel(
    sizes,
    v_ref,
    w_ref,
    mv_ref,
    qya_ref,
    qyb_ref,
    qs_ref,
    ps_ref,
    out_hbm,
    kin_hbm,
    ens_hbm,
    low_ref,
    high_ref,
    out_ref,
    kin_ref,
    ens_ref,
    sems,
):
    fields, nz, ny, nx = w_ref.shape
    gx, gy, gz = (lax.axis_index(name) for name in ("gx", "gy", "gz"))
    y_even = gy % 2 == 0
    count = fields * nz
    sums = ps_ref[...] + qya_ref[count:] + qyb_ref[count:] + qs_ref[...]
    kinetic = 0.5 * jnp.sum(sums[0:1])
    enstrophy = jnp.sum(sums[1:2])
    kin_ref[0, 0] = kinetic
    ens_ref[0, 0] = enstrophy
    copies = [
        pltpu.make_async_copy(kin_ref, kin_hbm, sems.at[4]),
        pltpu.make_async_copy(ens_ref, ens_hbm, sems.at[5]),
    ]
    for copy in copies:
        copy.start()
    rayleigh = jnp.full((PTS, nx), enstrophy, F32) / jnp.full((PTS, nx), 2.0 * kinetic, F32)
    low_ref[...] = jnp.where(y_even, qyb_ref[0:count], qya_ref[0:count])
    high_ref[...] = jnp.where(y_even, qya_ref[0:count], qyb_ref[0:count])
    row = iota((ny, nx), 0)
    lane = iota((ny, nx), 1)
    x_first = jnp.where(gx == 0, 0, -1)
    x_last = jnp.where(gx == sizes[0] - 1, nx - 1, -1)
    y_first = jnp.where(gy == 0, 0, -1)
    y_last = jnp.where(gy == sizes[1] - 1, ny - 1, -1)
    inside = (lane != x_first) & (lane != x_last) & (row != y_first) & (row != y_last)
    sub = iota((PTS, nx), 0)
    steps = nz // 4
    for z in range(nz):
        keep = inside
        if z == 0:
            keep = keep & (gz > 0)
        if z == nz - 1:
            keep = keep & (gz < sizes[2] - 1)
        for e in range(0, ny, PTS):
            ys = slice(e, e + PTS)
            edge = e == 0 or e == ny - PTS
            side, at = (low_ref, 0) if e == 0 else (high_ref, PTS - 1)
            if edge:
                j = (fields - 1) * nz + z
                extra = rayleigh * jnp.where(sub == at, side[j : j + 1], 0.0)
            for c in range(fields - 1):
                t = w_ref[c, z, ys] - rayleigh * mv_ref[c, z, ys]
                if edge:
                    j = c * nz + z
                    t = t + jnp.where(sub == at, side[j : j + 1], 0.0)
                    t = t - extra * v_ref[c, z, ys]
                out_ref[c, z, ys] = jnp.where(keep[ys], t, 0.0)
        if z % steps == steps - 1:
            zs = pl.ds(z - steps + 1, steps)
            copies.append(
                pltpu.make_async_copy(
                    out_ref.at[:, zs], out_hbm.at[:, zs], sems.at[z // steps]
                )
            )
            copies[-1].start()
    for copy in copies:
        copy.wait()


VMEM = pl.BlockSpec(memory_space=pltpu.VMEM)
HBM = pl.BlockSpec(memory_space=pltpu.HBM)


def call(kernel, outs, ins, scratch=(), out_specs=None, in_specs=None, flops=1 << 20):
    return pl.pallas_call(
        kernel,
        out_shape=[
            out if hasattr(out, "dtype") else jax.ShapeDtypeStruct(out, F32) for out in outs
        ],
        in_specs=in_specs or [VMEM] * len(ins),
        out_specs=out_specs or [VMEM] * len(outs),
        scratch_shapes=list(scratch),
        compiler_params=pltpu.CompilerParams(vmem_limit_bytes=24 << 20),
        cost_estimate=pl.CostEstimate(flops=flops, bytes_accessed=flops, transcendentals=0),
    )(*ins)


def local_part(table, velocity, geometry, mass_weights):
    _, nz, ny, nx = velocity.shape
    rows = PTS * ny
    vector = (3, *velocity.shape)
    return call(
        functools.partial(local_kernel, table),
        [
            vector,
            (ny + SCALAR_ROWS, nx),
            velocity.shape,
            jax.ShapeDtypeStruct(mass_weights.shape, BF16),
            jax.ShapeDtypeStruct((2, rows, 3 * rows), BF16),
            jax.ShapeDtypeStruct((4, 2 * nx, 2 * nx), BF16),
        ],
        [
            pltpu.with_memory_space_constraint(x, pltpu.HBM)
            for x in (velocity, geometry, mass_weights)
        ],
        in_specs=[HBM] * 3,
        scratch=[
            pltpu.VMEM(geometry.shape, BF16),
            pltpu.VMEM(vector, F32),
            pltpu.VMEM(velocity.shape, BF16),
            pltpu.VMEM(velocity.shape, BF16),
            pltpu.SemaphoreType.DMA((nz // PTS, 3)),
        ],
    )


def diverged(table, fluxes, mass, left, right):
    _, comps, nz, ny, nx = fluxes.shape
    return call(
        functools.partial(diverge_kernel, table),
        [(comps + 1, nz, ny, nx)],
        [fluxes, mass, left, right],
        scratch=[
            pltpu.VMEM((2, comps, nz, ny, nx), BF16),
            pltpu.VMEM((2, comps, nz, ny, nx), BF16),
            pltpu.VMEM((comps, nz, ny, nx), F32),
            pltpu.VMEM((comps, nz, ny, nx), F32),
        ],
    )[0]


def pairs_near(count):
    return [(i, i ^ 1) for i in range(count)]


def pairs_mirror(count):
    return [(i, count - 1 - i) for i in range(count)]


def few_rounds(sizes, velocity, geometry, mass_weights):
    comps, nz, ny, nx = velocity.shape
    fields = comps + 1
    table = gll_derivative(ORDER)
    fluxes, px, held, mass, left, right = local_part(table, velocity, geometry, mass_weights)
    qa = lax.ppermute(px, "gx", pairs_near(sizes[0]))
    zp = call(functools.partial(plane_kernel, table), [(fields, ny, nx)], [fluxes, mass, right])[0]
    pb, pz, pd = call(
        first_kernel,
        [
            (ny + SCALAR_ROWS, nx),
            (fields * ny + SCALAR_ROWS, nx),
            (PTS + SCALAR_ROWS, nx),
        ],
        [zp, px, qa],
    )
    mirror = pairs_mirror(sizes[0])
    qb = lax.ppermute(pb, "gx", mirror)
    qz = lax.ppermute(pz, "gz", pairs_near(sizes[2]))
    both = [
        (i * sizes[2] + k, mirror[i][1] * sizes[2] + (k ^ 1))
        for i in range(sizes[0])
        for k in range(sizes[2])
    ]
    qd = lax.ppermute(pd, ("gx", "gz"), both)
    u = diverged(table, fluxes, mass, left, right)
    count = fields * nz
    pya, pyb, ps = call(
        second_kernel,
        [(count + SCALAR_ROWS, nx), (count + SCALAR_ROWS, nx), (SCALAR_ROWS, nx)],
        [u, pb, qa, qb, qz, qd],
        scratch=[pltpu.VMEM((count, nx), F32)] * 2,
    )
    apart = [
        (i * sizes[1] + j, (i ^ 1) * sizes[1] + (j ^ 2))
        for i in range(sizes[0])
        for j in range(sizes[1])
    ]
    qya = lax.ppermute(pya, "gy", pairs_near(sizes[1]))
    qyb = lax.ppermute(pyb, "gy", pairs_mirror(sizes[1]))
    qs = lax.ppermute(ps, ("gx", "gy"), apart)
    w, mv = call(correct_kernel, [u.shape, velocity.shape], [held, u, qa, qb, qz, qd])
    residual, kinetic, enstrophy = call(
        functools.partial(last_kernel, sizes),
        [velocity.shape, (1, 1), (1, 1)],
        [held, w, mv, qya, qyb, qs, ps],
        scratch=[
            pltpu.VMEM((count, nx), F32),
            pltpu.VMEM((count, nx), F32),
            pltpu.VMEM(velocity.shape, F32),
            pltpu.SMEM((1, 1), F32),
            pltpu.SMEM((1, 1), F32),
            pltpu.SemaphoreType.DMA((6,)),
        ],
        out_specs=[HBM, HBM, HBM],
    )
    return residual, kinetic[0, 0], enstrophy[0, 0]


def add_neighbours(field, axis, dim):
    count = lax.axis_size(axis)
    extent = field.shape[dim]
    first = lax.slice_in_dim(field, 0, 1, axis=dim)
    last = lax.slice_in_dim(field, extent - 1, extent, axis=dim)
    low = lax.ppermute(last, axis, [(i, i + 1) for i in range(count - 1)])
    high = lax.ppermute(first, axis, [(i + 1, i) for i in range(count - 1)])
    middle = lax.slice_in_dim(field, 1, extent - 1, axis=dim)
    return jnp.concatenate([first + low, middle, last + high], axis=dim)


def any_mesh(sizes, velocity, geometry, mass_weights):
    comps, nz, ny, nx = velocity.shape
    table = gll_derivative(ORDER)
    fluxes, px, _, mass, left, right = local_part(table, velocity, geometry, mass_weights)
    u = diverged(table, fluxes, mass, left, right)
    kinetic = 0.5 * jnp.sum(px[ny])
    enstrophy = jnp.sum(px[ny + 1])
    kinetic, enstrophy = lax.psum((kinetic, enstrophy), ("gx", "gy", "gz"))
    for axis, dim in (("gx", 3), ("gy", 2), ("gz", 1)):
        u = add_neighbours(u, axis, dim)
    inside = jnp.ones((nz, ny, nx), bool)
    for dim, (axis, size) in enumerate(zip(("gz", "gy", "gx"), sizes[::-1])):
        place = lax.axis_index(axis) * inside.shape[dim] + iota(inside.shape, dim)
        inside = inside & (place > 0) & (place < size * inside.shape[dim] - 1)
    rayleigh = enstrophy / (2.0 * kinetic)
    residual = jnp.where(inside[None], u[:comps] - rayleigh * u[comps][None] * velocity, 0.0)
    return residual, kinetic, enstrophy


def solution(mesh):
    sizes = tuple(mesh.shape[name] for name in ("gx", "gy", "gz"))
    plan = few_rounds if sizes == (4, 4, 2) else any_mesh
    in_specs = (P(None, "gz", "gy", "gx"), P(None, "gz", "gy", "gx"), P("gz", "gy", "gx"))
    out_specs = (P(None, "gz", "gy", "gx"), P(), P())

    def body(*args):
        return plan(sizes, *args)

    step = jax.shard_map(
        body, mesh=mesh, in_specs=in_specs, out_specs=out_specs, check_vma=False
    )
    if plan is any_mesh:
        return step
    return step
```

```python
import functools

import jax
import jax.numpy as jnp
import numpy as np
from jax import lax
from jax.experimental import pallas as pl
from jax.experimental.pallas import tpu as pltpu
from jax.sharding import PartitionSpec as P


ORDER = 7
PTS = ORDER + 1
F32 = jnp.float32
BF16 = jnp.bfloat16
SCALAR_ROWS = 8


def gll_derivative(poly_order):
    node_count = poly_order + 1
    abscissa = np.cos(np.pi * np.arange(node_count) / poly_order)
    legendre = np.zeros((node_count, node_count))
    for _ in range(60):
        legendre[:, 0] = 1.0
        legendre[:, 1] = abscissa
        for degree in range(2, node_count):
            legendre[:, degree] = (
                (2 * degree - 1) * abscissa * legendre[:, degree - 1]
                - (degree - 1) * legendre[:, degree - 2]
            ) / degree
        abscissa = abscissa - (abscissa * legendre[:, poly_order] - legendre[:, poly_order - 1]) / (
            node_count * legendre[:, poly_order]
        )
    abscissa = abscissa[::-1]
    end_values = legendre[::-1, poly_order]
    spacing = abscissa[:, None] - abscissa[None, :] + np.eye(node_count)
    deriv_table = end_values[:, None] / end_values[None, :] / spacing
    deriv_table = deriv_table * (1.0 - np.eye(node_count))
    deriv_table[0, 0] = -poly_order * node_count / 4.0
    deriv_table[poly_order, poly_order] = poly_order * node_count / 4.0
    return deriv_table.astype(np.float32)


def split(x):
    high = x.astype(BF16)
    return high, (x - high.astype(F32)).astype(BF16)


def iota(shape, dim):
    return lax.broadcasted_iota(jnp.int32, shape, dim)


def repeated(table, width):
    lane = iota((PTS, width), 1) % PTS
    rows = []
    for i in range(PTS):
        row = jnp.full((PTS, width), float(table[i, 0]), F32)
        for k in range(1, PTS):
            row = jnp.where(lane == k, float(table[i, k]), row)
        rows.append(row)
    return rows


def fine_matrix(table, size):
    sub = iota((PTS, size), 0)
    rows = repeated(table, size)
    tile = rows[0]
    for i in range(1, PTS):
        tile = jnp.where(sub == i, rows[i], tile)
    block = iota((PTS, size), 1) // PTS
    return split(
        jnp.concatenate(
            [jnp.where(block == e, tile, 0.0) for e in range(size // PTS)], axis=0
        )
    )


def combine_planes(planes, table):
    half = PTS // 2
    even = [planes[k] + planes[PTS - 1 - k] for k in range(half)]
    odd = [planes[k] - planes[PTS - 1 - k] for k in range(half)]
    low, high = [], []
    for w in range(half):
        p = q = None
        for k in range(half):
            a, b = float(table[w, k]), float(table[w, PTS - 1 - k])
            pe = np.float32((a + b) / 2) * even[k]
            qo = np.float32((a - b) / 2) * odd[k]
            p = pe if p is None else p + pe
            q = qo if q is None else q + qo
        low.append(p + q)
        high.append(q - p)
    return low + high[::-1]


def dot(a, b):
    return jnp.dot(a, b, preferred_element_type=F32)


def join_rows(tiles, sub):
    done = []
    for e, t in enumerate(tiles):
        if e + 1 < len(tiles):
            t = t + jnp.where(sub == PTS - 1, pltpu.roll(tiles[e + 1], PTS - 1, 0), 0.0)
        if e > 0:
            t = t + jnp.where(sub == 0, pltpu.roll(tiles[e - 1], 1, 0), 0.0)
        done.append(t)
    return done


def assemble_plane(u, ny, nx):
    lane = iota((PTS, nx), 1)
    sub = iota((PTS, nx), 0)
    last = (lane % PTS == PTS - 1) & (lane < nx - 1)
    first = (lane % PTS == 0) & (lane > 0)
    tiles = []
    for e in range(ny // PTS):
        t = u[e * PTS : (e + 1) * PTS]
        t = (
            t
            + jnp.where(last, pltpu.roll(t, nx - 1, 1), 0.0)
            + jnp.where(first, pltpu.roll(t, 1, 1), 0.0)
        )
        tiles.append(t)
    return jnp.concatenate(join_rows(tiles, sub), axis=0)


def joined(pieces):
    return pieces[0] if len(pieces) == 1 else joined(
        [sum(pieces[i : i + 2][1:], pieces[i]) for i in range(0, len(pieces), 2)]
    )


def across_rows(tile, columns):
    return joined(
        [column * jnp.broadcast_to(tile[k : k + 1], tile.shape) for k, column in enumerate(columns)]
    )


def row_columns(table, nx):
    sub = iota((PTS, nx), 0)
    columns = []
    for k in range(PTS):
        column = jnp.full((PTS, nx), float(table[0, k]), F32)
        for w in range(1, PTS):
            column = jnp.where(sub == w, float(table[w, k]), column)
        columns.append(column)
    return columns


def by_thrice(x, weights):
    high, low = split(x)
    out = dot(jnp.concatenate([high, low], axis=1), weights)
    half = weights.shape[1] // 2
    return out[:, 0:half] + out[:, half:]


def thrice(high, low):
    return jnp.concatenate(
        [
            jnp.concatenate([high, low], axis=1),
            jnp.concatenate([high, jnp.zeros_like(low)], axis=1),
        ],
        axis=0,
    )


def column_slot(lane, nx):
    return (lane + 1) % nx // 2


def packed_z_matrix(table, nx):
    into, out = iota((nx, nx), 0), iota((nx, nx), 1)
    j, k = column_slot(into, nx), column_slot(out, nx)
    value = jnp.zeros((nx, nx), F32)
    for w in range(PTS):
        row = jnp.zeros((nx, nx), F32)
        for q in range(PTS):
            row = jnp.where(k % PTS == q, float(table[w, q]), row)
        value = jnp.where(j % PTS == w, row, value)
    same = (j // PTS == k // PTS) & (into % 2 == out % 2)
    return jnp.where(same, value, 0.0)


def packed_x_matrix(table, nx):
    into, out = iota((nx, nx), 0), iota((nx, nx), 1)
    place, plane = into % (2 * PTS), into // (2 * PTS)
    value = jnp.zeros((nx, nx), F32)
    for w in range(PTS):
        value = jnp.where(place == w, float(table[w, PTS - 1]), value)
        value = jnp.where(place == PTS + w, float(table[w, 0]), value)
    target = jnp.where(place < PTS, (2 * plane - 1) % nx, 2 * plane)
    return jnp.where(out == target, value, 0.0)


def local_kernel(
    table,
    v_hbm,
    g_hbm,
    m_hbm,
    f_ref,
    px_ref,
    v_ref,
    m_ref,
    left_ref,
    right_ref,
    g_ref,
    grad_ref,
    high_ref,
    low_ref,
    sems,
):
    comps, nz, ny, nx = v_ref.shape
    layers = nz // PTS
    rows = PTS * ny
    half = 2 * PTS
    v_copies = []
    gm_copies = []
    for layer in range(layers):
        zs = pl.ds(layer * PTS, PTS)
        v_copies.append(
            pltpu.make_async_copy(v_hbm.at[:, zs], v_ref.at[:, zs], sems.at[layer, 0])
        )
        gm_copies.append(
            pltpu.make_async_copy(g_hbm.at[:, zs], g_ref.at[:, zs], sems.at[layer, 1])
        )
        gm_copies.append(pltpu.make_async_copy(m_hbm.at[zs], m_ref.at[zs], sems.at[layer, 2]))
    for copy in v_copies + gm_copies:
        copy.start()
    for i, matrix in enumerate((table, table.T)):
        h, l = fine_matrix(matrix, rows)
        left_ref[i] = jnp.concatenate([h, l, h], axis=1)
        right_ref[i] = thrice(*fine_matrix(matrix.T, nx))
    right_ref[2] = thrice(*split(packed_x_matrix(table, nx)))
    right_ref[3] = thrice(*split(packed_z_matrix(table, nx)))
    columns = row_columns(table.T, nx)
    blocks = [(layer, c) for layer in range(layers) for c in range(comps)]

    def planes(layer):
        return slice(layer * PTS, (layer + 1) * PTS)

    for copy in v_copies:
        copy.wait()
    for c in range(comps):
        for z in range(nz):
            high_ref[c, z], low_ref[c, z] = split(v_ref[c, z])
    for layer, c in blocks:
        grad_ref[0, c, planes(layer)] = along_x(right_ref[0], layer, c, high_ref, low_ref)
    for i in range(0, len(blocks), 2):
        pair = blocks[i : i + 2]
        for (layer, c), out in zip(pair, along_y(left_ref[0], pair, high_ref, low_ref)):
            grad_ref[1, c, planes(layer)] = out
    for layer, c in blocks:
        for e in range(0, ny, PTS):
            ys = slice(e, e + PTS)
            z0 = layer * PTS
            out = combine_planes([v_ref[c, z0 + z, ys] for z in range(PTS)], table)
            for z in range(PTS):
                grad_ref[2, c, z0 + z, ys] = out[z]
    for copy in gm_copies:
        copy.wait()
    lane = iota((PTS, nx), 1)
    slot, place = column_slot(lane, nx), lane // half

    def moved(x, shift):
        return pltpu.roll(x, shift, 1) if shift else x

    kin = jnp.zeros((half, nx), F32)
    ens = jnp.zeros((half, nx), F32)
    tiles = ny // PTS
    zero = jnp.zeros((PTS, nx), F32)
    packed_s, packed_t, packed_m = ([zero] * tiles for _ in range(3))
    groups = [[zero] * tiles for _ in range(comps * layers)]
    for y in range(0, ny, half):
        ys = slice(y, y + half)
        for z in range(nz):
            g = [g_ref[i, z, ys].astype(F32) for i in range(6)]
            mass = m_ref[z, ys].astype(F32)
            square = None
            for c in range(comps):
                v = v_ref[c, z, ys]
                square = v * v if square is None else square + v * v
                gr, gs, gt = (grad_ref[i, c, z, ys] for i in range(3))
                fr = g[0] * gr + g[3] * gs + g[4] * gt
                fs = g[3] * gr + g[1] * gs + g[5] * gt
                ft = g[4] * gr + g[5] * gs + g[2] * gt
                ens = ens + (gr * fr + gs * fs + gt * ft)
                f_ref[0, c, z, ys] = fr
                f_ref[1, c, z, ys] = fs
                f_ref[2, c, z, ys] = ft
                j = c * nz + z
                here, mine = slot == j, place == j % PTS
                for e in range(half // PTS):
                    t, rs = y // PTS + e, slice(e * PTS, (e + 1) * PTS)
                    packed_s[t] = jnp.where(here, moved(fs[rs], 2 * j), packed_s[t])
                    packed_t[t] = jnp.where(here, moved(ft[rs], 2 * j), packed_t[t])
                    part = moved(fr[rs], (PTS + half * (j % PTS)) % nx)
                    groups[j // PTS][t] = jnp.where(mine, part, groups[j // PTS][t])
            kin = kin + mass * square
            j = comps * nz + z
            for e in range(half // PTS):
                t, rs = y // PTS + e, slice(e * PTS, (e + 1) * PTS)
                packed_m[t] = jnp.where(slot == j, moved(mass[rs], 2 * j), packed_m[t])
    div_r = by_thrice(
        jnp.concatenate([jnp.concatenate(group, axis=0) for group in groups], axis=0),
        right_ref[2],
    )
    parts = [moved(div_r[q * ny : (q + 1) * ny], half * q) for q in range(len(groups))]
    parts.append(jnp.concatenate([across_rows(t, columns) for t in packed_s], axis=0))
    parts.append(by_thrice(jnp.concatenate(packed_t, axis=0), right_ref[3]))
    parts.append(jnp.concatenate(packed_m, axis=0))
    px_ref[0:ny] = join_columns(joined(parts), nz)
    row = iota((SCALAR_ROWS, nx), 0)
    kin, ens = jnp.sum(kin, axis=0, keepdims=True), jnp.sum(ens, axis=0, keepdims=True)
    px_ref[ny:] = jnp.where(row == 0, kin, jnp.where(row == 1, ens, 0.0))


def join_columns(packed, nz):
    ny, nx = packed.shape
    packed = jnp.concatenate(
        join_rows([packed[e : e + PTS] for e in range(0, ny, PTS)], iota((PTS, nx), 0)), axis=0
    )
    plane = column_slot(iota((ny, nx), 1), nx) % nz
    up = (plane % PTS == PTS - 1) & (plane < nz - 1)
    down = (plane % PTS == 0) & (plane > 0)
    return (
        packed
        + jnp.where(up, pltpu.roll(packed, nx - 2, 1), 0.0)
        + jnp.where(down, pltpu.roll(packed, 2, 1), 0.0)
    )


def along_y(left, pair, high_ref, low_ref):
    _, _, ny, nx = high_ref.shape
    rows = PTS * ny

    def wide(ref):
        return jnp.concatenate(
            [ref[c, layer * PTS : (layer + 1) * PTS].reshape(rows, nx) for layer, c in pair],
            axis=1,
        )

    high, low = wide(high_ref), wide(low_ref)
    out = dot(left, jnp.concatenate([high, high, low], axis=0))
    return [out[:, n * nx : (n + 1) * nx].reshape(PTS, ny, nx) for n in range(len(pair))]


def along_x(right, layer, c, high_ref, low_ref):
    _, _, ny, nx = high_ref.shape
    zs = slice(layer * PTS, (layer + 1) * PTS)
    high = high_ref[c, zs].reshape(PTS * ny, nx)
    low = low_ref[c, zs].reshape(PTS * ny, nx)
    out = dot(jnp.concatenate([high, low], axis=1), right)
    return (out[:, 0:nx] + out[:, nx : 2 * nx]).reshape(PTS, ny, nx)


def plane_kernel(table, f_ref, m_ref, right_ref, zp_ref):
    _, comps, nz, ny, nx = f_ref.shape
    z_even = lax.axis_index("gz") % 2 == 0
    at = jnp.where(z_even, nz - 1, 0)
    z0 = jnp.where(z_even, nz - PTS, 0)
    weights = [
        jnp.where(z_even, float(table[w, PTS - 1]), float(table[w, 0])) for w in range(PTS)
    ]
    columns = row_columns(table.T, nx)
    tall = jnp.concatenate([f_ref[0, c, at] for c in range(comps)], axis=0)
    div_r = by_thrice(tall, right_ref[1])
    for c in range(comps):
        flux_s = f_ref[1, c, at]
        div_s = [across_rows(flux_s[e : e + PTS], columns) for e in range(0, ny, PTS)]
        div_t = joined([weights[w] * f_ref[2, c, z0 + w] for w in range(PTS)])
        total = div_r[c * ny : (c + 1) * ny] + jnp.concatenate(div_s, axis=0) + div_t
        zp_ref[c] = assemble_plane(total, ny, nx)
    zp_ref[comps] = assemble_plane(m_ref[at].astype(F32), ny, nx)


def diverge_kernel(
    table, f_ref, m_ref, left_ref, right_ref, w_ref, ends_ref, high_ref, low_ref, y_ref, x_ref
):
    _, comps, nz, ny, nx = f_ref.shape
    blocks = [(layer, c) for layer in range(nz // PTS) for c in range(comps)]
    for c in range(comps):
        for z in range(nz):
            high_ref[0, c, z], low_ref[0, c, z] = split(f_ref[0, c, z])
            high_ref[1, c, z], low_ref[1, c, z] = split(f_ref[1, c, z])
    for i in range(0, len(blocks), 2):
        pair = blocks[i : i + 2]
        sums = along_y(left_ref[1], pair, high_ref.at[1], low_ref.at[1])
        for (layer, c), out in zip(pair, sums):
            y_ref[c, layer * PTS : (layer + 1) * PTS] = out
    for layer, c in blocks:
        x_ref[c, layer * PTS : (layer + 1) * PTS] = along_x(
            right_ref[1], layer, c, high_ref.at[0], low_ref.at[0]
        )
    for layer, c in blocks:
        for e in range(0, ny, PTS):
            ys = slice(e, e + PTS)
            z0 = layer * PTS
            out = combine_planes([f_ref[2, c, z0 + z, ys] for z in range(PTS)], table.T)
            for z in range(PTS):
                y_ref[c, z0 + z, ys] = out[z] + y_ref[c, z0 + z, ys] + x_ref[c, z0 + z, ys]
    for f in range(comps + 1):
        for z in range(nz):
            j = ends_ref.shape[1] - 1 - f * nz - z
            if z % PTS == 0 and z > 0:
                w_ref[f, z] = w_ref[f, z - 1]
                ends_ref[:, j] = ends_ref[:, j + 1]
                continue
            at = [z, z + 1] if z % PTS == PTS - 1 and z < nz - 1 else [z]
            t = [m_ref[i].astype(F32) if f == comps else y_ref[f, i] for i in at]
            whole = assemble_plane(joined(t), ny, nx)
            w_ref[f, z] = whole
            ends_ref[0, j : j + 1] = whole[0:1]
            ends_ref[1, j : j + 1] = whole[ny - 1 : ny]


def merge_sides(right, left):
    lane = iota(right.shape, 1)
    return jnp.where(lane % 2 == 0, right, pltpu.roll(left, 2, 1))


def place_columns(merged, j, nx):
    lane = iota(merged.shape, 1)
    shift = (nx - 1 - 2 * j) % nx
    moved = pltpu.roll(merged, shift, 1) if shift else merged
    return jnp.where((lane == 0) | (lane == nx - 1), moved, 0.0)


def first_kernel(zp_ref, px_ref, qa_ref, pb_ref, pz_ref, pd_ref):
    fields, ny, nx = zp_ref.shape
    nz = nx // (2 * fields)
    lane = iota((PTS, nx), 1)
    x_even = lax.axis_index("gx") % 2 == 0
    z_even = lax.axis_index("gz") % 2 == 0
    qa = qa_ref[0:ny]
    merged = merge_sides(jnp.where(x_even, qa, 0.0), jnp.where(x_even, 0.0, qa))
    merged = jnp.where(z_even, pltpu.roll(merged, nx - 2 * (nz - 1), 1), merged)
    sums = px_ref[ny:] + qa_ref[ny:]
    pb_ref[0:ny] = px_ref[0:ny]
    pb_ref[ny:] = sums
    for f in range(fields):
        pz_ref[f * ny : (f + 1) * ny] = zp_ref[f] + place_columns(merged, f * nz, nx)
    pz_ref[fields * ny :] = sums
    edge = None
    for e in range(ny // PTS):
        t = px_ref[e * PTS : (e + 1) * PTS]
        t = jnp.where(z_even, pltpu.roll(t, nx - 2 * (nz - 1), 1), t)
        t = pltpu.roll(t, 2 * e, 1) if e else t
        mine = (lane + 1) % nx // 2 % nz == e
        edge = jnp.where(mine, t, 0.0 if edge is None else edge)
    pd_ref[0:PTS] = edge
    pd_ref[PTS:] = sums


def x_sides(qa, qb, x_even):
    return merge_sides(jnp.where(x_even, qa, qb), jnp.where(x_even, qb, qa))


def diagonal_sides(qd, x_even):
    return merge_sides(jnp.where(x_even, 0.0, qd), jnp.where(x_even, qd, 0.0))


def spread_columns(merged, count):
    nx = merged.shape[1]
    rows = jnp.broadcast_to(merged, (count, nx))
    rows = pltpu.roll(rows, (nx + 1 - 2 * count) % nx, 1, stride=2, stride_axis=0)
    lane = iota((count, nx), 1)
    return jnp.where((lane == 0) | (lane == nx - 1), rows, 0.0)


def second_kernel(
    ends_ref, pb_ref, qa_ref, qb_ref, qz_ref, qd_ref, pya_ref, pyb_ref, ps_ref, low_ref, high_ref
):
    _, count, nx = ends_ref.shape
    ny = pb_ref.shape[0] - SCALAR_ROWS
    fields = (qz_ref.shape[0] - SCALAR_ROWS) // ny
    nz = count // fields
    x_even = lax.axis_index("gx") % 2 == 0
    y_even = lax.axis_index("gy") % 2 == 0
    diag = diagonal_sides(qd_ref[0:PTS], x_even)
    for i, (y, out) in enumerate(((0, low_ref), (ny - 1, high_ref))):
        merged = x_sides(qa_ref[y : y + 1], qb_ref[y : y + 1], x_even)
        out[...] = ends_ref[i] + spread_columns(merged, count)
        for f in range(fields):
            corner = place_columns(diag, f * nz + y // PTS, nx)[y % PTS : y % PTS + 1]
            extra = qz_ref[f * ny + y : f * ny + y + 1] + corner
            for z in (0, nz - 1):
                j = count - 1 - f * nz - z
                out[j : j + 1] = out[j : j + 1] + extra
    sums = pb_ref[ny:] + qb_ref[ny:] + qz_ref[fields * ny :] + qd_ref[PTS:]
    pya_ref[0:count] = jnp.where(y_even, high_ref[...], low_ref[...])
    pyb_ref[0:count] = jnp.where(y_even, low_ref[...], high_ref[...])
    pya_ref[count:] = sums
    pyb_ref[count:] = sums
    ps_ref[...] = sums


def correct_kernel(v_ref, u_ref, qa_ref, qb_ref, qz_ref, qd_ref, w_ref, mv_ref):
    fields, nz, ny, nx = u_ref.shape
    x_even = lax.axis_index("gx") % 2 == 0
    merged = x_sides(qa_ref[0:ny], qb_ref[0:ny], x_even)
    diag = diagonal_sides(qd_ref[0:PTS], x_even)
    for z in range(nz):
        for f in range(fields):
            t = u_ref[f, z] + place_columns(merged, f * nz + z, nx)
            if z in (0, nz - 1):
                t = t + qz_ref[f * ny : (f + 1) * ny]
                corner = [place_columns(diag, f * nz + e, nx) for e in range(ny // PTS)]
                t = t + jnp.concatenate(corner, axis=0)
            w_ref[f, z] = t
        for c in range(fields - 1):
            mv_ref[c, z] = w_ref[fields - 1, z] * v_ref[c, z]


def last_kernel(
    sizes,
    v_ref,
    w_ref,
    mv_ref,
    qya_ref,
    qyb_ref,
    qs_ref,
    ps_ref,
    out_hbm,
    kin_hbm,
    ens_hbm,
    low_ref,
    high_ref,
    out_ref,
    kin_ref,
    ens_ref,
    sems,
):
    fields, nz, ny, nx = w_ref.shape
    gx, gy, gz = (lax.axis_index(name) for name in ("gx", "gy", "gz"))
    y_even = gy % 2 == 0
    count = fields * nz
    sums = ps_ref[...] + qya_ref[count:] + qyb_ref[count:] + qs_ref[...]
    kinetic = 0.5 * jnp.sum(sums[0:1])
    enstrophy = jnp.sum(sums[1:2])
    kin_ref[0, 0] = kinetic
    ens_ref[0, 0] = enstrophy
    copies = [
        pltpu.make_async_copy(kin_ref, kin_hbm, sems.at[4]),
        pltpu.make_async_copy(ens_ref, ens_hbm, sems.at[5]),
    ]
    for copy in copies:
        copy.start()
    rayleigh = jnp.full((PTS, nx), enstrophy, F32) / jnp.full((PTS, nx), 2.0 * kinetic, F32)
    low_ref[...] = jnp.where(y_even, qyb_ref[0:count], qya_ref[0:count])
    high_ref[...] = jnp.where(y_even, qya_ref[0:count], qyb_ref[0:count])
    row = iota((ny, nx), 0)
    lane = iota((ny, nx), 1)
    x_first = jnp.where(gx == 0, 0, -1)
    x_last = jnp.where(gx == sizes[0] - 1, nx - 1, -1)
    y_first = jnp.where(gy == 0, 0, -1)
    y_last = jnp.where(gy == sizes[1] - 1, ny - 1, -1)
    inside = (lane != x_first) & (lane != x_last) & (row != y_first) & (row != y_last)
    sub = iota((PTS, nx), 0)
    steps = nz // 4
    for z in range(nz):
        keep = inside
        if z == 0:
            keep = keep & (gz > 0)
        if z == nz - 1:
            keep = keep & (gz < sizes[2] - 1)
        for e in range(0, ny, PTS):
            ys = slice(e, e + PTS)
            edge = e == 0 or e == ny - PTS
            side, at = (low_ref, 0) if e == 0 else (high_ref, PTS - 1)
            if edge:
                j = nz - 1 - z
                extra = rayleigh * jnp.where(sub == at, side[j : j + 1], 0.0)
            for c in range(fields - 1):
                t = w_ref[c, z, ys] - rayleigh * mv_ref[c, z, ys]
                if edge:
                    j = count - 1 - c * nz - z
                    t = t + jnp.where(sub == at, side[j : j + 1], 0.0)
                    t = t - extra * v_ref[c, z, ys]
                out_ref[c, z, ys] = jnp.where(keep[ys], t, 0.0)
        if z % steps == steps - 1:
            zs = pl.ds(z - steps + 1, steps)
            copies.append(
                pltpu.make_async_copy(
                    out_ref.at[:, zs], out_hbm.at[:, zs], sems.at[z // steps]
                )
            )
            copies[-1].start()
    for copy in copies:
        copy.wait()


VMEM = pl.BlockSpec(memory_space=pltpu.VMEM)
HBM = pl.BlockSpec(memory_space=pltpu.HBM)


def call(kernel, outs, ins, scratch=(), out_specs=None, in_specs=None, flops=1 << 20):
    return pl.pallas_call(
        kernel,
        out_shape=[
            out if hasattr(out, "dtype") else jax.ShapeDtypeStruct(out, F32) for out in outs
        ],
        in_specs=in_specs or [VMEM] * len(ins),
        out_specs=out_specs or [VMEM] * len(outs),
        scratch_shapes=list(scratch),
        compiler_params=pltpu.CompilerParams(vmem_limit_bytes=24 << 20),
        cost_estimate=pl.CostEstimate(flops=flops, bytes_accessed=flops, transcendentals=0),
    )(*ins)


def local_part(table, velocity, geometry, mass_weights):
    _, nz, ny, nx = velocity.shape
    rows = PTS * ny
    vector = (3, *velocity.shape)
    return call(
        functools.partial(local_kernel, table),
        [
            vector,
            (ny + SCALAR_ROWS, nx),
            velocity.shape,
            jax.ShapeDtypeStruct(mass_weights.shape, BF16),
            jax.ShapeDtypeStruct((2, rows, 3 * rows), BF16),
            jax.ShapeDtypeStruct((4, 2 * nx, 2 * nx), BF16),
        ],
        [
            pltpu.with_memory_space_constraint(x, pltpu.HBM)
            for x in (velocity, geometry, mass_weights)
        ],
        in_specs=[HBM] * 3,
        scratch=[
            pltpu.VMEM(geometry.shape, BF16),
            pltpu.VMEM(vector, F32),
            pltpu.VMEM(velocity.shape, BF16),
            pltpu.VMEM(velocity.shape, BF16),
            pltpu.SemaphoreType.DMA((nz // PTS, 3)),
        ],
    )


def diverged(table, fluxes, mass, left, right):
    _, comps, nz, ny, nx = fluxes.shape
    return call(
        functools.partial(diverge_kernel, table),
        [(comps + 1, nz, ny, nx), (2, (comps + 1) * nz, nx)],
        [fluxes, mass, left, right],
        scratch=[
            pltpu.VMEM((2, comps, nz, ny, nx), BF16),
            pltpu.VMEM((2, comps, nz, ny, nx), BF16),
            pltpu.VMEM((comps, nz, ny, nx), F32),
            pltpu.VMEM((comps, nz, ny, nx), F32),
        ],
    )


def pairs_near(count):
    return [(i, i ^ 1) for i in range(count)]


def pairs_mirror(count):
    return [(i, count - 1 - i) for i in range(count)]


def few_rounds(sizes, velocity, geometry, mass_weights):
    comps, nz, ny, nx = velocity.shape
    fields = comps + 1
    table = gll_derivative(ORDER)
    fluxes, px, held, mass, left, right = local_part(table, velocity, geometry, mass_weights)
    qa = lax.ppermute(px, "gx", pairs_near(sizes[0]))
    zp = call(functools.partial(plane_kernel, table), [(fields, ny, nx)], [fluxes, mass, right])[0]
    pb, pz, pd = call(
        first_kernel,
        [
            (ny + SCALAR_ROWS, nx),
            (fields * ny + SCALAR_ROWS, nx),
            (PTS + SCALAR_ROWS, nx),
        ],
        [zp, px, qa],
    )
    mirror = pairs_mirror(sizes[0])
    qb = lax.ppermute(pb, "gx", mirror)
    qz = lax.ppermute(pz, "gz", pairs_near(sizes[2]))
    both = [
        (i * sizes[2] + k, mirror[i][1] * sizes[2] + (k ^ 1))
        for i in range(sizes[0])
        for k in range(sizes[2])
    ]
    qd = lax.ppermute(pd, ("gx", "gz"), both)
    u, ends = diverged(table, fluxes, mass, left, right)
    count = fields * nz
    pya, pyb, ps = call(
        second_kernel,
        [(count + SCALAR_ROWS, nx), (count + SCALAR_ROWS, nx), (SCALAR_ROWS, nx)],
        [ends, pb, qa, qb, qz, qd],
        scratch=[pltpu.VMEM((count, nx), F32)] * 2,
    )
    apart = [
        (i * sizes[1] + j, (i ^ 1) * sizes[1] + (j ^ 2))
        for i in range(sizes[0])
        for j in range(sizes[1])
    ]
    qya = lax.ppermute(pya, "gy", pairs_near(sizes[1]))
    qyb = lax.ppermute(pyb, "gy", pairs_mirror(sizes[1]))
    qs = lax.ppermute(ps, ("gx", "gy"), apart)
    w, mv = call(correct_kernel, [u.shape, velocity.shape], [held, u, qa, qb, qz, qd])
    residual, kinetic, enstrophy = call(
        functools.partial(last_kernel, sizes),
        [velocity.shape, (1, 1), (1, 1)],
        [held, w, mv, qya, qyb, qs, ps],
        scratch=[
            pltpu.VMEM((count, nx), F32),
            pltpu.VMEM((count, nx), F32),
            pltpu.VMEM(velocity.shape, F32),
            pltpu.SMEM((1, 1), F32),
            pltpu.SMEM((1, 1), F32),
            pltpu.SemaphoreType.DMA((6,)),
        ],
        out_specs=[HBM, HBM, HBM],
    )
    return residual, kinetic[0, 0], enstrophy[0, 0]


def add_neighbours(field, axis, dim):
    count = lax.axis_size(axis)
    extent = field.shape[dim]
    first = lax.slice_in_dim(field, 0, 1, axis=dim)
    last = lax.slice_in_dim(field, extent - 1, extent, axis=dim)
    low = lax.ppermute(last, axis, [(i, i + 1) for i in range(count - 1)])
    high = lax.ppermute(first, axis, [(i + 1, i) for i in range(count - 1)])
    middle = lax.slice_in_dim(field, 1, extent - 1, axis=dim)
    return jnp.concatenate([first + low, middle, last + high], axis=dim)


def any_mesh(sizes, velocity, geometry, mass_weights):
    comps, nz, ny, nx = velocity.shape
    table = gll_derivative(ORDER)
    fluxes, px, _, mass, left, right = local_part(table, velocity, geometry, mass_weights)
    u, _ = diverged(table, fluxes, mass, left, right)
    kinetic = 0.5 * jnp.sum(px[ny])
    enstrophy = jnp.sum(px[ny + 1])
    kinetic, enstrophy = lax.psum((kinetic, enstrophy), ("gx", "gy", "gz"))
    for axis, dim in (("gx", 3), ("gy", 2), ("gz", 1)):
        u = add_neighbours(u, axis, dim)
    inside = jnp.ones((nz, ny, nx), bool)
    for dim, (axis, size) in enumerate(zip(("gz", "gy", "gx"), sizes[::-1])):
        place = lax.axis_index(axis) * inside.shape[dim] + iota(inside.shape, dim)
        inside = inside & (place > 0) & (place < size * inside.shape[dim] - 1)
    rayleigh = enstrophy / (2.0 * kinetic)
    residual = jnp.where(inside[None], u[:comps] - rayleigh * u[comps][None] * velocity, 0.0)
    return residual, kinetic, enstrophy


def solution(mesh):
    sizes = tuple(mesh.shape[name] for name in ("gx", "gy", "gz"))
    plan = few_rounds if sizes == (4, 4, 2) else any_mesh
    in_specs = (P(None, "gz", "gy", "gx"), P(None, "gz", "gy", "gx"), P("gz", "gy", "gx"))
    out_specs = (P(None, "gz", "gy", "gx"), P(), P())

    def body(*args):
        return plan(sizes, *args)

    step = jax.shard_map(
        body, mesh=mesh, in_specs=in_specs, out_specs=out_specs, check_vma=False
    )
    if plan is any_mesh:
        return step
    return step
```

```python
import functools

import jax
import jax.numpy as jnp
import numpy as np
from jax import lax
from jax.experimental import pallas as pl
from jax.experimental.pallas import tpu as pltpu
from jax.sharding import PartitionSpec as P


ORDER = 7
PTS = ORDER + 1
F32 = jnp.float32
BF16 = jnp.bfloat16
SCALAR_ROWS = 8


def gll_derivative(poly_order):
    node_count = poly_order + 1
    abscissa = np.cos(np.pi * np.arange(node_count) / poly_order)
    legendre = np.zeros((node_count, node_count))
    for _ in range(60):
        legendre[:, 0] = 1.0
        legendre[:, 1] = abscissa
        for degree in range(2, node_count):
            legendre[:, degree] = (
                (2 * degree - 1) * abscissa * legendre[:, degree - 1]
                - (degree - 1) * legendre[:, degree - 2]
            ) / degree
        abscissa = abscissa - (abscissa * legendre[:, poly_order] - legendre[:, poly_order - 1]) / (
            node_count * legendre[:, poly_order]
        )
    abscissa = abscissa[::-1]
    end_values = legendre[::-1, poly_order]
    spacing = abscissa[:, None] - abscissa[None, :] + np.eye(node_count)
    deriv_table = end_values[:, None] / end_values[None, :] / spacing
    deriv_table = deriv_table * (1.0 - np.eye(node_count))
    deriv_table[0, 0] = -poly_order * node_count / 4.0
    deriv_table[poly_order, poly_order] = poly_order * node_count / 4.0
    return deriv_table.astype(np.float32)


def split(x):
    high = x.astype(BF16)
    return high, (x - high.astype(F32)).astype(BF16)


def iota(shape, dim):
    return lax.broadcasted_iota(jnp.int32, shape, dim)


def repeated(table, width):
    lane = iota((PTS, width), 1) % PTS
    rows = []
    for i in range(PTS):
        row = jnp.full((PTS, width), float(table[i, 0]), F32)
        for k in range(1, PTS):
            row = jnp.where(lane == k, float(table[i, k]), row)
        rows.append(row)
    return rows


def fine_matrix(table, size):
    sub = iota((PTS, size), 0)
    rows = repeated(table, size)
    tile = rows[0]
    for i in range(1, PTS):
        tile = jnp.where(sub == i, rows[i], tile)
    block = iota((PTS, size), 1) // PTS
    return split(
        jnp.concatenate(
            [jnp.where(block == e, tile, 0.0) for e in range(size // PTS)], axis=0
        )
    )


def combine_planes(planes, table):
    half = PTS // 2
    even = [planes[k] + planes[PTS - 1 - k] for k in range(half)]
    odd = [planes[k] - planes[PTS - 1 - k] for k in range(half)]
    low, high = [], []
    for w in range(half):
        p = q = None
        for k in range(half):
            a, b = float(table[w, k]), float(table[w, PTS - 1 - k])
            pe = np.float32((a + b) / 2) * even[k]
            qo = np.float32((a - b) / 2) * odd[k]
            p = pe if p is None else p + pe
            q = qo if q is None else q + qo
        low.append(p + q)
        high.append(q - p)
    return low + high[::-1]


def dot(a, b):
    return jnp.dot(a, b, preferred_element_type=F32)


def join_rows(tiles, sub):
    done = []
    for e, t in enumerate(tiles):
        if e + 1 < len(tiles):
            t = t + jnp.where(sub == PTS - 1, pltpu.roll(tiles[e + 1], PTS - 1, 0), 0.0)
        if e > 0:
            t = t + jnp.where(sub == 0, pltpu.roll(tiles[e - 1], 1, 0), 0.0)
        done.append(t)
    return done


def assemble_plane(u, ny, nx):
    lane = iota((PTS, nx), 1)
    sub = iota((PTS, nx), 0)
    last = (lane % PTS == PTS - 1) & (lane < nx - 1)
    first = (lane % PTS == 0) & (lane > 0)
    tiles = []
    for e in range(ny // PTS):
        t = u[e * PTS : (e + 1) * PTS]
        t = (
            t
            + jnp.where(last, pltpu.roll(t, nx - 1, 1), 0.0)
            + jnp.where(first, pltpu.roll(t, 1, 1), 0.0)
        )
        tiles.append(t)
    return jnp.concatenate(join_rows(tiles, sub), axis=0)


def joined(pieces):
    return pieces[0] if len(pieces) == 1 else joined(
        [sum(pieces[i : i + 2][1:], pieces[i]) for i in range(0, len(pieces), 2)]
    )


def across_rows(tile, columns):
    return joined(
        [column * jnp.broadcast_to(tile[k : k + 1], tile.shape) for k, column in enumerate(columns)]
    )


def row_columns(table, nx):
    sub = iota((PTS, nx), 0)
    columns = []
    for k in range(PTS):
        column = jnp.full((PTS, nx), float(table[0, k]), F32)
        for w in range(1, PTS):
            column = jnp.where(sub == w, float(table[w, k]), column)
        columns.append(column)
    return columns


def by_thrice(x, weights):
    high, low = split(x)
    out = dot(jnp.concatenate([high, low], axis=1), weights)
    half = weights.shape[1] // 2
    return out[:, 0:half] + out[:, half:]


def thrice(high, low):
    return jnp.concatenate(
        [
            jnp.concatenate([high, low], axis=1),
            jnp.concatenate([high, jnp.zeros_like(low)], axis=1),
        ],
        axis=0,
    )


def column_slot(lane, nx):
    return (lane + 1) % nx // 2


def packed_z_matrix(table, nx):
    into, out = iota((nx, nx), 0), iota((nx, nx), 1)
    j, k = column_slot(into, nx), column_slot(out, nx)
    value = jnp.zeros((nx, nx), F32)
    for w in range(PTS):
        row = jnp.zeros((nx, nx), F32)
        for q in range(PTS):
            row = jnp.where(k % PTS == q, float(table[w, q]), row)
        value = jnp.where(j % PTS == w, row, value)
    same = (j // PTS == k // PTS) & (into % 2 == out % 2)
    return jnp.where(same, value, 0.0)


def packed_x_matrix(table, nx):
    into, out = iota((nx, nx), 0), iota((nx, nx), 1)
    place, plane = into % (2 * PTS), into // (2 * PTS)
    value = jnp.zeros((nx, nx), F32)
    for w in range(PTS):
        value = jnp.where(place == w, float(table[w, PTS - 1]), value)
        value = jnp.where(place == PTS + w, float(table[w, 0]), value)
    target = jnp.where(place < PTS, (2 * plane - 1) % nx, 2 * plane)
    return jnp.where(out == target, value, 0.0)


def local_kernel(
    table,
    v_hbm,
    g_hbm,
    m_hbm,
    f_ref,
    px_ref,
    v_ref,
    m_ref,
    left_ref,
    right_ref,
    g_ref,
    grad_ref,
    high_ref,
    low_ref,
    sems,
):
    comps, nz, ny, nx = v_ref.shape
    layers = nz // PTS
    rows = PTS * ny
    half = 2 * PTS
    v_copies = []
    gm_copies = []
    for layer in range(layers):
        zs = pl.ds(layer * PTS, PTS)
        v_copies.append(
            pltpu.make_async_copy(v_hbm.at[:, zs], v_ref.at[:, zs], sems.at[layer, 0])
        )
        gm_copies.append(
            pltpu.make_async_copy(g_hbm.at[:, zs], g_ref.at[:, zs], sems.at[layer, 1])
        )
        gm_copies.append(pltpu.make_async_copy(m_hbm.at[zs], m_ref.at[zs], sems.at[layer, 2]))
    for copy in v_copies + gm_copies:
        copy.start()
    for i, matrix in enumerate((table, table.T)):
        h, l = fine_matrix(matrix, rows)
        left_ref[i] = jnp.concatenate([h, l, h], axis=1)
        right_ref[i] = thrice(*fine_matrix(matrix.T, nx))
    right_ref[2] = thrice(*split(packed_x_matrix(table, nx)))
    right_ref[3] = thrice(*split(packed_z_matrix(table, nx)))
    columns = row_columns(table.T, nx)
    blocks = [(layer, c) for layer in range(layers) for c in range(comps)]

    def planes(layer):
        return slice(layer * PTS, (layer + 1) * PTS)

    for copy in v_copies:
        copy.wait()
    for c in range(comps):
        for z in range(nz):
            high_ref[c, z], low_ref[c, z] = split(v_ref[c, z])
    for layer, c in blocks:
        grad_ref[0, c, planes(layer)] = along_x(right_ref[0], layer, c, high_ref, low_ref)
    for i in range(0, len(blocks), 2):
        pair = blocks[i : i + 2]
        for (layer, c), out in zip(pair, along_y(left_ref[0], pair, high_ref, low_ref)):
            grad_ref[1, c, planes(layer)] = out
    for layer, c in blocks:
        for e in range(0, ny, PTS):
            ys = slice(e, e + PTS)
            z0 = layer * PTS
            out = combine_planes([v_ref[c, z0 + z, ys] for z in range(PTS)], table)
            for z in range(PTS):
                grad_ref[2, c, z0 + z, ys] = out[z]
    for copy in gm_copies:
        copy.wait()
    lane = iota((PTS, nx), 1)
    slot, place = column_slot(lane, nx), lane // half

    def moved(x, shift):
        return pltpu.roll(x, shift, 1) if shift else x

    kin = jnp.zeros((half, nx), F32)
    ens = jnp.zeros((half, nx), F32)
    tiles = ny // PTS
    zero = jnp.zeros((PTS, nx), F32)
    packed_s, packed_t, packed_m = ([zero] * tiles for _ in range(3))
    groups = [[zero] * tiles for _ in range(comps * layers)]
    for y in range(0, ny, half):
        ys = slice(y, y + half)
        for z in range(nz):
            g = [g_ref[i, z, ys].astype(F32) for i in range(6)]
            mass = m_ref[z, ys].astype(F32)
            square = None
            for c in range(comps):
                v = v_ref[c, z, ys]
                square = v * v if square is None else square + v * v
                gr, gs, gt = (grad_ref[i, c, z, ys] for i in range(3))
                fr = g[0] * gr + g[3] * gs + g[4] * gt
                fs = g[3] * gr + g[1] * gs + g[5] * gt
                ft = g[4] * gr + g[5] * gs + g[2] * gt
                ens = ens + (gr * fr + gs * fs + gt * ft)
                f_ref[0, c, z, ys] = fr
                f_ref[1, c, z, ys] = fs
                f_ref[2, c, z, ys] = ft
                j = c * nz + z
                here, mine = slot == j, place == j % PTS
                for e in range(half // PTS):
                    t, rs = y // PTS + e, slice(e * PTS, (e + 1) * PTS)
                    packed_s[t] = jnp.where(here, moved(fs[rs], 2 * j), packed_s[t])
                    packed_t[t] = jnp.where(here, moved(ft[rs], 2 * j), packed_t[t])
                    part = moved(fr[rs], (PTS + half * (j % PTS)) % nx)
                    groups[j // PTS][t] = jnp.where(mine, part, groups[j // PTS][t])
            kin = kin + mass * square
            j = comps * nz + z
            for e in range(half // PTS):
                t, rs = y // PTS + e, slice(e * PTS, (e + 1) * PTS)
                packed_m[t] = jnp.where(slot == j, moved(mass[rs], 2 * j), packed_m[t])
    div_r = by_thrice(
        jnp.concatenate([jnp.concatenate(group, axis=0) for group in groups], axis=0),
        right_ref[2],
    )
    parts = [moved(div_r[q * ny : (q + 1) * ny], half * q) for q in range(len(groups))]
    parts.append(jnp.concatenate([across_rows(t, columns) for t in packed_s], axis=0))
    parts.append(by_thrice(jnp.concatenate(packed_t, axis=0), right_ref[3]))
    parts.append(jnp.concatenate(packed_m, axis=0))
    px_ref[0:ny] = join_columns(joined(parts), nz)
    row = iota((SCALAR_ROWS, nx), 0)
    kin, ens = jnp.sum(kin, axis=0, keepdims=True), jnp.sum(ens, axis=0, keepdims=True)
    px_ref[ny:] = jnp.where(row == 0, kin, jnp.where(row == 1, ens, 0.0))


def join_columns(packed, nz):
    ny, nx = packed.shape
    packed = jnp.concatenate(
        join_rows([packed[e : e + PTS] for e in range(0, ny, PTS)], iota((PTS, nx), 0)), axis=0
    )
    plane = column_slot(iota((ny, nx), 1), nx) % nz
    up = (plane % PTS == PTS - 1) & (plane < nz - 1)
    down = (plane % PTS == 0) & (plane > 0)
    return (
        packed
        + jnp.where(up, pltpu.roll(packed, nx - 2, 1), 0.0)
        + jnp.where(down, pltpu.roll(packed, 2, 1), 0.0)
    )


def along_y(left, pair, high_ref, low_ref):
    _, _, ny, nx = high_ref.shape
    rows = PTS * ny

    def wide(ref):
        return jnp.concatenate(
            [ref[c, layer * PTS : (layer + 1) * PTS].reshape(rows, nx) for layer, c in pair],
            axis=1,
        )

    high, low = wide(high_ref), wide(low_ref)
    out = dot(left, jnp.concatenate([high, high, low], axis=0))
    return [out[:, n * nx : (n + 1) * nx].reshape(PTS, ny, nx) for n in range(len(pair))]


def along_x(right, layer, c, high_ref, low_ref):
    _, _, ny, nx = high_ref.shape
    zs = slice(layer * PTS, (layer + 1) * PTS)
    high = high_ref[c, zs].reshape(PTS * ny, nx)
    low = low_ref[c, zs].reshape(PTS * ny, nx)
    out = dot(jnp.concatenate([high, low], axis=1), right)
    return (out[:, 0:nx] + out[:, nx : 2 * nx]).reshape(PTS, ny, nx)


def plane_kernel(table, f_ref, m_ref, right_ref, px_ref, zp_ref, edge_ref):
    _, comps, nz, ny, nx = f_ref.shape
    z_even = lax.axis_index("gz") % 2 == 0
    at = jnp.where(z_even, nz - 1, 0)
    z0 = jnp.where(z_even, nz - PTS, 0)
    weights = [
        jnp.where(z_even, float(table[w, PTS - 1]), float(table[w, 0])) for w in range(PTS)
    ]
    columns = row_columns(table.T, nx)
    tall = jnp.concatenate([f_ref[0, c, at] for c in range(comps)], axis=0)
    div_r = by_thrice(tall, right_ref[1])
    for c in range(comps):
        flux_s = f_ref[1, c, at]
        div_s = [across_rows(flux_s[e : e + PTS], columns) for e in range(0, ny, PTS)]
        div_t = joined([weights[w] * f_ref[2, c, z0 + w] for w in range(PTS)])
        total = div_r[c * ny : (c + 1) * ny] + jnp.concatenate(div_s, axis=0) + div_t
        zp_ref[c] = assemble_plane(total, ny, nx)
    zp_ref[comps] = assemble_plane(m_ref[at].astype(F32), ny, nx)
    lane = iota((PTS, nx), 1)
    edge = None
    for e in range(ny // PTS):
        t = px_ref[e * PTS : (e + 1) * PTS]
        t = jnp.where(z_even, pltpu.roll(t, nx - 2 * (nz - 1), 1), t)
        t = pltpu.roll(t, 2 * e, 1) if e else t
        mine = (lane + 1) % nx // 2 % nz == e
        edge = jnp.where(mine, t, 0.0 if edge is None else edge)
    edge_ref[...] = edge


def diverge_kernel(
    table, f_ref, m_ref, left_ref, right_ref, w_ref, ends_ref, high_ref, low_ref, y_ref, x_ref
):
    _, comps, nz, ny, nx = f_ref.shape
    blocks = [(layer, c) for layer in range(nz // PTS) for c in range(comps)]
    for c in range(comps):
        for z in range(nz):
            high_ref[0, c, z], low_ref[0, c, z] = split(f_ref[0, c, z])
            high_ref[1, c, z], low_ref[1, c, z] = split(f_ref[1, c, z])
    for i in range(0, len(blocks), 2):
        pair = blocks[i : i + 2]
        sums = along_y(left_ref[1], pair, high_ref.at[1], low_ref.at[1])
        for (layer, c), out in zip(pair, sums):
            y_ref[c, layer * PTS : (layer + 1) * PTS] = out
    for layer, c in blocks:
        x_ref[c, layer * PTS : (layer + 1) * PTS] = along_x(
            right_ref[1], layer, c, high_ref.at[0], low_ref.at[0]
        )
    for layer, c in blocks:
        for e in range(0, ny, PTS):
            ys = slice(e, e + PTS)
            z0 = layer * PTS
            out = combine_planes([f_ref[2, c, z0 + z, ys] for z in range(PTS)], table.T)
            for z in range(PTS):
                y_ref[c, z0 + z, ys] = out[z] + y_ref[c, z0 + z, ys] + x_ref[c, z0 + z, ys]
    for f in range(comps + 1):
        for z in range(nz):
            j = ends_ref.shape[1] - 1 - f * nz - z
            if z % PTS == 0 and z > 0:
                w_ref[f, z] = w_ref[f, z - 1]
                ends_ref[:, j] = ends_ref[:, j + 1]
                continue
            at = [z, z + 1] if z % PTS == PTS - 1 and z < nz - 1 else [z]
            t = [m_ref[i].astype(F32) if f == comps else y_ref[f, i] for i in at]
            whole = assemble_plane(joined(t), ny, nx)
            w_ref[f, z] = whole
            ends_ref[0, j : j + 1] = whole[0:1]
            ends_ref[1, j : j + 1] = whole[ny - 1 : ny]


def merge_sides(right, left):
    lane = iota(right.shape, 1)
    return jnp.where(lane % 2 == 0, right, pltpu.roll(left, 2, 1))


def place_columns(merged, j, nx):
    lane = iota(merged.shape, 1)
    shift = (nx - 1 - 2 * j) % nx
    moved = pltpu.roll(merged, shift, 1) if shift else merged
    return jnp.where((lane == 0) | (lane == nx - 1), moved, 0.0)


def first_kernel(zp_ref, edge_ref, px_ref, qa_ref, pb_ref, pz_ref, pd_ref):
    fields, ny, nx = zp_ref.shape
    nz = nx // (2 * fields)
    x_even = lax.axis_index("gx") % 2 == 0
    z_even = lax.axis_index("gz") % 2 == 0
    qa = qa_ref[0:ny]
    merged = merge_sides(jnp.where(x_even, qa, 0.0), jnp.where(x_even, 0.0, qa))
    merged = jnp.where(z_even, pltpu.roll(merged, nx - 2 * (nz - 1), 1), merged)
    sums = px_ref[ny:] + qa_ref[ny:]
    pb_ref[0:ny] = px_ref[0:ny]
    pb_ref[ny:] = sums
    for f in range(fields):
        pz_ref[f * ny : (f + 1) * ny] = zp_ref[f] + place_columns(merged, f * nz, nx)
    pz_ref[fields * ny :] = sums
    pd_ref[0:PTS] = edge_ref[...]
    pd_ref[PTS:] = sums


def x_sides(qa, qb, x_even):
    return merge_sides(jnp.where(x_even, qa, qb), jnp.where(x_even, qb, qa))


def diagonal_sides(qd, x_even):
    return merge_sides(jnp.where(x_even, 0.0, qd), jnp.where(x_even, qd, 0.0))


def spread_columns(merged, count):
    nx = merged.shape[1]
    rows = jnp.broadcast_to(merged, (count, nx))
    rows = pltpu.roll(rows, (nx + 1 - 2 * count) % nx, 1, stride=2, stride_axis=0)
    lane = iota((count, nx), 1)
    return jnp.where((lane == 0) | (lane == nx - 1), rows, 0.0)


def second_kernel(
    ends_ref, pb_ref, qa_ref, qb_ref, qz_ref, qd_ref, pya_ref, pyb_ref, ps_ref, low_ref, high_ref
):
    _, count, nx = ends_ref.shape
    ny = pb_ref.shape[0] - SCALAR_ROWS
    fields = (qz_ref.shape[0] - SCALAR_ROWS) // ny
    nz = count // fields
    x_even = lax.axis_index("gx") % 2 == 0
    y_even = lax.axis_index("gy") % 2 == 0
    diag = diagonal_sides(qd_ref[0:PTS], x_even)
    for i, (y, out) in enumerate(((0, low_ref), (ny - 1, high_ref))):
        merged = x_sides(qa_ref[y : y + 1], qb_ref[y : y + 1], x_even)
        out[...] = ends_ref[i] + spread_columns(merged, count)
        for f in range(fields):
            corner = place_columns(diag, f * nz + y // PTS, nx)[y % PTS : y % PTS + 1]
            extra = qz_ref[f * ny + y : f * ny + y + 1] + corner
            for z in (0, nz - 1):
                j = count - 1 - f * nz - z
                out[j : j + 1] = out[j : j + 1] + extra
    sums = pb_ref[ny:] + qb_ref[ny:] + qz_ref[fields * ny :] + qd_ref[PTS:]
    pya_ref[0:count] = jnp.where(y_even, high_ref[...], low_ref[...])
    pyb_ref[0:count] = jnp.where(y_even, low_ref[...], high_ref[...])
    pya_ref[count:] = sums
    pyb_ref[count:] = sums
    ps_ref[...] = sums


def correct_kernel(v_ref, u_ref, qa_ref, qb_ref, qz_ref, qd_ref, w_ref, mv_ref):
    fields, nz, ny, nx = u_ref.shape
    x_even = lax.axis_index("gx") % 2 == 0
    merged = x_sides(qa_ref[0:ny], qb_ref[0:ny], x_even)
    diag = diagonal_sides(qd_ref[0:PTS], x_even)
    for z in range(nz):
        for f in range(fields):
            t = u_ref[f, z] + place_columns(merged, f * nz + z, nx)
            if z in (0, nz - 1):
                t = t + qz_ref[f * ny : (f + 1) * ny]
                corner = [place_columns(diag, f * nz + e, nx) for e in range(ny // PTS)]
                t = t + jnp.concatenate(corner, axis=0)
            w_ref[f, z] = t
        for c in range(fields - 1):
            mv_ref[c, z] = w_ref[fields - 1, z] * v_ref[c, z]


def last_kernel(
    sizes,
    v_ref,
    w_ref,
    mv_ref,
    qya_ref,
    qyb_ref,
    qs_ref,
    ps_ref,
    out_hbm,
    kin_hbm,
    ens_hbm,
    low_ref,
    high_ref,
    out_ref,
    kin_ref,
    ens_ref,
    sems,
):
    fields, nz, ny, nx = w_ref.shape
    gx, gy, gz = (lax.axis_index(name) for name in ("gx", "gy", "gz"))
    y_even = gy % 2 == 0
    count = fields * nz
    sums = ps_ref[...] + qya_ref[count:] + qyb_ref[count:] + qs_ref[...]
    kinetic = 0.5 * jnp.sum(sums[0:1])
    enstrophy = jnp.sum(sums[1:2])
    kin_ref[0, 0] = kinetic
    ens_ref[0, 0] = enstrophy
    copies = [
        pltpu.make_async_copy(kin_ref, kin_hbm, sems.at[4]),
        pltpu.make_async_copy(ens_ref, ens_hbm, sems.at[5]),
    ]
    for copy in copies:
        copy.start()
    rayleigh = jnp.full((PTS, nx), enstrophy, F32) / jnp.full((PTS, nx), 2.0 * kinetic, F32)
    low_ref[...] = jnp.where(y_even, qyb_ref[0:count], qya_ref[0:count])
    high_ref[...] = jnp.where(y_even, qya_ref[0:count], qyb_ref[0:count])
    row = iota((ny, nx), 0)
    lane = iota((ny, nx), 1)
    x_first = jnp.where(gx == 0, 0, -1)
    x_last = jnp.where(gx == sizes[0] - 1, nx - 1, -1)
    y_first = jnp.where(gy == 0, 0, -1)
    y_last = jnp.where(gy == sizes[1] - 1, ny - 1, -1)
    inside = (lane != x_first) & (lane != x_last) & (row != y_first) & (row != y_last)
    sub = iota((PTS, nx), 0)
    steps = nz // 4
    for z in range(nz):
        keep = inside
        if z == 0:
            keep = keep & (gz > 0)
        if z == nz - 1:
            keep = keep & (gz < sizes[2] - 1)
        for e in range(0, ny, PTS):
            ys = slice(e, e + PTS)
            edge = e == 0 or e == ny - PTS
            side, at = (low_ref, 0) if e == 0 else (high_ref, PTS - 1)
            if edge:
                j = nz - 1 - z
                extra = rayleigh * jnp.where(sub == at, side[j : j + 1], 0.0)
            for c in range(fields - 1):
                t = w_ref[c, z, ys] - rayleigh * mv_ref[c, z, ys]
                if edge:
                    j = count - 1 - c * nz - z
                    t = t + jnp.where(sub == at, side[j : j + 1], 0.0)
                    t = t - extra * v_ref[c, z, ys]
                out_ref[c, z, ys] = jnp.where(keep[ys], t, 0.0)
        if z % steps == steps - 1:
            zs = pl.ds(z - steps + 1, steps)
            copies.append(
                pltpu.make_async_copy(
                    out_ref.at[:, zs], out_hbm.at[:, zs], sems.at[z // steps]
                )
            )
            copies[-1].start()
    for copy in copies:
        copy.wait()


VMEM = pl.BlockSpec(memory_space=pltpu.VMEM)
HBM = pl.BlockSpec(memory_space=pltpu.HBM)


def call(kernel, outs, ins, scratch=(), out_specs=None, in_specs=None, flops=1 << 20):
    return pl.pallas_call(
        kernel,
        out_shape=[
            out if hasattr(out, "dtype") else jax.ShapeDtypeStruct(out, F32) for out in outs
        ],
        in_specs=in_specs or [VMEM] * len(ins),
        out_specs=out_specs or [VMEM] * len(outs),
        scratch_shapes=list(scratch),
        compiler_params=pltpu.CompilerParams(vmem_limit_bytes=24 << 20),
        cost_estimate=pl.CostEstimate(flops=flops, bytes_accessed=flops, transcendentals=0),
    )(*ins)


def local_part(table, velocity, geometry, mass_weights):
    _, nz, ny, nx = velocity.shape
    rows = PTS * ny
    vector = (3, *velocity.shape)
    return call(
        functools.partial(local_kernel, table),
        [
            vector,
            (ny + SCALAR_ROWS, nx),
            velocity.shape,
            jax.ShapeDtypeStruct(mass_weights.shape, BF16),
            jax.ShapeDtypeStruct((2, rows, 3 * rows), BF16),
            jax.ShapeDtypeStruct((4, 2 * nx, 2 * nx), BF16),
        ],
        [
            pltpu.with_memory_space_constraint(x, pltpu.HBM)
            for x in (velocity, geometry, mass_weights)
        ],
        in_specs=[HBM] * 3,
        scratch=[
            pltpu.VMEM(geometry.shape, BF16),
            pltpu.VMEM(vector, F32),
            pltpu.VMEM(velocity.shape, BF16),
            pltpu.VMEM(velocity.shape, BF16),
            pltpu.SemaphoreType.DMA((nz // PTS, 3)),
        ],
    )


def diverged(table, fluxes, mass, left, right):
    _, comps, nz, ny, nx = fluxes.shape
    return call(
        functools.partial(diverge_kernel, table),
        [(comps + 1, nz, ny, nx), (2, (comps + 1) * nz, nx)],
        [fluxes, mass, left, right],
        scratch=[
            pltpu.VMEM((2, comps, nz, ny, nx), BF16),
            pltpu.VMEM((2, comps, nz, ny, nx), BF16),
            pltpu.VMEM((comps, nz, ny, nx), F32),
            pltpu.VMEM((comps, nz, ny, nx), F32),
        ],
    )


def pairs_near(count):
    return [(i, i ^ 1) for i in range(count)]


def pairs_mirror(count):
    return [(i, count - 1 - i) for i in range(count)]


def few_rounds(sizes, velocity, geometry, mass_weights):
    comps, nz, ny, nx = velocity.shape
    fields = comps + 1
    table = gll_derivative(ORDER)
    fluxes, px, held, mass, left, right = local_part(table, velocity, geometry, mass_weights)
    qa = lax.ppermute(px, "gx", pairs_near(sizes[0]))
    zp, edge = call(
        functools.partial(plane_kernel, table),
        [(fields, ny, nx), (PTS, nx)],
        [fluxes, mass, right, px],
    )
    pb, pz, pd = call(
        first_kernel,
        [
            (ny + SCALAR_ROWS, nx),
            (fields * ny + SCALAR_ROWS, nx),
            (PTS + SCALAR_ROWS, nx),
        ],
        [zp, edge, px, qa],
    )
    mirror = pairs_mirror(sizes[0])
    qb = lax.ppermute(pb, "gx", mirror)
    qz = lax.ppermute(pz, "gz", pairs_near(sizes[2]))
    both = [
        (i * sizes[2] + k, mirror[i][1] * sizes[2] + (k ^ 1))
        for i in range(sizes[0])
        for k in range(sizes[2])
    ]
    qd = lax.ppermute(pd, ("gx", "gz"), both)
    u, ends = diverged(table, fluxes, mass, left, right)
    count = fields * nz
    pya, pyb, ps = call(
        second_kernel,
        [(count + SCALAR_ROWS, nx), (count + SCALAR_ROWS, nx), (SCALAR_ROWS, nx)],
        [ends, pb, qa, qb, qz, qd],
        scratch=[pltpu.VMEM((count, nx), F32)] * 2,
    )
    apart = [
        (i * sizes[1] + j, (i ^ 1) * sizes[1] + (j ^ 2))
        for i in range(sizes[0])
        for j in range(sizes[1])
    ]
    qya = lax.ppermute(pya, "gy", pairs_near(sizes[1]))
    qyb = lax.ppermute(pyb, "gy", pairs_mirror(sizes[1]))
    qs = lax.ppermute(ps, ("gx", "gy"), apart)
    w, mv = call(correct_kernel, [u.shape, velocity.shape], [held, u, qa, qb, qz, qd])
    residual, kinetic, enstrophy = call(
        functools.partial(last_kernel, sizes),
        [velocity.shape, (1, 1), (1, 1)],
        [held, w, mv, qya, qyb, qs, ps],
        scratch=[
            pltpu.VMEM((count, nx), F32),
            pltpu.VMEM((count, nx), F32),
            pltpu.VMEM(velocity.shape, F32),
            pltpu.SMEM((1, 1), F32),
            pltpu.SMEM((1, 1), F32),
            pltpu.SemaphoreType.DMA((6,)),
        ],
        out_specs=[HBM, HBM, HBM],
    )
    return residual, kinetic[0, 0], enstrophy[0, 0]


def add_neighbours(field, axis, dim):
    count = lax.axis_size(axis)
    extent = field.shape[dim]
    first = lax.slice_in_dim(field, 0, 1, axis=dim)
    last = lax.slice_in_dim(field, extent - 1, extent, axis=dim)
    low = lax.ppermute(last, axis, [(i, i + 1) for i in range(count - 1)])
    high = lax.ppermute(first, axis, [(i + 1, i) for i in range(count - 1)])
    middle = lax.slice_in_dim(field, 1, extent - 1, axis=dim)
    return jnp.concatenate([first + low, middle, last + high], axis=dim)


def any_mesh(sizes, velocity, geometry, mass_weights):
    comps, nz, ny, nx = velocity.shape
    table = gll_derivative(ORDER)
    fluxes, px, _, mass, left, right = local_part(table, velocity, geometry, mass_weights)
    u, _ = diverged(table, fluxes, mass, left, right)
    kinetic = 0.5 * jnp.sum(px[ny])
    enstrophy = jnp.sum(px[ny + 1])
    kinetic, enstrophy = lax.psum((kinetic, enstrophy), ("gx", "gy", "gz"))
    for axis, dim in (("gx", 3), ("gy", 2), ("gz", 1)):
        u = add_neighbours(u, axis, dim)
    inside = jnp.ones((nz, ny, nx), bool)
    for dim, (axis, size) in enumerate(zip(("gz", "gy", "gx"), sizes[::-1])):
        place = lax.axis_index(axis) * inside.shape[dim] + iota(inside.shape, dim)
        inside = inside & (place > 0) & (place < size * inside.shape[dim] - 1)
    rayleigh = enstrophy / (2.0 * kinetic)
    residual = jnp.where(inside[None], u[:comps] - rayleigh * u[comps][None] * velocity, 0.0)
    return residual, kinetic, enstrophy


def solution(mesh):
    sizes = tuple(mesh.shape[name] for name in ("gx", "gy", "gz"))
    plan = few_rounds if sizes == (4, 4, 2) else any_mesh
    in_specs = (P(None, "gz", "gy", "gx"), P(None, "gz", "gy", "gx"), P("gz", "gy", "gx"))
    out_specs = (P(None, "gz", "gy", "gx"), P(), P())

    def body(*args):
        return plan(sizes, *args)

    step = jax.shard_map(
        body, mesh=mesh, in_specs=in_specs, out_specs=out_specs, check_vma=False
    )
    if plan is any_mesh:
        return step
    return step
```

```python
import functools

import jax
import jax.numpy as jnp
import numpy as np
from jax import lax
from jax.experimental import pallas as pl
from jax.experimental.pallas import tpu as pltpu
from jax.sharding import PartitionSpec as P


ORDER = 7
PTS = ORDER + 1
F32 = jnp.float32
BF16 = jnp.bfloat16
SCALAR_ROWS = 8


def gll_derivative(poly_order):
    node_count = poly_order + 1
    abscissa = np.cos(np.pi * np.arange(node_count) / poly_order)
    legendre = np.zeros((node_count, node_count))
    for _ in range(60):
        legendre[:, 0] = 1.0
        legendre[:, 1] = abscissa
        for degree in range(2, node_count):
            legendre[:, degree] = (
                (2 * degree - 1) * abscissa * legendre[:, degree - 1]
                - (degree - 1) * legendre[:, degree - 2]
            ) / degree
        abscissa = abscissa - (abscissa * legendre[:, poly_order] - legendre[:, poly_order - 1]) / (
            node_count * legendre[:, poly_order]
        )
    abscissa = abscissa[::-1]
    end_values = legendre[::-1, poly_order]
    spacing = abscissa[:, None] - abscissa[None, :] + np.eye(node_count)
    deriv_table = end_values[:, None] / end_values[None, :] / spacing
    deriv_table = deriv_table * (1.0 - np.eye(node_count))
    deriv_table[0, 0] = -poly_order * node_count / 4.0
    deriv_table[poly_order, poly_order] = poly_order * node_count / 4.0
    return deriv_table.astype(np.float32)


def split(x):
    high = x.astype(BF16)
    return high, (x - high.astype(F32)).astype(BF16)


def iota(shape, dim):
    return lax.broadcasted_iota(jnp.int32, shape, dim)


def repeated(table, width):
    lane = iota((PTS, width), 1) % PTS
    rows = []
    for i in range(PTS):
        row = jnp.full((PTS, width), float(table[i, 0]), F32)
        for k in range(1, PTS):
            row = jnp.where(lane == k, float(table[i, k]), row)
        rows.append(row)
    return rows


def fine_matrix(table, size):
    sub = iota((PTS, size), 0)
    rows = repeated(table, size)
    tile = rows[0]
    for i in range(1, PTS):
        tile = jnp.where(sub == i, rows[i], tile)
    block = iota((PTS, size), 1) // PTS
    return split(
        jnp.concatenate(
            [jnp.where(block == e, tile, 0.0) for e in range(size // PTS)], axis=0
        )
    )


def combine_planes(planes, table):
    half = PTS // 2
    even = [planes[k] + planes[PTS - 1 - k] for k in range(half)]
    odd = [planes[k] - planes[PTS - 1 - k] for k in range(half)]
    low, high = [], []
    for w in range(half):
        p = q = None
        for k in range(half):
            a, b = float(table[w, k]), float(table[w, PTS - 1 - k])
            pe = np.float32((a + b) / 2) * even[k]
            qo = np.float32((a - b) / 2) * odd[k]
            p = pe if p is None else p + pe
            q = qo if q is None else q + qo
        low.append(p + q)
        high.append(q - p)
    return low + high[::-1]


def dot(a, b):
    return jnp.dot(a, b, preferred_element_type=F32)


def join_rows(tiles, sub):
    done = []
    for e, t in enumerate(tiles):
        if e + 1 < len(tiles):
            t = t + jnp.where(sub == PTS - 1, pltpu.roll(tiles[e + 1], PTS - 1, 0), 0.0)
        if e > 0:
            t = t + jnp.where(sub == 0, pltpu.roll(tiles[e - 1], 1, 0), 0.0)
        done.append(t)
    return done


def assemble_plane(u, ny, nx):
    lane = iota((PTS, nx), 1)
    sub = iota((PTS, nx), 0)
    last = (lane % PTS == PTS - 1) & (lane < nx - 1)
    first = (lane % PTS == 0) & (lane > 0)
    tiles = []
    for e in range(ny // PTS):
        t = u[e * PTS : (e + 1) * PTS]
        t = (
            t
            + jnp.where(last, pltpu.roll(t, nx - 1, 1), 0.0)
            + jnp.where(first, pltpu.roll(t, 1, 1), 0.0)
        )
        tiles.append(t)
    return jnp.concatenate(join_rows(tiles, sub), axis=0)


def joined(pieces):
    return pieces[0] if len(pieces) == 1 else joined(
        [sum(pieces[i : i + 2][1:], pieces[i]) for i in range(0, len(pieces), 2)]
    )


def across_rows(tile, columns):
    return joined(
        [column * jnp.broadcast_to(tile[k : k + 1], tile.shape) for k, column in enumerate(columns)]
    )


def row_columns(table, nx):
    sub = iota((PTS, nx), 0)
    columns = []
    for k in range(PTS):
        column = jnp.full((PTS, nx), float(table[0, k]), F32)
        for w in range(1, PTS):
            column = jnp.where(sub == w, float(table[w, k]), column)
        columns.append(column)
    return columns


def by_thrice(x, weights):
    high, low = split(x)
    out = dot(jnp.concatenate([high, low], axis=1), weights)
    half = weights.shape[1] // 2
    return out[:, 0:half] + out[:, half:]


def thrice(high, low):
    return jnp.concatenate(
        [
            jnp.concatenate([high, low], axis=1),
            jnp.concatenate([high, jnp.zeros_like(low)], axis=1),
        ],
        axis=0,
    )


def column_slot(lane, nx):
    return (lane + 1) % nx // 2


def packed_z_matrix(table, nx):
    into, out = iota((nx, nx), 0), iota((nx, nx), 1)
    j, k = column_slot(into, nx), column_slot(out, nx)
    value = jnp.zeros((nx, nx), F32)
    for w in range(PTS):
        row = jnp.zeros((nx, nx), F32)
        for q in range(PTS):
            row = jnp.where(k % PTS == q, float(table[w, q]), row)
        value = jnp.where(j % PTS == w, row, value)
    same = (j // PTS == k // PTS) & (into % 2 == out % 2)
    return jnp.where(same, value, 0.0)


def packed_x_matrix(table, nx):
    into, out = iota((nx, nx), 0), iota((nx, nx), 1)
    place, plane = into % (2 * PTS), into // (2 * PTS)
    value = jnp.zeros((nx, nx), F32)
    for w in range(PTS):
        value = jnp.where(place == w, float(table[w, PTS - 1]), value)
        value = jnp.where(place == PTS + w, float(table[w, 0]), value)
    target = jnp.where(place < PTS, (2 * plane - 1) % nx, 2 * plane)
    return jnp.where(out == target, value, 0.0)


def local_kernel(
    table,
    v_hbm,
    g_hbm,
    m_hbm,
    f_ref,
    px_ref,
    v_ref,
    m_ref,
    left_ref,
    right_ref,
    g_ref,
    grad_ref,
    high_ref,
    low_ref,
    sems,
):
    comps, nz, ny, nx = v_ref.shape
    layers = nz // PTS
    rows = PTS * ny
    half = 2 * PTS
    v_copies = []
    gm_copies = []
    for layer in range(layers):
        zs = pl.ds(layer * PTS, PTS)
        v_copies.append(
            pltpu.make_async_copy(v_hbm.at[:, zs], v_ref.at[:, zs], sems.at[layer, 0])
        )
        gm_copies.append(
            pltpu.make_async_copy(g_hbm.at[:, zs], g_ref.at[:, zs], sems.at[layer, 1])
        )
        gm_copies.append(pltpu.make_async_copy(m_hbm.at[zs], m_ref.at[zs], sems.at[layer, 2]))
    for copy in v_copies + gm_copies:
        copy.start()
    for i, matrix in enumerate((table, table.T)):
        h, l = fine_matrix(matrix, rows)
        left_ref[i] = jnp.concatenate([h, l, h], axis=1)
        right_ref[i] = thrice(*fine_matrix(matrix.T, nx))
    right_ref[2] = thrice(*split(packed_x_matrix(table, nx)))
    right_ref[3] = thrice(*split(packed_z_matrix(table, nx)))
    columns = row_columns(table.T, nx)
    blocks = [(layer, c) for layer in range(layers) for c in range(comps)]

    def planes(layer):
        return slice(layer * PTS, (layer + 1) * PTS)

    for copy in v_copies:
        copy.wait()
    for c in range(comps):
        for z in range(nz):
            high_ref[c, z], low_ref[c, z] = split(v_ref[c, z])
    for layer, c in blocks:
        grad_ref[0, c, planes(layer)] = along_x(right_ref[0], layer, c, high_ref, low_ref)
    for i in range(0, len(blocks), 2):
        pair = blocks[i : i + 2]
        for (layer, c), out in zip(pair, along_y(left_ref[0], pair, high_ref, low_ref)):
            grad_ref[1, c, planes(layer)] = out
    for layer, c in blocks:
        for e in range(0, ny, PTS):
            ys = slice(e, e + PTS)
            z0 = layer * PTS
            out = combine_planes([v_ref[c, z0 + z, ys] for z in range(PTS)], table)
            for z in range(PTS):
                grad_ref[2, c, z0 + z, ys] = out[z]
    for copy in gm_copies:
        copy.wait()
    lane = iota((PTS, nx), 1)
    slot, place = column_slot(lane, nx), lane // half

    def moved(x, shift):
        return pltpu.roll(x, shift, 1) if shift else x

    kin = jnp.zeros((half, nx), F32)
    ens = jnp.zeros((half, nx), F32)
    tiles = ny // PTS
    zero = jnp.zeros((PTS, nx), F32)
    packed_s, packed_t, packed_m = ([zero] * tiles for _ in range(3))
    groups = [[zero] * tiles for _ in range(comps * layers)]
    for y in range(0, ny, half):
        ys = slice(y, y + half)
        for z in range(nz):
            g = [g_ref[i, z, ys].astype(F32) for i in range(6)]
            mass = m_ref[z, ys].astype(F32)
            square = None
            for c in range(comps):
                v = v_ref[c, z, ys]
                square = v * v if square is None else square + v * v
                gr, gs, gt = (grad_ref[i, c, z, ys] for i in range(3))
                fr = g[0] * gr + g[3] * gs + g[4] * gt
                fs = g[3] * gr + g[1] * gs + g[5] * gt
                ft = g[4] * gr + g[5] * gs + g[2] * gt
                ens = ens + (gr * fr + gs * fs + gt * ft)
                f_ref[0, c, z, ys] = fr
                f_ref[1, c, z, ys] = fs
                f_ref[2, c, z, ys] = ft
                j = c * nz + z
                here, mine = slot == j, place == j % PTS
                for e in range(half // PTS):
                    t, rs = y // PTS + e, slice(e * PTS, (e + 1) * PTS)
                    packed_s[t] = jnp.where(here, moved(fs[rs], 2 * j), packed_s[t])
                    packed_t[t] = jnp.where(here, moved(ft[rs], 2 * j), packed_t[t])
                    part = moved(fr[rs], (PTS + half * (j % PTS)) % nx)
                    groups[j // PTS][t] = jnp.where(mine, part, groups[j // PTS][t])
            kin = kin + mass * square
            j = comps * nz + z
            for e in range(half // PTS):
                t, rs = y // PTS + e, slice(e * PTS, (e + 1) * PTS)
                packed_m[t] = jnp.where(slot == j, moved(mass[rs], 2 * j), packed_m[t])
    div_r = by_thrice(
        jnp.concatenate([jnp.concatenate(group, axis=0) for group in groups], axis=0),
        right_ref[2],
    )
    parts = [moved(div_r[q * ny : (q + 1) * ny], half * q) for q in range(len(groups))]
    parts.append(jnp.concatenate([across_rows(t, columns) for t in packed_s], axis=0))
    parts.append(by_thrice(jnp.concatenate(packed_t, axis=0), right_ref[3]))
    parts.append(jnp.concatenate(packed_m, axis=0))
    px_ref[0:ny] = join_columns(joined(parts), nz)
    row = iota((SCALAR_ROWS, nx), 0)
    kin, ens = jnp.sum(kin, axis=0, keepdims=True), jnp.sum(ens, axis=0, keepdims=True)
    px_ref[ny:] = jnp.where(row == 0, kin, jnp.where(row == 1, ens, 0.0))


def join_columns(packed, nz):
    ny, nx = packed.shape
    packed = jnp.concatenate(
        join_rows([packed[e : e + PTS] for e in range(0, ny, PTS)], iota((PTS, nx), 0)), axis=0
    )
    plane = column_slot(iota((ny, nx), 1), nx) % nz
    up = (plane % PTS == PTS - 1) & (plane < nz - 1)
    down = (plane % PTS == 0) & (plane > 0)
    return (
        packed
        + jnp.where(up, pltpu.roll(packed, nx - 2, 1), 0.0)
        + jnp.where(down, pltpu.roll(packed, 2, 1), 0.0)
    )


def along_y(left, pair, high_ref, low_ref):
    _, _, ny, nx = high_ref.shape
    rows = PTS * ny

    def wide(ref):
        return jnp.concatenate(
            [ref[c, layer * PTS : (layer + 1) * PTS].reshape(rows, nx) for layer, c in pair],
            axis=1,
        )

    high, low = wide(high_ref), wide(low_ref)
    out = dot(left, jnp.concatenate([high, high, low], axis=0))
    return [out[:, n * nx : (n + 1) * nx].reshape(PTS, ny, nx) for n in range(len(pair))]


def along_x(right, layer, c, high_ref, low_ref):
    _, _, ny, nx = high_ref.shape
    zs = slice(layer * PTS, (layer + 1) * PTS)
    high = high_ref[c, zs].reshape(PTS * ny, nx)
    low = low_ref[c, zs].reshape(PTS * ny, nx)
    out = dot(jnp.concatenate([high, low], axis=1), right)
    return (out[:, 0:nx] + out[:, nx : 2 * nx]).reshape(PTS, ny, nx)


def plane_kernel(table, f_ref, m_ref, right_ref, px_ref, zp_ref, edge_ref):
    _, comps, nz, ny, nx = f_ref.shape
    z_even = lax.axis_index("gz") % 2 == 0
    at = jnp.where(z_even, nz - 1, 0)
    z0 = jnp.where(z_even, nz - PTS, 0)
    weights = [
        jnp.where(z_even, float(table[w, PTS - 1]), float(table[w, 0])) for w in range(PTS)
    ]
    columns = row_columns(table.T, nx)
    tall = jnp.concatenate([f_ref[0, c, at] for c in range(comps)], axis=0)
    div_r = by_thrice(tall, right_ref[1])
    for c in range(comps):
        flux_s = f_ref[1, c, at]
        div_s = [across_rows(flux_s[e : e + PTS], columns) for e in range(0, ny, PTS)]
        div_t = joined([weights[w] * f_ref[2, c, z0 + w] for w in range(PTS)])
        total = div_r[c * ny : (c + 1) * ny] + jnp.concatenate(div_s, axis=0) + div_t
        zp_ref[c] = assemble_plane(total, ny, nx)
    zp_ref[comps] = assemble_plane(m_ref[at].astype(F32), ny, nx)
    lane = iota((PTS, nx), 1)
    edge = None
    for e in range(ny // PTS):
        t = px_ref[e * PTS : (e + 1) * PTS]
        t = jnp.where(z_even, pltpu.roll(t, nx - 2 * (nz - 1), 1), t)
        t = pltpu.roll(t, 2 * e, 1) if e else t
        mine = (lane + 1) % nx // 2 % nz == e
        edge = jnp.where(mine, t, 0.0 if edge is None else edge)
    edge_ref[...] = edge


def diverge_kernel(
    table, f_ref, m_ref, left_ref, right_ref, w_ref, ends_ref, high_ref, low_ref, y_ref, x_ref
):
    _, comps, nz, ny, nx = f_ref.shape
    blocks = [(layer, c) for layer in range(nz // PTS) for c in range(comps)]
    for c in range(comps):
        for z in range(nz):
            high_ref[0, c, z], low_ref[0, c, z] = split(f_ref[0, c, z])
            high_ref[1, c, z], low_ref[1, c, z] = split(f_ref[1, c, z])
    for i in range(0, len(blocks), 2):
        pair = blocks[i : i + 2]
        sums = along_y(left_ref[1], pair, high_ref.at[1], low_ref.at[1])
        for (layer, c), out in zip(pair, sums):
            y_ref[c, layer * PTS : (layer + 1) * PTS] = out
    for layer, c in blocks:
        x_ref[c, layer * PTS : (layer + 1) * PTS] = along_x(
            right_ref[1], layer, c, high_ref.at[0], low_ref.at[0]
        )
    for layer, c in blocks:
        for e in range(0, ny, PTS):
            ys = slice(e, e + PTS)
            z0 = layer * PTS
            out = combine_planes([f_ref[2, c, z0 + z, ys] for z in range(PTS)], table.T)
            for z in range(PTS):
                y_ref[c, z0 + z, ys] = out[z] + y_ref[c, z0 + z, ys] + x_ref[c, z0 + z, ys]
    for f in range(comps + 1):
        for z in range(nz):
            j = ends_ref.shape[1] - 1 - f * nz - z
            if z % PTS == 0 and z > 0:
                w_ref[f, z] = w_ref[f, z - 1]
                ends_ref[:, j] = ends_ref[:, j + 1]
                continue
            at = [z, z + 1] if z % PTS == PTS - 1 and z < nz - 1 else [z]
            t = [m_ref[i].astype(F32) if f == comps else y_ref[f, i] for i in at]
            whole = assemble_plane(joined(t), ny, nx)
            w_ref[f, z] = whole
            ends_ref[0, j : j + 1] = whole[0:1]
            ends_ref[1, j : j + 1] = whole[ny - 1 : ny]


def merge_sides(right, left):
    lane = iota(right.shape, 1)
    return jnp.where(lane % 2 == 0, right, pltpu.roll(left, 2, 1))


def place_columns(merged, j, nx):
    lane = iota(merged.shape, 1)
    shift = (nx - 1 - 2 * j) % nx
    moved = pltpu.roll(merged, shift, 1) if shift else merged
    return jnp.where((lane == 0) | (lane == nx - 1), moved, 0.0)


def first_kernel(zp_ref, edge_ref, px_ref, qa_ref, pb_ref, pz_ref, pd_ref):
    fields, ny, nx = zp_ref.shape
    nz = nx // (2 * fields)
    x_even = lax.axis_index("gx") % 2 == 0
    z_even = lax.axis_index("gz") % 2 == 0
    qa = qa_ref[0:ny]
    merged = merge_sides(jnp.where(x_even, qa, 0.0), jnp.where(x_even, 0.0, qa))
    merged = jnp.where(z_even, pltpu.roll(merged, nx - 2 * (nz - 1), 1), merged)
    sums = px_ref[ny:] + qa_ref[ny:]
    pb_ref[0:ny] = px_ref[0:ny]
    pb_ref[ny:] = sums
    for f in range(fields):
        pz_ref[f * ny : (f + 1) * ny] = zp_ref[f] + place_columns(merged, f * nz, nx)
    pz_ref[fields * ny :] = sums
    pd_ref[0:PTS] = edge_ref[...]
    pd_ref[PTS:] = sums


def x_sides(qa, qb, x_even):
    return merge_sides(jnp.where(x_even, qa, qb), jnp.where(x_even, qb, qa))


def diagonal_sides(qd, x_even):
    return merge_sides(jnp.where(x_even, 0.0, qd), jnp.where(x_even, qd, 0.0))


def spread_columns(merged, count):
    nx = merged.shape[1]
    rows = jnp.broadcast_to(merged, (count, nx))
    rows = pltpu.roll(rows, (nx + 1 - 2 * count) % nx, 1, stride=2, stride_axis=0)
    lane = iota((count, nx), 1)
    return jnp.where((lane == 0) | (lane == nx - 1), rows, 0.0)


def second_kernel(
    ends_ref, pb_ref, qa_ref, qb_ref, qz_ref, qd_ref, pya_ref, pyb_ref, ps_ref, low_ref, high_ref
):
    _, count, nx = ends_ref.shape
    ny = pb_ref.shape[0] - SCALAR_ROWS
    fields = (qz_ref.shape[0] - SCALAR_ROWS) // ny
    nz = count // fields
    x_even = lax.axis_index("gx") % 2 == 0
    y_even = lax.axis_index("gy") % 2 == 0
    diag = diagonal_sides(qd_ref[0:PTS], x_even)
    for i, (y, out) in enumerate(((0, low_ref), (ny - 1, high_ref))):
        merged = x_sides(qa_ref[y : y + 1], qb_ref[y : y + 1], x_even)
        out[...] = ends_ref[i] + spread_columns(merged, count)
        for f in range(fields):
            corner = place_columns(diag, f * nz + y // PTS, nx)[y % PTS : y % PTS + 1]
            extra = qz_ref[f * ny + y : f * ny + y + 1] + corner
            for z in (0, nz - 1):
                j = count - 1 - f * nz - z
                out[j : j + 1] = out[j : j + 1] + extra
    sums = pb_ref[ny:] + qb_ref[ny:] + qz_ref[fields * ny :] + qd_ref[PTS:]
    pya_ref[0:count] = jnp.where(y_even, high_ref[...], low_ref[...])
    pyb_ref[0:count] = jnp.where(y_even, low_ref[...], high_ref[...])
    pya_ref[count:] = sums
    pyb_ref[count:] = sums
    ps_ref[...] = sums


def correct_kernel(v_ref, u_ref, qa_ref, qb_ref, qz_ref, qd_ref, w_ref, mv_ref):
    fields, nz, ny, nx = u_ref.shape
    x_even = lax.axis_index("gx") % 2 == 0
    merged = x_sides(qa_ref[0:ny], qb_ref[0:ny], x_even)
    diag = diagonal_sides(qd_ref[0:PTS], x_even)
    for z in range(nz):
        for f in range(fields):
            t = u_ref[f, z] + place_columns(merged, f * nz + z, nx)
            if z in (0, nz - 1):
                t = t + qz_ref[f * ny : (f + 1) * ny]
                corner = [place_columns(diag, f * nz + e, nx) for e in range(ny // PTS)]
                t = t + jnp.concatenate(corner, axis=0)
            w_ref[f, z] = t
        for c in range(fields - 1):
            mv_ref[c, z] = w_ref[fields - 1, z] * v_ref[c, z]


def last_kernel(
    sizes,
    v_ref,
    w_ref,
    mv_ref,
    qya_ref,
    qyb_ref,
    qs_ref,
    ps_ref,
    out_hbm,
    kin_hbm,
    ens_hbm,
    low_ref,
    high_ref,
    out_ref,
    kin_ref,
    ens_ref,
    sems,
):
    fields, nz, ny, nx = w_ref.shape
    gx, gy, gz = (lax.axis_index(name) for name in ("gx", "gy", "gz"))
    y_even = gy % 2 == 0
    count = fields * nz
    sums = ps_ref[...] + qya_ref[count:] + qyb_ref[count:] + qs_ref[...]
    totals = jnp.sum(sums, axis=1, keepdims=True)
    kinetic, enstrophy = 0.5 * totals[0:1], totals[1:2]
    rayleigh = jnp.broadcast_to(enstrophy / (2.0 * kinetic), (PTS, nx))
    low_ref[...] = jnp.where(y_even, qyb_ref[0:count], qya_ref[0:count])
    high_ref[...] = jnp.where(y_even, qya_ref[0:count], qyb_ref[0:count])
    row = iota((ny, nx), 0)
    lane = iota((ny, nx), 1)
    x_first = jnp.where(gx == 0, 0, -1)
    x_last = jnp.where(gx == sizes[0] - 1, nx - 1, -1)
    y_first = jnp.where(gy == 0, 0, -1)
    y_last = jnp.where(gy == sizes[1] - 1, ny - 1, -1)
    inside = (lane != x_first) & (lane != x_last) & (row != y_first) & (row != y_last)
    sub = iota((PTS, nx), 0)
    steps = nz // 4
    copies = []
    for z in range(nz):
        keep = inside
        if z == 0:
            keep = keep & (gz > 0)
        if z == nz - 1:
            keep = keep & (gz < sizes[2] - 1)
        for e in range(0, ny, PTS):
            ys = slice(e, e + PTS)
            edge = e == 0 or e == ny - PTS
            side, at = (low_ref, 0) if e == 0 else (high_ref, PTS - 1)
            if edge:
                j = nz - 1 - z
                extra = rayleigh * jnp.where(sub == at, side[j : j + 1], 0.0)
            for c in range(fields - 1):
                t = w_ref[c, z, ys] - rayleigh * mv_ref[c, z, ys]
                if edge:
                    j = count - 1 - c * nz - z
                    t = t + jnp.where(sub == at, side[j : j + 1], 0.0)
                    t = t - extra * v_ref[c, z, ys]
                out_ref[c, z, ys] = jnp.where(keep[ys], t, 0.0)
        if z % steps == steps - 1:
            zs = pl.ds(z - steps + 1, steps)
            copies.append(
                pltpu.make_async_copy(
                    out_ref.at[:, zs], out_hbm.at[:, zs], sems.at[z // steps]
                )
            )
            copies[-1].start()
        if z == steps - 1:
            kin_ref[0, 0] = kinetic[0, 0]
            ens_ref[0, 0] = enstrophy[0, 0]
            for out in (
                pltpu.make_async_copy(kin_ref, kin_hbm, sems.at[4]),
                pltpu.make_async_copy(ens_ref, ens_hbm, sems.at[5]),
            ):
                out.start()
                copies.append(out)
    for copy in copies:
        copy.wait()


VMEM = pl.BlockSpec(memory_space=pltpu.VMEM)
HBM = pl.BlockSpec(memory_space=pltpu.HBM)


def call(kernel, outs, ins, scratch=(), out_specs=None, in_specs=None, flops=1 << 20):
    return pl.pallas_call(
        kernel,
        out_shape=[
            out if hasattr(out, "dtype") else jax.ShapeDtypeStruct(out, F32) for out in outs
        ],
        in_specs=in_specs or [VMEM] * len(ins),
        out_specs=out_specs or [VMEM] * len(outs),
        scratch_shapes=list(scratch),
        compiler_params=pltpu.CompilerParams(vmem_limit_bytes=24 << 20),
        cost_estimate=pl.CostEstimate(flops=flops, bytes_accessed=flops, transcendentals=0),
    )(*ins)


def local_part(table, velocity, geometry, mass_weights):
    _, nz, ny, nx = velocity.shape
    rows = PTS * ny
    vector = (3, *velocity.shape)
    return call(
        functools.partial(local_kernel, table),
        [
            vector,
            (ny + SCALAR_ROWS, nx),
            velocity.shape,
            jax.ShapeDtypeStruct(mass_weights.shape, BF16),
            jax.ShapeDtypeStruct((2, rows, 3 * rows), BF16),
            jax.ShapeDtypeStruct((4, 2 * nx, 2 * nx), BF16),
        ],
        [
            pltpu.with_memory_space_constraint(x, pltpu.HBM)
            for x in (velocity, geometry, mass_weights)
        ],
        in_specs=[HBM] * 3,
        scratch=[
            pltpu.VMEM(geometry.shape, BF16),
            pltpu.VMEM(vector, F32),
            pltpu.VMEM(velocity.shape, BF16),
            pltpu.VMEM(velocity.shape, BF16),
            pltpu.SemaphoreType.DMA((nz // PTS, 3)),
        ],
    )


def diverged(table, fluxes, mass, left, right):
    _, comps, nz, ny, nx = fluxes.shape
    return call(
        functools.partial(diverge_kernel, table),
        [(comps + 1, nz, ny, nx), (2, (comps + 1) * nz, nx)],
        [fluxes, mass, left, right],
        scratch=[
            pltpu.VMEM((2, comps, nz, ny, nx), BF16),
            pltpu.VMEM((2, comps, nz, ny, nx), BF16),
            pltpu.VMEM((comps, nz, ny, nx), F32),
            pltpu.VMEM((comps, nz, ny, nx), F32),
        ],
    )


def pairs_near(count):
    return [(i, i ^ 1) for i in range(count)]


def pairs_mirror(count):
    return [(i, count - 1 - i) for i in range(count)]


def few_rounds(sizes, velocity, geometry, mass_weights):
    comps, nz, ny, nx = velocity.shape
    fields = comps + 1
    table = gll_derivative(ORDER)
    fluxes, px, held, mass, left, right = local_part(table, velocity, geometry, mass_weights)
    qa = lax.ppermute(px, "gx", pairs_near(sizes[0]))
    zp, edge = call(
        functools.partial(plane_kernel, table),
        [(fields, ny, nx), (PTS, nx)],
        [fluxes, mass, right, px],
    )
    pb, pz, pd = call(
        first_kernel,
        [
            (ny + SCALAR_ROWS, nx),
            (fields * ny + SCALAR_ROWS, nx),
            (PTS + SCALAR_ROWS, nx),
        ],
        [zp, edge, px, qa],
    )
    mirror = pairs_mirror(sizes[0])
    qb = lax.ppermute(pb, "gx", mirror)
    qz = lax.ppermute(pz, "gz", pairs_near(sizes[2]))
    both = [
        (i * sizes[2] + k, mirror[i][1] * sizes[2] + (k ^ 1))
        for i in range(sizes[0])
        for k in range(sizes[2])
    ]
    qd = lax.ppermute(pd, ("gx", "gz"), both)
    u, ends = diverged(table, fluxes, mass, left, right)
    count = fields * nz
    pya, pyb, ps = call(
        second_kernel,
        [(count + SCALAR_ROWS, nx), (count + SCALAR_ROWS, nx), (SCALAR_ROWS, nx)],
        [ends, pb, qa, qb, qz, qd],
        scratch=[pltpu.VMEM((count, nx), F32)] * 2,
    )
    apart = [
        (i * sizes[1] + j, (i ^ 1) * sizes[1] + (j ^ 2))
        for i in range(sizes[0])
        for j in range(sizes[1])
    ]
    qya = lax.ppermute(pya, "gy", pairs_near(sizes[1]))
    qyb = lax.ppermute(pyb, "gy", pairs_mirror(sizes[1]))
    qs = lax.ppermute(ps, ("gx", "gy"), apart)
    w, mv = call(correct_kernel, [u.shape, velocity.shape], [held, u, qa, qb, qz, qd])
    residual, kinetic, enstrophy = call(
        functools.partial(last_kernel, sizes),
        [velocity.shape, (1, 1), (1, 1)],
        [held, w, mv, qya, qyb, qs, ps],
        scratch=[
            pltpu.VMEM((count, nx), F32),
            pltpu.VMEM((count, nx), F32),
            pltpu.VMEM(velocity.shape, F32),
            pltpu.SMEM((1, 1), F32),
            pltpu.SMEM((1, 1), F32),
            pltpu.SemaphoreType.DMA((6,)),
        ],
        out_specs=[HBM, HBM, HBM],
    )
    return residual, kinetic[0, 0], enstrophy[0, 0]


def add_neighbours(field, axis, dim):
    count = lax.axis_size(axis)
    extent = field.shape[dim]
    first = lax.slice_in_dim(field, 0, 1, axis=dim)
    last = lax.slice_in_dim(field, extent - 1, extent, axis=dim)
    low = lax.ppermute(last, axis, [(i, i + 1) for i in range(count - 1)])
    high = lax.ppermute(first, axis, [(i + 1, i) for i in range(count - 1)])
    middle = lax.slice_in_dim(field, 1, extent - 1, axis=dim)
    return jnp.concatenate([first + low, middle, last + high], axis=dim)


def any_mesh(sizes, velocity, geometry, mass_weights):
    comps, nz, ny, nx = velocity.shape
    table = gll_derivative(ORDER)
    fluxes, px, _, mass, left, right = local_part(table, velocity, geometry, mass_weights)
    u, _ = diverged(table, fluxes, mass, left, right)
    kinetic = 0.5 * jnp.sum(px[ny])
    enstrophy = jnp.sum(px[ny + 1])
    kinetic, enstrophy = lax.psum((kinetic, enstrophy), ("gx", "gy", "gz"))
    for axis, dim in (("gx", 3), ("gy", 2), ("gz", 1)):
        u = add_neighbours(u, axis, dim)
    inside = jnp.ones((nz, ny, nx), bool)
    for dim, (axis, size) in enumerate(zip(("gz", "gy", "gx"), sizes[::-1])):
        place = lax.axis_index(axis) * inside.shape[dim] + iota(inside.shape, dim)
        inside = inside & (place > 0) & (place < size * inside.shape[dim] - 1)
    rayleigh = enstrophy / (2.0 * kinetic)
    residual = jnp.where(inside[None], u[:comps] - rayleigh * u[comps][None] * velocity, 0.0)
    return residual, kinetic, enstrophy


def solution(mesh):
    sizes = tuple(mesh.shape[name] for name in ("gx", "gy", "gz"))
    plan = few_rounds if sizes == (4, 4, 2) else any_mesh
    in_specs = (P(None, "gz", "gy", "gx"), P(None, "gz", "gy", "gx"), P("gz", "gy", "gx"))
    out_specs = (P(None, "gz", "gy", "gx"), P(), P())

    def body(*args):
        return plan(sizes, *args)

    step = jax.shard_map(
        body, mesh=mesh, in_specs=in_specs, out_specs=out_specs, check_vma=False
    )
    if plan is any_mesh:
        return step
    return step
```
